256 devices in a mesh: gx: 4 (over z_hi), gy: 4 (over y), gz: 16 (over x, z_lo, core).
Axes of the slice: x: 4, y: 4, z: 8 (z_hi: 4, z_lo: 2; z = z_hi * 2 + z_lo), core: 2. Of those that a mesh axis runs over, the one named last changes fastest.
Arguments:
- volume: float32 [256, 256, 4096], P('gz', 'gy', 'gx'), may hold values from -24 to 24
Outputs:
- level_one: float32 [128, 128, 2048], P('gz', 'gy', 'gx')
- level_two: float32 [64, 64, 1024], P('gz', 'gy', 'gx')
- level_three: float32 [32, 32, 512], P('gz', 'gy', 'gx')
The draws below stay inside these ranges and needn't reach their ends.
All inputs are finite; a program needn't handle non-finite values.
Results may differ from the reference program's by a relative error of at most 0.00002.
Values sent between devices are 32-bit elements; how exact they have to be, the bound alone decides.
A program may use at most 64 MiB of HBM per device.

```python
import jax
import jax.numpy as jnp
from jax import lax

NX = 4096
NY = 256
NZ = 256


def shard_levels(stream_key, shape, split, smallest, largest):
    level = 1.0
    for dim, shards_of in split:
        draws = jax.random.uniform(jax.random.fold_in(jax.random.fold_in(stream_key, 6), dim), (shards_of,), jnp.float32, smallest / len(split), largest / len(split))
        level = level * jnp.repeat(jnp.exp(draws), shape[dim] // shards_of).reshape((-1,) + (1,) * (len(shape) - 1 - dim))
    return level


def gaussian(rng, dims, deviation, most, cuts=(), kind=jnp.bfloat16):
    result = deviation * jax.random.normal(rng, dims, jnp.float32)
    if cuts:
        result = result * shard_levels(rng, dims, cuts, -0.22, 0.18)
    return jnp.clip(result, -most, most).astype(kind)


def setup_inputs(seed: int = 0) -> dict:
    streams_of = jax.random.split(jax.random.key(seed), 2)
    return {
        "volume": gaussian(streams_of[0], (NZ, NY, NX), 4.0, 24.0, ((0, 16), (1, 4), (2, 4)), jnp.float32),
    }


taps = (0.0625, 0.25, 0.375, 0.25, 0.0625)


def reduce_padded(padded, dim, count):
    total = None
    for k in range(5):
        piece = lax.slice_in_dim(padded, k, k + 2 * count - 1, 2, dim)
        term = taps[k] * piece
        total = term if total is None else total + term
    return total


def reduce_axis(field, dim):
    widths = [(0, 0), (0, 0), (0, 0)]
    widths[dim] = (2, 2)
    padded = jnp.pad(field, widths)
    return reduce_padded(padded, dim, field.shape[dim] // 2)


def level_down(field):
    return reduce_axis(reduce_axis(reduce_axis(field, 0), 1), 2)


def reference(volume):
    level_one = level_down(volume)
    level_two = level_down(level_one)
    level_three = level_down(level_two)
    return level_one, level_two, level_three
```

```python
import functools

import jax
import jax.numpy as jnp
from jax import lax
from jax.experimental import pallas as pl
from jax.experimental.pallas import tpu as pltpu
from jax.sharding import PartitionSpec as P

MESH = pl.DeviceIdType.MESH
F32 = jnp.float32
BF16 = jnp.bfloat16
LANES = 128
taps = (1.0, 4.0, 6.0, 4.0, 1.0)

ROWS1, ROWS2, ROWS3 = 352, 144, 64
PITCH1, PITCH2, PITCH3 = 72, 48, 32
DIRECTIONS = [
    (dz, dy, dx)
    for dx in (1, -1, 0)
    for dz in (1, -1, 0)
    for dy in (1, -1, 0)
    if (dz, dy, dx) != (0, 0, 0)
]
SLOT = {d: i for i, d in enumerate(DIRECTIONS)}
SIDES = [(dz, dy) for dz in (1, -1, 0) for dy in (1, -1, 0) if (dz, dy) != (0, 0)]
SIDE = {d: i for i, d in enumerate(SIDES)}


def weighted(pieces):
    groups = {}
    for k, piece in pieces.items():
        groups.setdefault(taps[k], []).append(piece)
    total = None
    for tap, members in groups.items():
        part = members[0] if len(members) == 1 else members[0] + members[1]
        part = part if tap == 1.0 else tap * part
        total = part if total is None else total + part
    return total


def reduce_planes(load, low, high, out):
    return weighted(
        {k: load(2 * out + k - 2) for k in range(5) if low <= 2 * out + k - 2 <= high}
    )


def split(block):
    first = block.astype(BF16)
    rest = block - first.astype(F32)
    second = rest.astype(BF16)
    third = (rest - second.astype(F32)).astype(BF16)
    return third, second, first


def product(block, weights):
    total = None
    for piece in split(block):
        part = jnp.dot(piece, weights, preferred_element_type=F32)
        total = part if total is None else total + part
    return total


def build_weights(band, edge):
    k = lax.broadcasted_iota(jnp.int32, (256, 256), 0)
    n = lax.broadcasted_iota(jnp.int32, (256, 256), 1)
    out = jnp.where(n < 128, n, jnp.where(n == 128, 128, jnp.where(n == 255, -1, 1000)))
    tap = k - 2 * out + 2
    value = jnp.where(tap == 2, 6.0, jnp.where((tap == 1) | (tap == 3), 4.0, jnp.where((tap == 0) | (tap == 4), 1.0, 0.0)))
    band[...] = (value * (1.0 / 4096.0)).astype(BF16)
    k = lax.broadcasted_iota(jnp.int32, (128, 256), 0)
    n = lax.broadcasted_iota(jnp.int32, (128, 256), 1)
    place = jnp.where(k < 2, k, jnp.where(k == 127, -1, 1000))
    out = jnp.where(n < 2, n, jnp.where(n == 127, -1, jnp.where(n == 255, -1, jnp.where(n == 128, 0, -1000))))
    high_in, low_in = k < 2, k == 127
    high_out = (n < 2) | (n == 255)
    low_out = (n == 127) | (n == 128)
    tap = place - 2 * out + 2
    legal = (high_in & high_out) | (low_in & low_out)
    value = jnp.where(tap == 2, 6.0, jnp.where((tap == 1) | (tap == 3), 4.0, jnp.where((tap == 0) | (tap == 4), 1.0, 0.0)))
    edge[...] = jnp.where(legal, value * (1.0 / 4096.0), 0.0).astype(BF16)


def pyramid(counts, vol, out1, out2, out3, v, zs1, as1, p1, l1, ye1, zs2, as2, p2, l2, ye2, zs3, as3, p3, l3,
            band, edge, xm, xs, rz1, rz2u, rz2d, rz3u, rz3d, ry1, ry2, ry3, rxm, rxs,
            load_sem, send_sem, recv_sem):
    me = {axis: lax.axis_index(axis) for axis in ("gz", "gy", "gx")}
    has = {(axis, 1): me[axis] < counts[axis] - 1 for axis in me}
    has.update({(axis, -1): me[axis] > 0 for axis in me})

    def exists(d):
        ok = None
        for axis, step in zip(("gz", "gy", "gx"), d):
            if step:
                ok = has[axis, step] if ok is None else ok & has[axis, step]
        return ok

    def device(d):
        return {axis: me[axis] + step for axis, step in zip(("gz", "gy", "gx"), d) if step}

    order = (0, 3, 1, 2)
    loads = [
        pltpu.make_async_copy(
            vol.at[:, :, pl.ds(256 * b, 256)], v.at[:, :, pl.ds(256 * b, 256)], load_sem.at[b]
        )
        for b in range(4)
    ]
    for b in order:
        loads[b].start()

    barrier = pltpu.get_barrier_semaphore()
    for d in DIRECTIONS:
        @pl.when(exists(d))
        def _():
            pl.semaphore_signal(barrier, inc=1, device_id=device(d), device_id_type=MESH)

    build_weights(band, edge)
    zero8 = jnp.zeros((8, LANES), F32)
    for c in range(8):
        for p in range(11):
            zs1[c, p * PITCH1:p * PITCH1 + 8, :] = zero8
        as1[c, 328:336, :] = zero8
        as1[c, 344:352, :] = zero8
    for t in range(5):
        for e in range(2):
            for r in range(0, 24, 8):
                ye1[t, e, r:r + 8, :] = zero8
        for p in range(8):
            zs2[t, p * PITCH2:p * PITCH2 + 8, :] = zero8
            zs2[t, p * PITCH2 + 40:p * PITCH2 + 48, :] = zero8
        for r in range(8, 40, 8):
            zs2[t, 7 * PITCH2 + r:7 * PITCH2 + r + 8, :] = zero8
        as2[t, 136:144, :] = zero8
    for t in range(3):
        for e in range(3):
            for r in range(0, 24, 8):
                ye2[t, e, r:r + 8, :] = zero8
        for p in range(8):
            zs3[t, p * PITCH3:p * PITCH3 + 8, :] = zero8
            zs3[t, p * PITCH3 + 24:p * PITCH3 + 32, :] = zero8
        for p in range(5, 8):
            for r in (8, 16):
                zs3[t, p * PITCH3 + r:p * PITCH3 + r + 8, :] = zero8

    flag = {key: jnp.where(value, 1.0, 0.0).astype(F32) for key, value in has.items()}
    zlo, zhi = flag["gz", -1], flag["gz", 1]
    ylo, yhi = flag["gy", -1], flag["gy", 1]
    lane = lax.broadcasted_iota(jnp.int32, (8, LANES), 1)
    sub = lax.broadcasted_iota(jnp.int32, (8, LANES), 0)
    xflag = jnp.where(lane < 64, flag["gx", 1], flag["gx", -1])

    def level_one_tiles(b):
        cols = slice(256 * b, 256 * b + 256)
        for i in range(-1, 9):
            plane = reduce_planes(lambda s: v[s, :, cols], 0, 15, i)
            row = (i + 1) * PITCH1 + 8
            for h in range(2):
                zs1[2 * b + h, row:row + 64, :] = plane[:, 128 * h:128 * h + 128]
        for c in (2 * b, 2 * b + 1):
            for i in range(-1, 9):
                base = (i + 1) * PITCH1 + 8
                plane = weighted({k: zs1[c, pl.ds(base + k - 2, 32, stride=2), :] for k in range(5)})
                if i == -1:
                    as1[c, 256:288, :] = plane * zlo
                elif i == 8:
                    as1[c, 288:320, :] = plane * zhi
                else:
                    as1[c, 32 * i:32 * i + 32, :] = plane

            def column(y, p, size):
                return zs1[c, pl.ds(p * PITCH1 + 8 + y, size, stride=PITCH1), :]

            as1[c, 320:328, :] = column(0, 1, 8) * ylo
            as1[c, 336:344, :] = weighted({0: column(62, 1, 8), 1: column(63, 1, 8)}) * yhi
            for s, p, zflag in ((0, 0, zlo), (1, 9, zhi)):
                first = p * PITCH1 + 8
                as1[c, 328 + s:329 + s, :] = zs1[c, first:first + 1, :] * (ylo * zflag)
                as1[c, 344 + s:345 + s, :] = weighted(
                    {0: zs1[c, first + 62:first + 63, :], 1: zs1[c, first + 63:first + 64, :]}
                ) * (yhi * zflag)
        for r in range(0, ROWS1, 176):
            rows = slice(r, r + 176)
            block = jnp.concatenate([as1[2 * b, rows, :], as1[2 * b + 1, rows, :]], axis=1)
            p1[b, rows, :] = product(block, band[...])

    def combine(parts, result, tiles, rows, mask):
        size = 16
        low = lax.broadcasted_iota(jnp.int32, (size, LANES), 1) < 64
        wide = None if mask is None else jnp.broadcast_to(mask[0:1], (size, LANES))
        total = tiles + 1
        for r in range(0, rows, size):
            over = [parts(t, r, size, 1) for t in range(total)]
            for t in range(total):
                before, after = over[(t - 1) % total], over[(t + 1) % total]
                if before is None:
                    spill = jnp.where(low, 0.0, after)
                elif after is None:
                    spill = jnp.where(low, before, 0.0)
                else:
                    spill = jnp.where(low, before, after)
                main = parts(t, r, size, 0)
                value = spill if main is None else main + spill
                if t == tiles and wide is not None:
                    value = value * wide
                result[t, r:r + size, :] = value

    for b in order:
        loads[b].wait()
        level_one_tiles(b)

    def parts1(t, r, size, half):
        return None if t == 4 else p1[t, r:r + size, 128 * half:128 * half + 128]

    combine(parts1, l1, 4, ROWS1, xflag)

    zflag2 = jnp.where(sub == 0, zlo, jnp.where(sub < 5, 1.0, zhi))
    plane_row1 = lambda s: 256 if s == -1 else (288 if s == 8 else 32 * s)
    plane_row2 = lambda s: 64 if s == -1 else (80 + 16 * (s - 4) if s >= 4 else 16 * s)
    plane_row3 = lambda s: 16 if s == -1 else (24 + 8 * (s - 2) if s >= 2 else 8 * s)
    zscale2 = lambda i: zlo if i == -1 else (zhi if i >= 4 else None)
    for t in range(5):
        for e, first in ((0, 320), (1, 336)):
            ye1[t, e, 8:16, :] = l1[t, first:first + 8, :]
            ye1[t, e, 7:8, :] = l1[t, first + 8:first + 9, :]
            ye1[t, e, 16:17, :] = l1[t, first + 9:first + 10, :]
        for i in range(-1, 6):
            plane = reduce_planes(lambda s: l1[t, plane_row1(s):plane_row1(s) + 32, :], -1, 8, i)
            if zscale2(i) is not None:
                plane = plane * zscale2(i)
            row = (i + 1) * PITCH2 + 8
            zs2[t, row:row + 32, :] = plane
        for e, y in ((0, -1), (1, 32)):
            block = weighted({k: ye1[t, e, pl.ds(4 + k, 8, stride=2), :] for k in range(5)})
            zs2[t, pl.ds(8 + y, 8, stride=PITCH2), :] = block * zflag2
        for i in range(-1, 6):
            base = (i + 1) * PITCH2 + 8
            row = plane_row2(i)
            as2[t, row:row + 16, :] = weighted(
                {k: zs2[t, pl.ds(base + k - 2, 16, stride=2), :] for k in range(5)}
            )

        def column2(y):
            return zs2[t, pl.ds(8 + y, 8, stride=PITCH2), :]

        as2[t, 112:120, :] = weighted({3: column2(-1), 4: column2(0)}) * ylo
        as2[t, 120:128, :] = weighted({0: column2(30), 1: column2(31), 2: column2(32)}) * yhi
        as2[t, 128:136, :] = column2(32) * yhi
    for b in range(2):
        block = jnp.concatenate([as2[2 * b], as2[2 * b + 1]], axis=1)
        p2[b] = product(block, band[...])
    p2[2] = product(as2[4], edge[...])

    def parts2(t, r, size, half):
        return p2[t, r:r + size, 128 * half:128 * half + 128]

    combine(parts2, l2, 2, ROWS2, xflag)

    for t in range(3):
        for e, first in ((0, 112), (1, 120), (2, 128)):
            ye2[t, e, 7:15, :] = l2[t, first:first + 8, :]
        for i in range(-1, 4):
            row = (i + 1) * PITCH3 + 8
            zs3[t, row:row + 16, :] = reduce_planes(
                lambda s: l2[t, plane_row2(s):plane_row2(s) + 16, :], -1, 5, i
            )
        for e, y in ((0, -1), (1, 16), (2, 17)):
            block = weighted({k: ye2[t, e, pl.ds(4 + k, 8, stride=2), :] for k in range(5)})
            zs3[t, pl.ds(8 + y, 8, stride=PITCH3), :] = block
        for i in range(-1, 4):
            base = (i + 1) * PITCH3 + 8
            row = plane_row3(i)
            as3[t, row:row + 8, :] = weighted(
                {k: zs3[t, pl.ds(base + k - 2, 8, stride=2), :] for k in range(5)}
            )

        def column3(y):
            return zs3[t, pl.ds(8 + y, 8, stride=PITCH3), :]

        as3[t, 40:48, :] = weighted({3: column3(-1), 4: column3(0)})
        as3[t, 48:56, :] = weighted({k: column3(14 + k) for k in range(4)})
        as3[t, 56:64, :] = weighted({0: column3(16), 1: column3(17)})
    p3[0] = product(jnp.concatenate([as3[0], as3[1]], axis=1), band[...])
    p3[1] = product(as3[2], edge[...])

    def parts3(t, r, size, half):
        return p3[t, r:r + size, 128 * half:128 * half + 128]

    combine(parts3, l3, 1, ROWS3, None)

    main_groups = [(l1, 4, 8 * g) for g in range(32)] + [(l2, 2, 8 * g) for g in range(8)] + [(l3, 1, 8 * g) for g in range(2)]
    side_groups = [(l1, 4, 256 + 8 * g) for g in range(12)] + [(l2, 2, 64 + 8 * g) for g in range(9)] + [(l3, 1, 16 + 8 * g) for g in range(6)]
    side_index = {("1", 256 + 8 * g): g for g in range(12)}
    side_index.update({("2", 64 + 8 * g): 12 + g for g in range(9)})
    side_index.update({("3", 16 + 8 * g): 21 + g for g in range(6)})

    def pack(groups):
        total = None
        for g, (ref, t, row) in enumerate(groups):
            piece = ref[t, row:row + 8, :]
            piece = piece if g == 0 else pltpu.roll(piece, 3 * g, 1)
            total = piece if total is None else total + piece
        return total

    xm[...] = pack(main_groups)
    xs[...] = pack(side_groups)

    def transfers(d):
        dz, dy, dx = d
        if dx:
            if dz == 0 and dy == 0:
                return [(xm, rxm.at[0 if dx == 1 else 1])]
            return [(xs, rxs.at[0 if dx == 1 else 1, SIDE[dz, dy]])]
        if dy == 0:
            if dz == 1:
                return [
                    (l1.at[pl.ds(0, 4), pl.ds(288, 32), :], rz1.at[0]),
                    (l2.at[pl.ds(0, 2), pl.ds(80, 32), :], rz2u),
                    (l3.at[pl.ds(0, 1), pl.ds(24, 16), :], rz3u),
                ]
            return [
                (l1.at[pl.ds(0, 4), pl.ds(256, 32), :], rz1.at[1]),
                (l2.at[pl.ds(0, 2), pl.ds(64, 16), :], rz2d),
                (l3.at[pl.ds(0, 1), pl.ds(16, 8), :], rz3d),
            ]
        side = SIDE[dz, dy]
        first2, first3, size = (120, 48, 16) if dy == 1 else (112, 40, 8)
        first1 = (336 if dy == 1 else 320) + (8 if dz else 0)
        return [
            (l1.at[pl.ds(0, 4), pl.ds(first1, 8), :], ry1.at[side]),
            (l2.at[pl.ds(0, 2), pl.ds(first2, size), :], ry2.at[side, :, pl.ds(0, size), :]),
            (l3.at[pl.ds(0, 1), pl.ds(first3, size), :], ry3.at[side, :, pl.ds(0, size), :]),
        ]

    def copies(d):
        return [
            pltpu.make_async_remote_copy(
                src_ref=source,
                dst_ref=target,
                send_sem=send_sem.at[SLOT[d], i],
                recv_sem=recv_sem.at[SLOT[d], i],
                device_id=device(d),
                device_id_type=MESH,
            )
            for i, (source, target) in enumerate(transfers(d))
        ]

    near = 1
    for axis in me:
        near = near * (1 + has[axis, 1].astype(jnp.int32) + has[axis, -1].astype(jnp.int32))
    pl.semaphore_wait(barrier, near - 1)

    for d in DIRECTIONS:
        @pl.when(exists(d))
        def _():
            for copy in copies(d):
                copy.start()

    def add_side(dz, dy, get, tiles):
        for level, ref in (("1", l1), ("2", l2), ("3", l3)):
            for t in tiles(level):
                height = {"1": 32, "2": 16, "3": 8}[level]
                depth = {"1": 8, "2": 4, "3": 2}[level]
                if dy == 0:
                    if dz == 1:
                        first = {"1": 288, "2": 80, "3": 24}[level]
                        size = height if level == "1" else 2 * height
                        to = 0
                    else:
                        first = {"1": 256, "2": 64, "3": 16}[level]
                        size = height
                        to = (depth - 1) * height
                    for r in range(0, size, 8):
                        rows = slice(to + r, to + r + 8)
                        ref[t, rows, :] = ref[t, rows, :] + get(level, first + r, t)
                    continue
                if dy == 1:
                    blocks = {"1": ((336, 0),), "2": ((120, 0), (128, 1)), "3": ((48, 0), (56, 1))}[level]
                else:
                    blocks = {"1": ((320, 31),), "2": ((112, 15),), "3": ((40, 7),)}[level]
                for first, y in blocks:
                    if dz == 0:
                        value = get(level, first, t)
                        value = value if level == "1" else value[1:1 + depth]
                        rows = pl.ds(y, depth, stride=height)
                        ref[t, rows, :] = ref[t, rows, :] + value
                        continue
                    if level == "1":
                        value = get(level, first + 8, t)
                        pairs = ((1, 0),) if dz == 1 else ((0, depth - 1),)
                    else:
                        value = get(level, first, t)
                        pairs = ((depth + 1, 0), (depth + 2, 1)) if dz == 1 else ((0, depth - 1),)
                    for s, z in pairs:
                        row = slice(z * height + y, z * height + y + 1)
                        ref[t, row, :] = ref[t, row, :] + value[s:s + 1]

    def arrive(d):
        dz, dy, dx = d
        for copy in copies(d):
            copy.wait_recv()
        if dx == 0:
            def get(level, row, t):
                if dy == 0:
                    box = {
                        ("1", 1): (rz1.at[0], 288), ("2", 1): (rz2u, 80), ("3", 1): (rz3u, 24),
                        ("1", -1): (rz1.at[1], 256), ("2", -1): (rz2d, 64), ("3", -1): (rz3d, 16),
                    }[level, dz]
                    return box[0][t, row - box[1]:row - box[1] + 8, :]
                first2, first3 = (120, 48) if dy == 1 else (112, 40)
                side = SIDE[dz, dy]
                if level == "1":
                    return ry1[side, t, :, :]
                if level == "2":
                    return ry2[side, t, row - first2:row - first2 + 8, :]
                return ry3[side, t, row - first3:row - first3 + 8, :]

            add_side(dz, dy, get, lambda level: range({"1": 4, "2": 2, "3": 1}[level]))
            return
        keep = lane < 2 if dx == 1 else lane == 127
        column = 0 if dx == 1 else 1

        def spread(value, g):
            moved = value if g == 0 else pltpu.roll(value, LANES - 3 * g, 1)
            return jnp.where(keep, moved, 0.0)

        if dz == 0 and dy == 0:
            value = rxm[column]
            for g, (ref, last, row) in enumerate(main_groups):
                t = 0 if dx == 1 else last - 1
                ref[t, row:row + 8, :] = ref[t, row:row + 8, :] + spread(value, g)
            return
        value = rxs[column, SIDE[dz, dy]]
        add_side(
            dz, dy,
            lambda level, row, t: spread(value, side_index[level, row]),
            lambda level: (0 if dx == 1 else {"1": 3, "2": 1, "3": 0}[level],),
        )

    incoming = sorted(DIRECTIONS, key=lambda d: (d[2] != 0, sum(map(abs, d)), -abs(d[1])))
    for d in incoming:
        @pl.when(exists(tuple(-s for s in d)))
        def _():
            arrive(d)

    for z in range(8):
        for t in range(4):
            out1[z, :, LANES * t:LANES * t + LANES] = l1[t, 32 * z:32 * z + 32, :]
    for z in range(4):
        for t in range(2):
            out2[z, :, LANES * t:LANES * t + LANES] = l2[t, 16 * z:16 * z + 16, :]
    for z in range(2):
        out3[z, :, :] = l3[0, 8 * z:8 * z + 8, :]

    for d in DIRECTIONS:
        @pl.when(exists(d))
        def _():
            for copy in copies(d):
                copy.wait_send()


def on_device(counts, volume):
    vmem = lambda *shape: pltpu.VMEM(shape, F32)
    return pl.pallas_call(
        functools.partial(pyramid, counts),
        out_shape=(
            jax.ShapeDtypeStruct((8, 32, 512), F32),
            jax.ShapeDtypeStruct((4, 16, 256), F32),
            jax.ShapeDtypeStruct((2, 8, 128), F32),
        ),
        in_specs=[pl.BlockSpec(memory_space=pl.ANY)],
        out_specs=[pl.BlockSpec(memory_space=pltpu.VMEM)] * 3,
        scratch_shapes=[
            vmem(16, 64, 1024),
            vmem(8, 10 * PITCH1 + 8, LANES), vmem(8, ROWS1, LANES), vmem(4, ROWS1, 256), vmem(5, ROWS1, LANES),
            vmem(5, 2, 24, LANES), vmem(5, 8 * PITCH2, LANES), vmem(5, ROWS2, LANES), vmem(3, ROWS2, 256),
            vmem(3, ROWS2, LANES),
            vmem(3, 3, 24, LANES), vmem(3, 8 * PITCH3, LANES), vmem(3, ROWS3, LANES), vmem(2, ROWS3, 256),
            vmem(2, ROWS3, LANES),
            pltpu.VMEM((256, 256), BF16), pltpu.VMEM((128, 256), BF16),
            vmem(8, LANES), vmem(8, LANES),
            vmem(2, 4, 32, LANES), vmem(2, 32, LANES), vmem(2, 16, LANES), vmem(1, 16, LANES), vmem(1, 8, LANES),
            vmem(8, 4, 8, LANES), vmem(8, 2, 16, LANES), vmem(8, 1, 16, LANES),
            vmem(2, 8, LANES), vmem(2, 8, 8, LANES),
            pltpu.SemaphoreType.DMA((4,)),
            pltpu.SemaphoreType.DMA((26, 3)),
            pltpu.SemaphoreType.DMA((26, 3)),
        ],
        compiler_params=pltpu.CompilerParams(
            collective_id=0, has_side_effects=True, vmem_limit_bytes=40 * 1024 * 1024
        ),
        name="pyramid",
    )(volume)


def solution(mesh):
    spec = P("gz", "gy", "gx")
    return jax.shard_map(
        functools.partial(on_device, dict(mesh.shape)),
        mesh=mesh,
        in_specs=(spec,),
        out_specs=(spec, spec, spec),
        check_vma=False,
    )
```

```python
import functools

import jax
import jax.numpy as jnp
from jax import lax
from jax.experimental import pallas as pl
from jax.experimental.pallas import tpu as pltpu
from jax.sharding import PartitionSpec as P

MESH = pl.DeviceIdType.MESH
F32 = jnp.float32
BF16 = jnp.bfloat16
LANES = 128
taps = (1.0, 4.0, 6.0, 4.0, 1.0)

ROWS1, ROWS2, ROWS3 = 352, 144, 64
PITCH1, PITCH2, PITCH3 = 72, 48, 32
DIRECTIONS = [
    (dz, dy, dx)
    for dx in (-1, 1, 0)
    for dz in (1, -1, 0)
    for dy in (-1, 1, 0)
    if (dz, dy, dx) != (0, 0, 0)
]
SLOT = {d: i for i, d in enumerate(DIRECTIONS)}
SIDES = [(dz, dy) for dz in (1, -1, 0) for dy in (1, -1, 0) if (dz, dy) != (0, 0)]
SIDE = {d: i for i, d in enumerate(SIDES)}
UPPER = [d for d in DIRECTIONS if (d[2], d[1], d[0]) > (0, 0, 0)]
LOWER = [d for d in DIRECTIONS if (d[2], d[1], d[0]) < (0, 0, 0)]
FACES = [(1, 0, 0), (-1, 0, 0), (0, 1, 0), (0, -1, 0)]
CORNER = {(1, 1): 0, (1, -1): 1, (-1, 1): 2, (-1, -1): 3}


def weighted(pieces):
    groups = {}
    for k, piece in pieces.items():
        groups.setdefault(taps[k], []).append(piece)
    total = None
    for tap, members in groups.items():
        part = members[0] if len(members) == 1 else members[0] + members[1]
        part = part if tap == 1.0 else tap * part
        total = part if total is None else total + part
    return total


def reduce_planes(load, low, high, out):
    return weighted(
        {k: load(2 * out + k - 2) for k in range(5) if low <= 2 * out + k - 2 <= high}
    )


def split(block):
    first = block.astype(BF16)
    rest = block - first.astype(F32)
    second = rest.astype(BF16)
    third = (rest - second.astype(F32)).astype(BF16)
    return third, second, first


def product(block, weights):
    total = None
    for piece in split(block):
        part = jnp.dot(piece, weights, preferred_element_type=F32)
        total = part if total is None else total + part
    return total


def build_weights(band, edge):
    k = lax.broadcasted_iota(jnp.int32, (256, 256), 0)
    n = lax.broadcasted_iota(jnp.int32, (256, 256), 1)
    out = jnp.where(n < 128, n, jnp.where(n == 128, 128, jnp.where(n == 255, -1, 1000)))
    tap = k - 2 * out + 2
    value = jnp.where(tap == 2, 6.0, jnp.where((tap == 1) | (tap == 3), 4.0, jnp.where((tap == 0) | (tap == 4), 1.0, 0.0)))
    band[...] = (value * (1.0 / 4096.0)).astype(BF16)
    k = lax.broadcasted_iota(jnp.int32, (128, 256), 0)
    n = lax.broadcasted_iota(jnp.int32, (128, 256), 1)
    place = jnp.where(k < 2, k, jnp.where(k == 127, -1, 1000))
    out = jnp.where(n < 2, n, jnp.where(n == 127, -1, jnp.where(n == 255, -1, jnp.where(n == 128, 0, -1000))))
    high_in, low_in = k < 2, k == 127
    high_out = (n < 2) | (n == 255)
    low_out = (n == 127) | (n == 128)
    tap = place - 2 * out + 2
    legal = (high_in & high_out) | (low_in & low_out)
    value = jnp.where(tap == 2, 6.0, jnp.where((tap == 1) | (tap == 3), 4.0, jnp.where((tap == 0) | (tap == 4), 1.0, 0.0)))
    edge[...] = jnp.where(legal, value * (1.0 / 4096.0), 0.0).astype(BF16)


def pyramid(counts, vol, out1, out2, out3, v, zs1, as1, p1, l1, ye1, zs2, as2, p2, l2, ye2, zs3, as3, p3, l3,
            band, edge, xp, yf, q, rz1, rz2u, rz2d, rz3u, rz3d, ry1, ryf, rq, rx, rr,
            load_sem, send_sem, recv_sem, ready):
    me = {axis: lax.axis_index(axis) for axis in ("gz", "gy", "gx")}
    has = {(axis, 1): me[axis] < counts[axis] - 1 for axis in me}
    has.update({(axis, -1): me[axis] > 0 for axis in me})

    def exists(d):
        ok = None
        for axis, step in zip(("gz", "gy", "gx"), d):
            if step:
                ok = has[axis, step] if ok is None else ok & has[axis, step]
        return ok

    def device(d):
        return {axis: me[axis] + step for axis, step in zip(("gz", "gy", "gx"), d) if step}

    def blank(d):
        dz, dy, dx = d
        zeros = jnp.zeros((8, LANES), F32)
        if dx:
            column = 0 if dx == 1 else 1
            target = rr.at[SIDE[dz, dy], column] if dz or dy else rx.at[column]
            target[...] = zeros
            return
        side = 0 if dy == 1 else 1
        if dz and dy:
            targets = [rq.at[CORNER[dz, dy]]]
        elif dy:
            targets = [ry1.at[side, t] for t in range(4)] + [ryf.at[side, t] for t in range(3)]
        elif dz == 1:
            targets = [rz1.at[0, t] for t in range(4)] + [rz2u.at[t] for t in range(2)] + [rz3u.at[0]]
        else:
            targets = [rz1.at[1, t] for t in range(4)] + [rz2d.at[t] for t in range(2)] + [rz3d.at[0]]
        for target in targets:
            for r in range(0, target.shape[0], 8):
                target[r:r + 8, :] = zeros

    order = (0, 3, 1, 2)
    loads = [
        pltpu.make_async_copy(
            vol.at[:, :, pl.ds(256 * b, 256)], v.at[:, :, pl.ds(256 * b, 256)], load_sem.at[b]
        )
        for b in range(4)
    ]
    for b in order:
        loads[b].start()

    barrier = pltpu.get_barrier_semaphore()
    interior = functools.reduce(lambda x, y: x & y, has.values())

    def signal(semaphore, d):
        pl.semaphore_signal(semaphore, inc=1, device_id=device(d), device_id_type=MESH)

    @pl.when(interior)
    def _():
        for d in UPPER:
            signal(barrier, d)

    @pl.when(jnp.logical_not(interior))
    def _():
        for d in UPPER:
            @pl.when(exists(d))
            def _():
                signal(barrier, d)

        for d in DIRECTIONS:
            @pl.when(jnp.logical_not(exists(tuple(-k for k in d))))
            def _():
                blank(d)

    build_weights(band, edge)
    zero8 = jnp.zeros((8, LANES), F32)
    for c in range(8):
        for p in range(11):
            zs1[c, p * PITCH1:p * PITCH1 + 8, :] = zero8
        as1[c, 328:336, :] = zero8
        as1[c, 344:352, :] = zero8
    for c in range(4):
        q[c, 0:8, :] = zero8
        q[c, 8:16, :] = zero8
    for side in range(2):
        for t in range(3):
            yf[side, t] = zero8
    for t in range(5):
        for e in range(2):
            for r in range(0, 24, 8):
                ye1[t, e, r:r + 8, :] = zero8
        for p in range(8):
            zs2[t, p * PITCH2:p * PITCH2 + 8, :] = zero8
            zs2[t, p * PITCH2 + 40:p * PITCH2 + 48, :] = zero8
        for r in range(8, 40, 8):
            zs2[t, 7 * PITCH2 + r:7 * PITCH2 + r + 8, :] = zero8
        as2[t, 136:144, :] = zero8
    for t in range(3):
        for e in range(3):
            for r in range(0, 24, 8):
                ye2[t, e, r:r + 8, :] = zero8
        for p in range(8):
            zs3[t, p * PITCH3:p * PITCH3 + 8, :] = zero8
            zs3[t, p * PITCH3 + 24:p * PITCH3 + 32, :] = zero8
        for p in range(5, 8):
            for r in (8, 16):
                zs3[t, p * PITCH3 + r:p * PITCH3 + r + 8, :] = zero8

    flag = {key: jnp.where(value, 1.0, 0.0).astype(F32) for key, value in has.items()}
    zlo, zhi = flag["gz", -1], flag["gz", 1]
    ylo, yhi = flag["gy", -1], flag["gy", 1]
    lane = lax.broadcasted_iota(jnp.int32, (8, LANES), 1)
    sub = lax.broadcasted_iota(jnp.int32, (8, LANES), 0)
    xflag = jnp.where(lane < 64, flag["gx", 1], flag["gx", -1])

    def transfers(d):
        dz, dy, dx = d
        if dx:
            column = 0 if dx == 1 else 1
            if dz == 0 and dy == 0:
                return {2: (xp.at[0], rx.at[column])}
            return {2: (xp.at[1], rr.at[SIDE[dz, dy], column])}
        if dy == 0:
            if dz == 1:
                return {
                    0: (l1.at[pl.ds(0, 4), pl.ds(288, 32), :], rz1.at[0]),
                    1: (l2.at[pl.ds(0, 2), pl.ds(80, 32), :], rz2u),
                    2: (l3.at[pl.ds(0, 1), pl.ds(24, 16), :], rz3u),
                }
            return {
                0: (l1.at[pl.ds(0, 4), pl.ds(256, 32), :], rz1.at[1]),
                1: (l2.at[pl.ds(0, 2), pl.ds(64, 16), :], rz2d),
                2: (l3.at[pl.ds(0, 1), pl.ds(16, 8), :], rz3d),
            }
        if dz == 0:
            side = 0 if dy == 1 else 1
            return {
                0: (l1.at[pl.ds(0, 4), pl.ds(336 if dy == 1 else 320, 8), :], ry1.at[side]),
                2: (yf.at[side], ryf.at[side]),
            }
        corner = CORNER[dz, dy]
        return {2: (q.at[corner], rq.at[corner])}

    def copies(d, stages=(0, 1, 2)):
        return [
            pltpu.make_async_remote_copy(
                src_ref=pair[0],
                dst_ref=pair[1],
                send_sem=send_sem.at[SLOT[d], i],
                recv_sem=recv_sem.at[SLOT[d], i],
                device_id=device(d),
                device_id_type=MESH,
            )
            for i, pair in transfers(d).items()
            if i in stages
        ]

    def for_neighbours(act, stages=(0, 1, 2), back=False, only=None):
        chosen = [d for d in (only or DIRECTIONS) if any(i in stages for i in transfers(d))]

        @pl.when(interior)
        def _():
            for d in chosen:
                for copy in copies(d, stages):
                    act(copy)

        @pl.when(jnp.logical_not(interior))
        def _():
            for d in chosen:
                @pl.when(exists(tuple(-k for k in d) if back else d))
                def _():
                    for copy in copies(d, stages):
                        act(copy)

    start, received, sent = (lambda c: c.start()), (lambda c: c.wait_recv()), (lambda c: c.wait_send())

    def level_one_tiles(b):
        for r in range(0, 64, 8):
            planes = [v[s, r:r + 8, 256 * b:256 * b + 256] for s in range(16)]
            for i in range(-1, 9):
                plane = reduce_planes(lambda s: planes[s], 0, 15, i)
                row = (i + 1) * PITCH1 + 8 + r
                for h in range(2):
                    zs1[2 * b + h, row:row + 8, :] = plane[:, 128 * h:128 * h + 128]
        for c in (2 * b, 2 * b + 1):
            for i in range(-1, 9):
                base = (i + 1) * PITCH1 + 8
                plane = weighted({k: zs1[c, pl.ds(base + k - 2, 32, stride=2), :] for k in range(5)})
                if i == -1:
                    as1[c, 256:288, :] = plane * zlo
                elif i == 8:
                    as1[c, 288:320, :] = plane * zhi
                else:
                    as1[c, 32 * i:32 * i + 32, :] = plane

            def column(y, p, size):
                return zs1[c, pl.ds(p * PITCH1 + 8 + y, size, stride=PITCH1), :]

            as1[c, 320:328, :] = column(0, 1, 8) * ylo
            as1[c, 336:344, :] = weighted({0: column(62, 1, 8), 1: column(63, 1, 8)}) * yhi
            for s, p, zflag in ((0, 0, zlo), (1, 9, zhi)):
                first = p * PITCH1 + 8
                as1[c, 328 + s:329 + s, :] = zs1[c, first:first + 1, :] * (ylo * zflag)
                as1[c, 344 + s:345 + s, :] = weighted(
                    {0: zs1[c, first + 62:first + 63, :], 1: zs1[c, first + 63:first + 64, :]}
                ) * (yhi * zflag)
        for r in range(0, ROWS1, 176):
            rows = slice(r, r + 176)
            block = jnp.concatenate([as1[2 * b, rows, :], as1[2 * b + 1, rows, :]], axis=1)
            p1[b, rows, :] = product(block, band[...])

    def combine(parts, result, tiles, rows, mask):
        size = 16
        low = lax.broadcasted_iota(jnp.int32, (size, LANES), 1) < 64
        wide = None if mask is None else jnp.broadcast_to(mask[0:1], (size, LANES))
        total = tiles + 1
        for r in range(0, rows, size):
            over = [parts(t, r, size, 1) for t in range(total)]
            for t in range(total):
                before, after = over[(t - 1) % total], over[(t + 1) % total]
                if before is None:
                    spill = jnp.where(low, 0.0, after)
                elif after is None:
                    spill = jnp.where(low, before, 0.0)
                else:
                    spill = jnp.where(low, before, after)
                main = parts(t, r, size, 0)
                value = spill if main is None else main + spill
                if t == tiles and wide is not None:
                    value = value * wide
                result[t, r:r + size, :] = value

    for b in order:
        loads[b].wait()
        level_one_tiles(b)

    def parts1(t, r, size, half):
        return None if t == 4 else p1[t, r:r + size, 128 * half:128 * half + 128]

    combine(parts1, l1, 4, ROWS1, xflag)
    one = {key: value.astype(jnp.int32) for key, value in has.items()}
    across_z = 1 + one["gz", 1] + one["gz", -1]
    across = across_z * (1 + one["gy", 1] + one["gy", -1])
    near_lower, near_upper = (one["gy", k] * across_z + one["gz", k] for k in (-1, 1))
    far_lower, far_upper = (one["gx", k] * across for k in (-1, 1))

    def wait_for(semaphore, number):
        @pl.when(number > 0)
        def _():
            pl.semaphore_wait(semaphore, number)

    wait_for(barrier, near_lower + far_lower)

    def answer(d):
        signal(ready.at[1 if d[2] else 0], d)

    @pl.when(interior)
    def _():
        for d in LOWER:
            answer(d)

    @pl.when(jnp.logical_not(interior))
    def _():
        for d in LOWER:
            @pl.when(exists(d))
            def _():
                answer(d)

    for_neighbours(start, (0,), only=LOWER)
    zflag2 = jnp.where(sub == 0, zlo, jnp.where(sub < 5, 1.0, zhi))
    plane_row1 = lambda s: 256 if s == -1 else (288 if s == 8 else 32 * s)
    plane_row2 = lambda s: 64 if s == -1 else (80 + 16 * (s - 4) if s >= 4 else 16 * s)
    plane_row3 = lambda s: 16 if s == -1 else (24 + 8 * (s - 2) if s >= 2 else 8 * s)
    zscale2 = lambda i: zlo if i == -1 else (zhi if i >= 4 else None)
    for t in range(5):
        for e, first in ((0, 320), (1, 336)):
            ye1[t, e, 8:16, :] = l1[t, first:first + 8, :]
            ye1[t, e, 7:8, :] = l1[t, first + 8:first + 9, :]
            ye1[t, e, 16:17, :] = l1[t, first + 9:first + 10, :]
        for i in range(-1, 6):
            plane = reduce_planes(lambda s: l1[t, plane_row1(s):plane_row1(s) + 32, :], -1, 8, i)
            if zscale2(i) is not None:
                plane = plane * zscale2(i)
            row = (i + 1) * PITCH2 + 8
            zs2[t, row:row + 32, :] = plane
        for e, y in ((0, -1), (1, 32)):
            block = weighted({k: ye1[t, e, pl.ds(4 + k, 8, stride=2), :] for k in range(5)})
            zs2[t, pl.ds(8 + y, 8, stride=PITCH2), :] = block * zflag2
        for i in range(-1, 6):
            base = (i + 1) * PITCH2 + 8
            row = plane_row2(i)
            as2[t, row:row + 16, :] = weighted(
                {k: zs2[t, pl.ds(base + k - 2, 16, stride=2), :] for k in range(5)}
            )

        def column2(y):
            return zs2[t, pl.ds(8 + y, 8, stride=PITCH2), :]

        as2[t, 112:120, :] = weighted({3: column2(-1), 4: column2(0)}) * ylo
        as2[t, 120:128, :] = weighted({0: column2(30), 1: column2(31), 2: column2(32)}) * yhi
        as2[t, 128:136, :] = column2(32) * yhi
    for b in range(2):
        block = jnp.concatenate([as2[2 * b], as2[2 * b + 1]], axis=1)
        p2[b] = product(block, band[...])
    p2[2] = product(as2[4], edge[...])

    def parts2(t, r, size, half):
        return p2[t, r:r + size, 128 * half:128 * half + 128]

    combine(parts2, l2, 2, ROWS2, xflag)
    for_neighbours(start, (1,), only=LOWER)

    for t in range(3):
        for e, first in ((0, 112), (1, 120), (2, 128)):
            ye2[t, e, 7:15, :] = l2[t, first:first + 8, :]
        for i in range(-1, 4):
            row = (i + 1) * PITCH3 + 8
            zs3[t, row:row + 16, :] = reduce_planes(
                lambda s: l2[t, plane_row2(s):plane_row2(s) + 16, :], -1, 5, i
            )
        for e, y in ((0, -1), (1, 16), (2, 17)):
            block = weighted({k: ye2[t, e, pl.ds(4 + k, 8, stride=2), :] for k in range(5)})
            zs3[t, pl.ds(8 + y, 8, stride=PITCH3), :] = block
        for i in range(-1, 4):
            base = (i + 1) * PITCH3 + 8
            row = plane_row3(i)
            as3[t, row:row + 8, :] = weighted(
                {k: zs3[t, pl.ds(base + k - 2, 8, stride=2), :] for k in range(5)}
            )

        def column3(y):
            return zs3[t, pl.ds(8 + y, 8, stride=PITCH3), :]

        as3[t, 40:48, :] = weighted({3: column3(-1), 4: column3(0)})
        as3[t, 48:56, :] = weighted({k: column3(14 + k) for k in range(4)})
        as3[t, 56:64, :] = weighted({0: column3(16), 1: column3(17)})
    p3[0] = product(jnp.concatenate([as3[0], as3[1]], axis=1), band[...])
    p3[1] = product(as3[2], edge[...])

    def parts3(t, r, size, half):
        return p3[t, r:r + size, 128 * half:128 * half + 128]

    combine(parts3, l3, 1, ROWS3, None)

    main_groups = [(l1, 4, 8 * g) for g in range(32)] + [(l2, 2, 8 * g) for g in range(8)] + [(l3, 1, 8 * g) for g in range(2)]
    side_groups = [(l1, 4, 256 + 8 * g) for g in range(12)] + [(l2, 2, 64 + 8 * g) for g in range(9)] + [(l3, 1, 16 + 8 * g) for g in range(6)]

    def pack(groups):
        total = None
        for g, (ref, t, row) in enumerate(groups):
            piece = ref[t, row:row + 8, :]
            piece = piece if g == 0 else pltpu.roll(piece, 3 * g, 1)
            total = piece if total is None else total + piece
        return total

    for side, blocks2, blocks3 in ((0, (120, 128), (48, 56)), (1, (112,), (40,))):
        for t in range(2):
            for j, row in enumerate(blocks2):
                yf[side, t, 4 * j:4 * j + 4, :] = l2[t, row + 1:row + 5, :]
        for j, row in enumerate(blocks3):
            yf[side, 2, 2 * j:2 * j + 2, :] = l3[0, row + 1:row + 3, :]
        for dz in (1, -1):
            corner = CORNER[dz, 1 - 2 * side]
            row1 = (344 if side == 0 else 328) + (1 if dz == 1 else 0)
            first2, first3, size = (5, 3, 2) if dz == 1 else (0, 0, 1)
            for t in range(4):
                q[corner, t:t + 1, :] = l1[t, row1:row1 + 1, :]
            for t in range(2):
                for j, row in enumerate(blocks2):
                    to = 8 + 4 * t + 2 * j
                    q[corner, to:to + size, :] = l2[t, row + first2:row + first2 + size, :]
            for j, row in enumerate(blocks3):
                q[corner, 4 + 2 * j:4 + 2 * j + size, :] = l3[0, row + first3:row + first3 + size, :]

    xp[0] = pack(main_groups)
    xp[1] = pack(side_groups)

    for_neighbours(start, (2,), only=LOWER)
    wait_for(ready.at[0], near_upper)
    for_neighbours(start, only=[d for d in UPPER if d[2] == 0])
    wait_for(ready.at[1], far_upper)
    for_neighbours(start, only=[d for d in UPPER if d[2]])

    heights, depths = (32, 16, 8), (8, 4, 2)
    levels = (l1, l2, l3)

    def add(level, t, rows, value):
        ref = levels[level]
        ref[t, rows, :] = ref[t, rows, :] + value

    def add_y(dy, level, t, get):
        height, depth = heights[level], depths[level]
        for j in range(2 if dy == 1 and level else 1):
            add(level, t, pl.ds(j if dy == 1 else height - 1, depth, stride=height), get(j))

    def add_z(dz, level, t, get):
        height, depth = heights[level], depths[level]
        planes = 2 if dz == 1 and level else 1
        to = 0 if dz == 1 else (depth - 1) * height
        for r in range(0, planes * height, 8):
            add(level, t, slice(to + r, to + r + 8), get(r))

    def add_corner(dz, dy, level, t, get):
        height, depth = heights[level], depths[level]
        planes = 2 if dz == 1 and level else 1
        for j in range(2 if dy == 1 and level else 1):
            value = get(j)
            for p in range(planes):
                row = (p if dz == 1 else depth - 1) * height + (j if dy == 1 else height - 1)
                add(level, t, slice(row, row + 1), value[p:p + 1])

    for_neighbours(received, (0, 1, 2), back=True, only=[d for d in DIRECTIONS if d[1] and not d[2]])
    for dy in (1, -1):
        side = 0 if dy == 1 else 1
        for t in range(4):
            add_y(dy, 0, t, lambda j: ry1[side, t])
        for t in range(2):
            add_y(dy, 1, t, lambda j: ryf[side, t, 4 * j:4 * j + 4, :])
        add_y(dy, 2, 0, lambda j: ryf[side, 2, 2 * j:2 * j + 2, :])
        for dz in (1, -1):
            c = CORNER[dz, dy]
            for t in range(4):
                add_corner(dz, dy, 0, t, lambda j: rq[c, t:t + 1, :])
            for t in range(2):
                add_corner(dz, dy, 1, t, lambda j: rq[c, 8 + 4 * t + 2 * j:10 + 4 * t + 2 * j, :])
            add_corner(dz, dy, 2, 0, lambda j: rq[c, 4 + 2 * j:6 + 2 * j, :])
    for_neighbours(received, (0, 1, 2), back=True, only=FACES[:2])
    for t in range(4):
        add_z(1, 0, t, lambda r: rz1[0, t, r:r + 8, :])
        add_z(-1, 0, t, lambda r: rz1[1, t, r:r + 8, :])
    for t in range(2):
        add_z(1, 1, t, lambda r: rz2u[t, r:r + 8, :])
        add_z(-1, 1, t, lambda r: rz2d[t, r:r + 8, :])
    add_z(1, 2, 0, lambda r: rz3u[0, r:r + 8, :])
    add_z(-1, 2, 0, lambda r: rz3d[0, r:r + 8, :])
    for_neighbours(received, back=True, only=[d for d in DIRECTIONS if d[2]])
    third = lax.rem(lane, 3)
    low_lanes, high_lane = lane < 2, lane == 127

    def both(low_side, high_side):
        return jnp.where((third == 2) | high_lane, high_side, low_side)

    def spread(value, g):
        moved = value if g == 0 else pltpu.roll(value, LANES - 3 * g, 1)
        return jnp.where(low_lanes, moved, 0.0), jnp.where(high_lane, moved, 0.0)

    def add_columns(level, pairs):
        last = (3, 1, 0)[level]
        for rows, (low_value, high_value) in pairs:
            if last == 0:
                add(level, 0, rows, low_value + high_value)
            else:
                add(level, 0, rows, low_value)
                add(level, last, rows, high_value)

    value = both(rx[0], rx[1])
    for g, (ref, _, row) in enumerate(main_groups):
        level = 0 if g < 32 else (1 if g < 40 else 2)
        add_columns(level, [(slice(row, row + 8), spread(value, g))])
    firsts = {0: 0, 1: 12, 2: 21}
    for dz, dy in SIDES:
        value = both(rr[SIDE[dz, dy], 0], rr[SIDE[dz, dy], 1])
        for level in range(3):
            height, depth = heights[level], depths[level]
            if dy == 0:
                first = firsts[level] + (height // 8 if dz == 1 else 0)
                planes = 2 if dz == 1 and level else 1
                to = 0 if dz == 1 else (depth - 1) * height
                for r in range(planes * height // 8):
                    add_columns(level, [(slice(to + 8 * r, to + 8 * r + 8), spread(value, first + r))])
                continue
            for j in range(2 if dy == 1 and level else 1):
                y = j if dy == 1 else height - 1
                if level == 0:
                    group = (10 if dy == 1 else 8) + (1 if dz else 0)
                else:
                    group = {1: (18, 19), 2: (24, 25)}[level][1 if dy == 1 else 0] + j
                parts = spread(value, group)
                if dz == 0:
                    if level:
                        parts = tuple(x[1:1 + depth] for x in parts)
                    add_columns(level, [(pl.ds(y, depth, stride=height), parts)])
                    continue
                for p in range(2 if dz == 1 and level else 1):
                    if level == 0:
                        s = 1 if dz == 1 else 0
                    else:
                        s = depth + 1 + p if dz == 1 else 0
                    z = p if dz == 1 else depth - 1
                    row = slice(z * height + y, z * height + y + 1)
                    add_columns(level, [(row, tuple(x[s:s + 1] for x in parts))])

    for z in range(8):
        for t in range(4):
            out1[z, :, LANES * t:LANES * t + LANES] = l1[t, 32 * z:32 * z + 32, :]
    for z in range(4):
        for t in range(2):
            out2[z, :, LANES * t:LANES * t + LANES] = l2[t, 16 * z:16 * z + 16, :]
    for z in range(2):
        out3[z, :, :] = l3[0, 8 * z:8 * z + 8, :]

    for_neighbours(sent)


def store(in1, in2, in3, out1, out2, out3, sem):
    copies = [
        pltpu.make_async_copy(source, target, sem.at[i])
        for i, (source, target) in enumerate(((in1, out1), (in2, out2), (in3, out3)))
    ]
    for copy in copies:
        copy.start()
    for copy in copies:
        copy.wait()


def on_device(counts, volume):
    shapes = tuple(jax.ShapeDtypeStruct(s, F32) for s in ((8, 32, 512), (4, 16, 256), (2, 8, 128)))
    levels = levels_of(counts, shapes, volume)
    return pl.pallas_call(
        store,
        out_shape=shapes,
        in_specs=[pl.BlockSpec(memory_space=pltpu.VMEM)] * 3,
        out_specs=[pl.BlockSpec(memory_space=pltpu.HBM)] * 3,
        scratch_shapes=[pltpu.SemaphoreType.DMA((3,))],
        compiler_params=pltpu.CompilerParams(vmem_limit_bytes=52 * 1024 * 1024),
        name="store",
    )(*levels)


def levels_of(counts, shapes, volume):
    vmem = lambda *shape: pltpu.VMEM(shape, F32)
    return pl.pallas_call(
        functools.partial(pyramid, counts),
        out_shape=shapes,
        in_specs=[pl.BlockSpec(memory_space=pltpu.HBM)],
        out_specs=[pl.BlockSpec(memory_space=pltpu.VMEM)] * 3,
        scratch_shapes=[
            vmem(16, 64, 1024),
            vmem(8, 10 * PITCH1 + 8, LANES), vmem(8, ROWS1, LANES), vmem(4, ROWS1, 256), vmem(5, ROWS1, LANES),
            vmem(5, 2, 24, LANES), vmem(5, 8 * PITCH2, LANES), vmem(5, ROWS2, LANES), vmem(3, ROWS2, 256),
            vmem(3, ROWS2, LANES),
            vmem(3, 3, 24, LANES), vmem(3, 8 * PITCH3, LANES), vmem(3, ROWS3, LANES), vmem(2, ROWS3, 256),
            vmem(2, ROWS3, LANES),
            pltpu.VMEM((256, 256), BF16), pltpu.VMEM((128, 256), BF16),
            vmem(2, 8, LANES), vmem(2, 3, 8, LANES), vmem(4, 16, LANES),
            vmem(2, 4, 32, LANES), vmem(2, 32, LANES), vmem(2, 16, LANES), vmem(1, 16, LANES), vmem(1, 8, LANES),
            vmem(2, 4, 8, LANES), vmem(2, 3, 8, LANES), vmem(4, 16, LANES),
            vmem(2, 8, LANES), vmem(8, 2, 8, LANES),
            pltpu.SemaphoreType.DMA((4,)),
            pltpu.SemaphoreType.DMA((26, 3)),
            pltpu.SemaphoreType.DMA((26, 3)),
            pltpu.SemaphoreType.REGULAR((2,)),
        ],
        compiler_params=pltpu.CompilerParams(
            collective_id=0, has_side_effects=True, vmem_limit_bytes=52 * 1024 * 1024
        ),
        name="pyramid",
    )(volume)


def solution(mesh):
    spec = P("gz", "gy", "gx")
    return jax.shard_map(
        functools.partial(on_device, dict(mesh.shape)),
        mesh=mesh,
        in_specs=(spec,),
        out_specs=(spec, spec, spec),
        check_vma=False,
    )
```

```python
import functools

import jax
import jax.numpy as jnp
from jax import lax
from jax.experimental import pallas as pl
from jax.experimental.pallas import tpu as pltpu
from jax.sharding import PartitionSpec as P

MESH = pl.DeviceIdType.MESH
F32 = jnp.float32
BF16 = jnp.bfloat16
LANES = 128
taps = (1.0, 4.0, 6.0, 4.0, 1.0)

ROWS1, ROWS2, ROWS3 = 352, 144, 64
PITCH1, PITCH2, PITCH3 = 72, 48, 32
DIRECTIONS = [
    (dz, dy, dx)
    for dx in (-1, 1, 0)
    for dz in (1, -1, 0)
    for dy in (-1, 1, 0)
    if (dz, dy, dx) != (0, 0, 0)
]
SLOT = {d: i for i, d in enumerate(DIRECTIONS)}
SIDES = [(dz, dy) for dz in (1, -1, 0) for dy in (1, -1, 0) if (dz, dy) != (0, 0)]
SIDE = {d: i for i, d in enumerate(SIDES)}
UPPER = [d for d in DIRECTIONS if (d[2], d[1], d[0]) > (0, 0, 0)]
LOWER = [d for d in DIRECTIONS if (d[2], d[1], d[0]) < (0, 0, 0)]
FACES = [(1, 0, 0), (-1, 0, 0), (0, 1, 0), (0, -1, 0)]
GROUP = {0: (0, 0), 3: (0, 1), 1: (1, 0), 2: (1, 1)}
CORNER = {(1, 1): 0, (1, -1): 1, (-1, 1): 2, (-1, -1): 3}


def weighted(pieces):
    groups = {}
    for k, piece in pieces.items():
        groups.setdefault(taps[k], []).append(piece)
    total = None
    for tap, members in groups.items():
        part = members[0] if len(members) == 1 else members[0] + members[1]
        part = part if tap == 1.0 else tap * part
        total = part if total is None else total + part
    return total


def reduce_planes(load, low, high, out):
    return weighted(
        {k: load(2 * out + k - 2) for k in range(5) if low <= 2 * out + k - 2 <= high}
    )


def split(block):
    first = block.astype(BF16)
    rest = block - first.astype(F32)
    second = rest.astype(BF16)
    third = (rest - second.astype(F32)).astype(BF16)
    return third, second, first


def product(block, weights):
    total = None
    for piece in split(block):
        part = jnp.dot(piece, weights, preferred_element_type=F32)
        total = part if total is None else total + part
    return total


def build_weights(band, edge):
    k = lax.broadcasted_iota(jnp.int32, (256, 256), 0)
    n = lax.broadcasted_iota(jnp.int32, (256, 256), 1)
    out = jnp.where(n < 128, n, jnp.where(n == 128, 128, jnp.where(n == 255, -1, 1000)))
    tap = k - 2 * out + 2
    value = jnp.where(tap == 2, 6.0, jnp.where((tap == 1) | (tap == 3), 4.0, jnp.where((tap == 0) | (tap == 4), 1.0, 0.0)))
    band[...] = (value * (1.0 / 4096.0)).astype(BF16)
    k = lax.broadcasted_iota(jnp.int32, (128, 256), 0)
    n = lax.broadcasted_iota(jnp.int32, (128, 256), 1)
    place = jnp.where(k < 2, k, jnp.where(k == 127, -1, 1000))
    out = jnp.where(n < 2, n, jnp.where(n == 127, -1, jnp.where(n == 255, -1, jnp.where(n == 128, 0, -1000))))
    high_in, low_in = k < 2, k == 127
    high_out = (n < 2) | (n == 255)
    low_out = (n == 127) | (n == 128)
    tap = place - 2 * out + 2
    legal = (high_in & high_out) | (low_in & low_out)
    value = jnp.where(tap == 2, 6.0, jnp.where((tap == 1) | (tap == 3), 4.0, jnp.where((tap == 0) | (tap == 4), 1.0, 0.0)))
    edge[...] = jnp.where(legal, value * (1.0 / 4096.0), 0.0).astype(BF16)


def build_end_weights(ends1, ends2, ends3):
    tap1 = [6, 4, 1]
    tap2 = [44, 40, 31, 20, 10, 4, 1]
    tap3 = [344, 336, 315, 284, 246, 204, 161, 120, 84, 56, 35, 20, 10, 4, 1]
    k = lax.broadcasted_iota(jnp.int32, (32, LANES), 0) - 16
    lane = lax.broadcasted_iota(jnp.int32, (32, LANES), 1)
    zero = jnp.zeros((112, LANES), BF16)

    def fill(ref, value):
        ref[0:112, :] = zero
        ref[112:144, :] = value.astype(BF16)
        ref[144:256, :] = zero

    for level, taps_of in enumerate((tap1, tap2, tap3)):
        step = 2 << level
        high = jnp.where((k < 0) & (lane < 2), step * lane - k, 99)
        distance = jnp.where((k >= 0) & (lane == 127), k + step, high)
        scale = 1.0 / 4096.0 ** (level + 1)
        value = jnp.zeros((32, LANES), F32)
        for offset, tap in enumerate(taps_of):
            value = jnp.where(distance == offset, (316 if tap == 315 else tap) * scale, value)
        if level == 0:
            fill(ends1, value)
        elif level == 1:
            fill(ends2, value)
        else:
            fill(ends3.at[0], value)
            fill(ends3.at[1], jnp.where(distance == 2, -scale, 0.0))


def pyramid(counts, vol, out1, out2, out3, v, zs1, as1, cut1, p1, l1, ye1, zs2, as2, p2, l2, ye2, zs3, as3, p3, l3,
            band, edge, ends1, ends2, ends3, x1, x2, x3, xp, yf, q, rz1, rz2u, rz2d, rz3u, rz3d, ry1, ryf, rq, rx, rr,
            load_sem, send_sem, recv_sem, ready):
    me = {axis: lax.axis_index(axis) for axis in ("gz", "gy", "gx")}
    has = {(axis, 1): me[axis] < counts[axis] - 1 for axis in me}
    has.update({(axis, -1): me[axis] > 0 for axis in me})

    def exists(d):
        ok = None
        for axis, step in zip(("gz", "gy", "gx"), d):
            if step:
                ok = has[axis, step] if ok is None else ok & has[axis, step]
        return ok

    def device(d):
        return {axis: me[axis] + step for axis, step in zip(("gz", "gy", "gx"), d) if step}

    def blank(d):
        dz, dy, dx = d
        zeros = jnp.zeros((8, LANES), F32)
        if dx:
            column = 0 if dx == 1 else 1
            target = rr.at[SIDE[dz, dy], column] if dz or dy else rx.at[column]
            target[...] = zeros
            return
        side = 0 if dy == 1 else 1
        if dz and dy:
            targets = [rq.at[CORNER[dz, dy]]]
        elif dy:
            targets = [ry1.at[side, t] for t in range(4)] + [ryf.at[side, t] for t in range(3)]
        elif dz == 1:
            targets = [rz1.at[0, t] for t in range(4)] + [rz2u.at[t] for t in range(2)] + [rz3u.at[0]]
        else:
            targets = [rz1.at[1, t] for t in range(4)] + [rz2d.at[t] for t in range(2)] + [rz3d.at[0]]
        for target in targets:
            for r in range(0, target.shape[0], 8):
                target[r:r + 8, :] = zeros

    pieces = ((0, 1), (7, 1), (1, 1), (6, 1), (2, 2), (4, 2))
    loads = [
        pltpu.make_async_copy(
            vol.at[:, :, pl.ds(LANES * c, LANES * n)], v.at[:, :, pl.ds(LANES * c, LANES * n)], load_sem.at[i]
        )
        for i, (c, n) in enumerate(pieces)
    ]
    for load in loads:
        load.start()

    barrier = pltpu.get_barrier_semaphore()
    interior = functools.reduce(lambda x, y: x & y, has.values())

    def signal(semaphore, d):
        pl.semaphore_signal(semaphore, inc=1, device_id=device(d), device_id_type=MESH)

    @pl.when(interior)
    def _():
        for d in UPPER:
            signal(barrier, d)

    @pl.when(jnp.logical_not(interior))
    def _():
        for d in UPPER:
            @pl.when(exists(d))
            def _():
                signal(barrier, d)

        for d in DIRECTIONS:
            @pl.when(jnp.logical_not(exists(tuple(-k for k in d))))
            def _():
                blank(d)

    build_weights(band, edge)
    build_end_weights(ends1, ends2, ends3)
    zero8 = jnp.zeros((8, LANES), F32)
    for c in range(8):
        for p in range(11):
            zs1[c, p * PITCH1:p * PITCH1 + 8, :] = zero8
        as1[c, 328:336, :] = zero8
        as1[c, 344:352, :] = zero8
    for c in range(4):
        q[c, 0:8, :] = zero8
        q[c, 8:16, :] = zero8
    for side in range(2):
        for t in range(3):
            yf[side, t] = zero8
    for t in range(7):
        for e in range(2):
            for r in range(0, 24, 8):
                ye1[t, e, r:r + 8, :] = zero8
        for p in range(8):
            zs2[t, p * PITCH2:p * PITCH2 + 8, :] = zero8
            zs2[t, p * PITCH2 + 40:p * PITCH2 + 48, :] = zero8
        for r in range(8, 40, 8):
            zs2[t, 7 * PITCH2 + r:7 * PITCH2 + r + 8, :] = zero8
        as2[t, 136:144, :] = zero8
    for t in range(5):
        for e in range(3):
            for r in range(0, 24, 8):
                ye2[t, e, r:r + 8, :] = zero8
        for p in range(8):
            zs3[t, p * PITCH3:p * PITCH3 + 8, :] = zero8
            zs3[t, p * PITCH3 + 24:p * PITCH3 + 32, :] = zero8
        for p in range(5, 8):
            for r in (8, 16):
                zs3[t, p * PITCH3 + r:p * PITCH3 + r + 8, :] = zero8

    flag = {key: jnp.where(value, 1.0, 0.0).astype(F32) for key, value in has.items()}
    zlo, zhi = flag["gz", -1], flag["gz", 1]
    ylo, yhi = flag["gy", -1], flag["gy", 1]
    lane = lax.broadcasted_iota(jnp.int32, (8, LANES), 1)
    sub = lax.broadcasted_iota(jnp.int32, (8, LANES), 0)
    xflag = jnp.where(lane < 64, flag["gx", 1], flag["gx", -1])

    def transfers(d):
        dz, dy, dx = d
        if dx:
            column = 0 if dx == 1 else 1
            if dz == 0 and dy == 0:
                return {2: (xp.at[0], rx.at[column])}
            return {2: (xp.at[1], rr.at[SIDE[dz, dy], column])}
        if dy == 0:
            if dz == 1:
                return {
                    0: (l1.at[pl.ds(0, 4), pl.ds(288, 32), :], rz1.at[0]),
                    1: (l2.at[pl.ds(0, 2), pl.ds(80, 32), :], rz2u),
                    2: (l3.at[pl.ds(0, 1), pl.ds(24, 16), :], rz3u),
                }
            return {
                0: (l1.at[pl.ds(0, 4), pl.ds(256, 32), :], rz1.at[1]),
                1: (l2.at[pl.ds(0, 2), pl.ds(64, 16), :], rz2d),
                2: (l3.at[pl.ds(0, 1), pl.ds(16, 8), :], rz3d),
            }
        if dz == 0:
            side = 0 if dy == 1 else 1
            return {
                0: (l1.at[pl.ds(0, 4), pl.ds(336 if dy == 1 else 320, 8), :], ry1.at[side]),
                2: (yf.at[side], ryf.at[side]),
            }
        corner = CORNER[dz, dy]
        return {2: (q.at[corner], rq.at[corner])}

    def copies(d, stages=(0, 1, 2)):
        return [
            pltpu.make_async_remote_copy(
                src_ref=pair[0],
                dst_ref=pair[1],
                send_sem=send_sem.at[SLOT[d], i],
                recv_sem=recv_sem.at[SLOT[d], i],
                device_id=device(d),
                device_id_type=MESH,
            )
            for i, pair in transfers(d).items()
            if i in stages
        ]

    def for_neighbours(act, stages=(0, 1, 2), back=False, only=None):
        chosen = [d for d in (only or DIRECTIONS) if any(i in stages for i in transfers(d))]

        @pl.when(interior)
        def _():
            for d in chosen:
                for copy in copies(d, stages):
                    act(copy)

        @pl.when(jnp.logical_not(interior))
        def _():
            for d in chosen:
                @pl.when(exists(tuple(-k for k in d) if back else d))
                def _():
                    for copy in copies(d, stages):
                        act(copy)

    start, received, sent = (lambda c: c.start()), (lambda c: c.wait_recv()), (lambda c: c.wait_send())

    zflag2 = jnp.where(sub == 0, zlo, jnp.where(sub < 5, 1.0, zhi))
    plane_row1 = lambda s: 256 if s == -1 else (288 if s == 8 else 32 * s)
    plane_row2 = lambda s: 64 if s == -1 else (80 + 16 * (s - 4) if s >= 4 else 16 * s)
    plane_row3 = lambda s: 16 if s == -1 else (24 + 8 * (s - 2) if s >= 2 else 8 * s)
    zscale2 = lambda i: zlo if i == -1 else (zhi if i >= 4 else None)

    def cut(c, row, block):
        group, place = GROUP[c // 2]
        at = place * ROWS1 + row
        for piece, value in enumerate(split(block)):
            cut1[group, piece, at:at + block.shape[0], LANES * (c % 2):LANES * (c % 2) + LANES] = value

    def level_one_tiles(c, n):
        for r in range(0, 64, 8):
            planes = [v[s, r:r + 8, LANES * c:LANES * (c + n)] for s in range(16)]
            for i in range(-1, 9):
                plane = reduce_planes(lambda s: planes[s], 0, 15, i)
                row = (i + 1) * PITCH1 + 8 + r
                for h in range(n):
                    zs1[c + h, row:row + 8, :] = plane[:, LANES * h:LANES * h + LANES]
        for c in range(c, c + n):
            for i in range(-1, 9):
                base = (i + 1) * PITCH1 + 8
                plane = weighted({k: zs1[c, pl.ds(base + k - 2, 32, stride=2), :] for k in range(5)})
                if i == -1:
                    plane = plane * zlo
                elif i == 8:
                    plane = plane * zhi
                row = plane_row1(i)
                if c in (0, 7):
                    as1[c, row:row + 32, :] = plane
                cut(c, row, plane)

            def column(y, p, size):
                return zs1[c, pl.ds(p * PITCH1 + 8 + y, size, stride=PITCH1), :]

            as1[c, 320:328, :] = column(0, 1, 8) * ylo
            as1[c, 336:344, :] = weighted({0: column(62, 1, 8), 1: column(63, 1, 8)}) * yhi
            for s, p, zflag in ((0, 0, zlo), (1, 9, zhi)):
                first = p * PITCH1 + 8
                as1[c, 328 + s:329 + s, :] = zs1[c, first:first + 1, :] * (ylo * zflag)
                as1[c, 344 + s:345 + s, :] = weighted(
                    {0: zs1[c, first + 62:first + 63, :], 1: zs1[c, first + 63:first + 64, :]}
                ) * (yhi * zflag)
            cut(c, 320, as1[c, 320:352, :])

    def level_one_product(blocks):
        group = GROUP[blocks[0]][0]
        total = None
        for piece in range(3):
            part = jnp.dot(cut1[group, piece], band[...], preferred_element_type=F32)
            total = part if total is None else total + part
        for b in blocks:
            at = GROUP[b][1] * ROWS1
            p1[b] = total[at:at + ROWS1]

    def level_two_tile(source, t):
        for e, first in ((0, 320), (1, 336)):
            ye1[t, e, 8:16, :] = source[first:first + 8, :]
            ye1[t, e, 7:8, :] = source[first + 8:first + 9, :]
            ye1[t, e, 16:17, :] = source[first + 9:first + 10, :]
        for i in range(-1, 6):
            plane = reduce_planes(lambda s: source[plane_row1(s):plane_row1(s) + 32, :], -1, 8, i)
            if zscale2(i) is not None:
                plane = plane * zscale2(i)
            row = (i + 1) * PITCH2 + 8
            zs2[t, row:row + 32, :] = plane
        for e, y in ((0, -1), (1, 32)):
            block = weighted({k: ye1[t, e, pl.ds(4 + k, 8, stride=2), :] for k in range(5)})
            zs2[t, pl.ds(8 + y, 8, stride=PITCH2), :] = block * zflag2
        for i in range(-1, 6):
            base = (i + 1) * PITCH2 + 8
            row = plane_row2(i)
            as2[t, row:row + 16, :] = weighted(
                {k: zs2[t, pl.ds(base + k - 2, 16, stride=2), :] for k in range(5)}
            )

        def column2(y):
            return zs2[t, pl.ds(8 + y, 8, stride=PITCH2), :]

        as2[t, 112:120, :] = weighted({3: column2(-1), 4: column2(0)}) * ylo
        as2[t, 120:128, :] = weighted({0: column2(30), 1: column2(31), 2: column2(32)}) * yhi
        as2[t, 128:136, :] = column2(32) * yhi

    def level_three_tile(source, t):
        for e, first in ((0, 112), (1, 120), (2, 128)):
            ye2[t, e, 7:15, :] = source[first:first + 8, :]
        for i in range(-1, 4):
            row = (i + 1) * PITCH3 + 8
            zs3[t, row:row + 16, :] = reduce_planes(
                lambda s: source[plane_row2(s):plane_row2(s) + 16, :], -1, 5, i
            )
        for e, y in ((0, -1), (1, 16), (2, 17)):
            block = weighted({k: ye2[t, e, pl.ds(4 + k, 8, stride=2), :] for k in range(5)})
            zs3[t, pl.ds(8 + y, 8, stride=PITCH3), :] = block
        for i in range(-1, 4):
            base = (i + 1) * PITCH3 + 8
            row = plane_row3(i)
            as3[t, row:row + 8, :] = weighted(
                {k: zs3[t, pl.ds(base + k - 2, 8, stride=2), :] for k in range(5)}
            )

        def column3(y):
            return zs3[t, pl.ds(8 + y, 8, stride=PITCH3), :]

        as3[t, 40:48, :] = weighted({3: column3(-1), 4: column3(0)})
        as3[t, 48:56, :] = weighted({k: column3(14 + k) for k in range(4)})
        as3[t, 56:64, :] = weighted({0: column3(16), 1: column3(17)})

    def combine(parts, result, tiles, rows, mask):
        size = 16
        low = lax.broadcasted_iota(jnp.int32, (size, LANES), 1) < 64
        wide = None if mask is None else jnp.broadcast_to(mask[0:1], (size, LANES))
        total = tiles + 1
        for r in range(0, rows, size):
            over = [parts(t, r, size, 1) for t in range(total)]
            for t in range(total):
                before, after = over[(t - 1) % total], over[(t + 1) % total]
                if before is None:
                    spill = jnp.where(low, 0.0, after)
                elif after is None:
                    spill = jnp.where(low, before, 0.0)
                else:
                    spill = jnp.where(low, before, after)
                main = parts(t, r, size, 0)
                value = spill if main is None else main + spill
                if t == tiles and wide is not None:
                    value = value * wide
                result[t, r:r + size, :] = value

    main_groups = [(l1, 4, 8 * g) for g in range(32)] + [(l2, 2, 8 * g) for g in range(8)] + [(l3, 1, 8 * g) for g in range(2)]
    main_rows = [(x1, 8 * g) for g in range(32)] + [(x2, 8 * g) for g in range(8)] + [(x3, 8 * g) for g in range(2)]
    side_rows = (
        [(x1, 256 + 8 * g) for g in range(12)] + [(x2, 64 + 8 * g) for g in range(9)] + [(x3, 16 + 8 * g) for g in range(6)]
    )

    def pack(groups):
        total = None
        for g, (ref, row) in enumerate(groups):
            piece = ref[row:row + 8, :]
            piece = piece if g == 0 else pltpu.roll(piece, 3 * g, 1)
            total = piece if total is None else total + piece
        return total

    def ends(source, high, low):
        return jnp.concatenate([source[high], source[low]], axis=1)

    for i in range(2):
        loads[i].wait()
        level_one_tiles(*pieces[i])
    for i in range(2, 4):
        loads[i].wait()
    level_one_tiles(*pieces[2])
    level_one_tiles(*pieces[3])
    level_one_product((0, 3))
    level_two_tile(as1.at[0], 5)
    level_two_tile(as1.at[7], 6)
    level_three_tile(as2.at[5], 3)
    level_three_tile(as2.at[6], 4)
    x1[...] = product(ends(as1, 7, 0), ends1[...])
    x2[...] = product(ends(as2, 6, 5), ends2[...])
    block = ends(as3, 4, 3)
    x3[...] = product(block, ends3[0]) + product(block, ends3[1])
    xp[0] = pack(main_rows)
    xp[1] = pack(side_rows)
    one = {key: value.astype(jnp.int32) for key, value in has.items()}
    across_z = 1 + one["gz", 1] + one["gz", -1]
    across = across_z * (1 + one["gy", 1] + one["gy", -1])
    near_lower, near_upper = (one["gy", k] * across_z + one["gz", k] for k in (-1, 1))
    far_lower, far_upper = (one["gx", k] * across for k in (-1, 1))

    def wait_for(semaphore, number):
        @pl.when(number > 0)
        def _():
            pl.semaphore_wait(semaphore, number)

    def answer(d):
        signal(ready.at[1 if d[2] else 0], d)


    def enter():
        wait_for(barrier, near_lower + far_lower)

        @pl.when(interior)
        def _():
            for d in LOWER:
                answer(d)

        @pl.when(jnp.logical_not(interior))
        def _():
            for d in LOWER:
                @pl.when(exists(d))
                def _():
                    answer(d)

    last_column = jnp.logical_not(has["gx", 1])

    @pl.when(jnp.logical_not(last_column))
    def _():
        enter()
        for_neighbours(start, (2,), only=[d for d in LOWER if d[2]])

    for i in range(4, 6):
        loads[i].wait()
    level_one_tiles(*pieces[4])
    @pl.when(last_column)
    def _():
        enter()
        for_neighbours(start, (2,), only=[d for d in LOWER if d[2]])

    level_one_tiles(*pieces[5])
    level_one_product((1, 2))

    def parts1(t, r, size, half):
        return None if t == 4 else p1[t, r:r + size, 128 * half:128 * half + 128]

    combine(parts1, l1, 4, ROWS1, xflag)
    for_neighbours(start, (0,), only=LOWER)
    for t in range(5):
        level_two_tile(l1.at[t], t)
    for b in range(2):
        block = jnp.concatenate([as2[2 * b], as2[2 * b + 1]], axis=1)
        p2[b] = product(block, band[...])
    p2[2] = product(as2[4], edge[...])

    def parts2(t, r, size, half):
        return p2[t, r:r + size, 128 * half:128 * half + 128]

    combine(parts2, l2, 2, ROWS2, xflag)
    for_neighbours(start, (1,), only=LOWER)

    for t in range(3):
        level_three_tile(l2.at[t], t)
    p3[0] = product(jnp.concatenate([as3[0], as3[1]], axis=1), band[...])
    p3[1] = product(as3[2], edge[...])

    def parts3(t, r, size, half):
        return p3[t, r:r + size, 128 * half:128 * half + 128]

    combine(parts3, l3, 1, ROWS3, None)

    for side, blocks2, blocks3 in ((0, (120, 128), (48, 56)), (1, (112,), (40,))):
        for t in range(2):
            for j, row in enumerate(blocks2):
                yf[side, t, 4 * j:4 * j + 4, :] = l2[t, row + 1:row + 5, :]
        for j, row in enumerate(blocks3):
            yf[side, 2, 2 * j:2 * j + 2, :] = l3[0, row + 1:row + 3, :]
        for dz in (1, -1):
            corner = CORNER[dz, 1 - 2 * side]
            row1 = (344 if side == 0 else 328) + (1 if dz == 1 else 0)
            first2, first3, size = (5, 3, 2) if dz == 1 else (0, 0, 1)
            for t in range(4):
                q[corner, t:t + 1, :] = l1[t, row1:row1 + 1, :]
            for t in range(2):
                for j, row in enumerate(blocks2):
                    to = 8 + 4 * t + 2 * j
                    q[corner, to:to + size, :] = l2[t, row + first2:row + first2 + size, :]
            for j, row in enumerate(blocks3):
                q[corner, 4 + 2 * j:4 + 2 * j + size, :] = l3[0, row + first3:row + first3 + size, :]


    for_neighbours(start, (2,), only=[d for d in LOWER if not d[2]])
    wait_for(ready.at[0], near_upper)
    for_neighbours(start, only=[d for d in UPPER if d[2] == 0])
    wait_for(ready.at[1], far_upper)
    for_neighbours(start, only=[d for d in UPPER if d[2]])

    heights, depths = (32, 16, 8), (8, 4, 2)
    levels = (l1, l2, l3)

    def add(level, t, rows, value):
        ref = levels[level]
        ref[t, rows, :] = ref[t, rows, :] + value

    def add_y(dy, level, t, get):
        height, depth = heights[level], depths[level]
        for j in range(2 if dy == 1 and level else 1):
            add(level, t, pl.ds(j if dy == 1 else height - 1, depth, stride=height), get(j))

    def add_z(dz, level, t, get):
        height, depth = heights[level], depths[level]
        planes = 2 if dz == 1 and level else 1
        to = 0 if dz == 1 else (depth - 1) * height
        for r in range(0, planes * height, 8):
            add(level, t, slice(to + r, to + r + 8), get(r))

    def add_corner(dz, dy, level, t, get):
        height, depth = heights[level], depths[level]
        planes = 2 if dz == 1 and level else 1
        for j in range(2 if dy == 1 and level else 1):
            value = get(j)
            for p in range(planes):
                row = (p if dz == 1 else depth - 1) * height + (j if dy == 1 else height - 1)
                add(level, t, slice(row, row + 1), value[p:p + 1])

    for_neighbours(received, (0, 1, 2), back=True, only=[d for d in DIRECTIONS if d[1] and not d[2]])
    for dy in (1, -1):
        side = 0 if dy == 1 else 1
        for t in range(4):
            add_y(dy, 0, t, lambda j: ry1[side, t])
        for t in range(2):
            add_y(dy, 1, t, lambda j: ryf[side, t, 4 * j:4 * j + 4, :])
        add_y(dy, 2, 0, lambda j: ryf[side, 2, 2 * j:2 * j + 2, :])
        for dz in (1, -1):
            c = CORNER[dz, dy]
            for t in range(4):
                add_corner(dz, dy, 0, t, lambda j: rq[c, t:t + 1, :])
            for t in range(2):
                add_corner(dz, dy, 1, t, lambda j: rq[c, 8 + 4 * t + 2 * j:10 + 4 * t + 2 * j, :])
            add_corner(dz, dy, 2, 0, lambda j: rq[c, 4 + 2 * j:6 + 2 * j, :])
    for_neighbours(received, (0, 1, 2), back=True, only=FACES[:2])
    for t in range(4):
        add_z(1, 0, t, lambda r: rz1[0, t, r:r + 8, :])
        add_z(-1, 0, t, lambda r: rz1[1, t, r:r + 8, :])
    for t in range(2):
        add_z(1, 1, t, lambda r: rz2u[t, r:r + 8, :])
        add_z(-1, 1, t, lambda r: rz2d[t, r:r + 8, :])
    add_z(1, 2, 0, lambda r: rz3u[0, r:r + 8, :])
    add_z(-1, 2, 0, lambda r: rz3d[0, r:r + 8, :])
    for_neighbours(sent)
    for_neighbours(received, back=True, only=[d for d in DIRECTIONS if d[2]])
    third = lax.rem(lane, 3)
    low_lanes, high_lane = lane < 2, lane == 127

    def both(low_side, high_side):
        return jnp.where((third == 2) | high_lane, high_side, low_side)

    def spread(value, g):
        moved = value if g == 0 else pltpu.roll(value, LANES - 3 * g, 1)
        return jnp.where(low_lanes, moved, 0.0), jnp.where(high_lane, moved, 0.0)

    def add_columns(level, pairs):
        last = (3, 1, 0)[level]
        for rows, (low_value, high_value) in pairs:
            if last == 0:
                add(level, 0, rows, low_value + high_value)
            else:
                add(level, 0, rows, low_value)
                add(level, last, rows, high_value)

    value = both(rx[0], rx[1])
    for g, (ref, _, row) in enumerate(main_groups):
        level = 0 if g < 32 else (1 if g < 40 else 2)
        add_columns(level, [(slice(row, row + 8), spread(value, g))])
    firsts = {0: 0, 1: 12, 2: 21}
    for dz, dy in SIDES:
        value = both(rr[SIDE[dz, dy], 0], rr[SIDE[dz, dy], 1])
        for level in range(3):
            height, depth = heights[level], depths[level]
            if dy == 0:
                first = firsts[level] + (height // 8 if dz == 1 else 0)
                planes = 2 if dz == 1 and level else 1
                to = 0 if dz == 1 else (depth - 1) * height
                for r in range(planes * height // 8):
                    add_columns(level, [(slice(to + 8 * r, to + 8 * r + 8), spread(value, first + r))])
                continue
            for j in range(2 if dy == 1 and level else 1):
                y = j if dy == 1 else height - 1
                if level == 0:
                    group = (10 if dy == 1 else 8) + (1 if dz else 0)
                else:
                    group = {1: (18, 19), 2: (24, 25)}[level][1 if dy == 1 else 0] + j
                parts = spread(value, group)
                if dz == 0:
                    if level:
                        parts = tuple(x[1:1 + depth] for x in parts)
                    add_columns(level, [(pl.ds(y, depth, stride=height), parts)])
                    continue
                for p in range(2 if dz == 1 and level else 1):
                    if level == 0:
                        s = 1 if dz == 1 else 0
                    else:
                        s = depth + 1 + p if dz == 1 else 0
                    z = p if dz == 1 else depth - 1
                    row = slice(z * height + y, z * height + y + 1)
                    add_columns(level, [(row, tuple(x[s:s + 1] for x in parts))])

    for z in range(8):
        for t in range(4):
            out1[z, :, LANES * t:LANES * t + LANES] = l1[t, 32 * z:32 * z + 32, :]
    for z in range(4):
        for t in range(2):
            out2[z, :, LANES * t:LANES * t + LANES] = l2[t, 16 * z:16 * z + 16, :]
    for z in range(2):
        out3[z, :, :] = l3[0, 8 * z:8 * z + 8, :]


def store(in1, in2, in3, out1, out2, out3, sem):
    copies = [
        pltpu.make_async_copy(source, target, sem.at[i])
        for i, (source, target) in enumerate(((in1, out1), (in2, out2), (in3, out3)))
    ]
    for copy in copies:
        copy.start()
    for copy in copies:
        copy.wait()


def on_device(counts, volume):
    shapes = tuple(jax.ShapeDtypeStruct(s, F32) for s in ((8, 32, 512), (4, 16, 256), (2, 8, 128)))
    levels = levels_of(counts, shapes, volume)
    return pl.pallas_call(
        store,
        out_shape=shapes,
        in_specs=[pl.BlockSpec(memory_space=pltpu.VMEM)] * 3,
        out_specs=[pl.BlockSpec(memory_space=pltpu.HBM)] * 3,
        scratch_shapes=[pltpu.SemaphoreType.DMA((3,))],
        compiler_params=pltpu.CompilerParams(vmem_limit_bytes=52 * 1024 * 1024),
        name="store",
    )(*levels)


def levels_of(counts, shapes, volume):
    vmem = lambda *shape: pltpu.VMEM(shape, F32)
    return pl.pallas_call(
        functools.partial(pyramid, counts),
        out_shape=shapes,
        in_specs=[pl.BlockSpec(memory_space=pltpu.HBM)],
        out_specs=[pl.BlockSpec(memory_space=pltpu.VMEM)] * 3,
        scratch_shapes=[
            vmem(16, 64, 1024),
            vmem(8, 10 * PITCH1 + 8, LANES), vmem(8, ROWS1, LANES),
            pltpu.VMEM((2, 3, 2 * ROWS1, 256), BF16), vmem(4, ROWS1, 256), vmem(5, ROWS1, LANES),
            vmem(7, 2, 24, LANES), vmem(7, 8 * PITCH2, LANES), vmem(7, ROWS2, LANES), vmem(3, ROWS2, 256),
            vmem(3, ROWS2, LANES),
            vmem(5, 3, 24, LANES), vmem(5, 8 * PITCH3, LANES), vmem(5, ROWS3, LANES), vmem(2, ROWS3, 256),
            vmem(2, ROWS3, LANES),
            pltpu.VMEM((256, 256), BF16), pltpu.VMEM((128, 256), BF16),
            pltpu.VMEM((256, LANES), BF16), pltpu.VMEM((256, LANES), BF16), pltpu.VMEM((2, 256, LANES), BF16),
            vmem(ROWS1, LANES), vmem(ROWS2, LANES), vmem(ROWS3, LANES),
            vmem(2, 8, LANES), vmem(2, 3, 8, LANES), vmem(4, 16, LANES),
            vmem(2, 4, 32, LANES), vmem(2, 32, LANES), vmem(2, 16, LANES), vmem(1, 16, LANES), vmem(1, 8, LANES),
            vmem(2, 4, 8, LANES), vmem(2, 3, 8, LANES), vmem(4, 16, LANES),
            vmem(2, 8, LANES), vmem(8, 2, 8, LANES),
            pltpu.SemaphoreType.DMA((6,)),
            pltpu.SemaphoreType.DMA((26, 3)),
            pltpu.SemaphoreType.DMA((26, 3)),
            pltpu.SemaphoreType.REGULAR((2,)),
        ],
        compiler_params=pltpu.CompilerParams(
            collective_id=0, has_side_effects=True, vmem_limit_bytes=52 * 1024 * 1024
        ),
        name="pyramid",
    )(volume)


def solution(mesh):
    spec = P("gz", "gy", "gx")
    return jax.shard_map(
        functools.partial(on_device, dict(mesh.shape)),
        mesh=mesh,
        in_specs=(spec,),
        out_specs=(spec, spec, spec),
        check_vma=False,
    )
```

```python
import functools
import math

import jax
import jax.numpy as jnp
from jax import lax
from jax.experimental import pallas as pl
from jax.experimental.pallas import tpu as pltpu
from jax.sharding import PartitionSpec as P

MESH = pl.DeviceIdType.MESH
F32 = jnp.float32
BF16 = jnp.bfloat16
LANES = 128
AXES = ("gz", "gy", "gx")
taps = (1.0, 4.0, 6.0, 4.0, 1.0)

ROWS1, ROWS2, ROWS3 = 352, 144, 64
PITCH1, PITCH2, PITCH3 = 72, 48, 32
DIRECTIONS = [
    (dz, dy, dx)
    for dx in (-1, 1, 0)
    for dz in (1, -1, 0)
    for dy in (-1, 1, 0)
    if (dz, dy, dx) != (0, 0, 0)
]
SIDES = [(1, -1), (-1, -1), (0, -1), (-1, 0), (1, 1), (-1, 1), (0, 1), (1, 0)]
SIDE = {d: i for i, d in enumerate(SIDES)}
UPPER = [d for d in DIRECTIONS if (d[2], d[1], d[0]) > (0, 0, 0)]
LOWER = [d for d in DIRECTIONS if (d[2], d[1], d[0]) < (0, 0, 0)]
TARGETS = [d for d in DIRECTIONS if d[2] < 1 or d == (0, 0, 1)]
NEAR_LOWER, NEAR_UPPER = ([d for d in half if not d[2]] for half in (LOWER, UPPER))
FAR_LOWER, NEXT, BEFORE = [d for d in LOWER if d[2]], (0, 0, 1), (0, 0, -1)
FACES = [(1, 0, 0), (-1, 0, 0), (0, 1, 0), (0, -1, 0)]
GROUP = {0: (0, 0), 3: (0, 1), 1: (1, 0), 2: (1, 1)}
CORNER = {(1, 1): 0, (1, -1): 1, (-1, 1): 2, (-1, -1): 3}


def weighted(pieces):
    groups = {}
    for k, piece in pieces.items():
        groups.setdefault(taps[k], []).append(piece)
    total = None
    for tap, members in groups.items():
        part = members[0] if len(members) == 1 else members[0] + members[1]
        part = part if tap == 1.0 else tap * part
        total = part if total is None else total + part
    return total


def reduce_planes(load, low, high, out):
    return weighted(
        {k: load(2 * out + k - 2) for k in range(5) if low <= 2 * out + k - 2 <= high}
    )


def split(block):
    first = block.astype(BF16)
    rest = block - first.astype(F32)
    second = rest.astype(BF16)
    third = (rest - second.astype(F32)).astype(BF16)
    return third, second, first


def product(block, weights):
    total = None
    for piece in split(block):
        part = jnp.dot(piece, weights, preferred_element_type=F32)
        total = part if total is None else total + part
    return total


def build_weights(band, edge):
    k = lax.broadcasted_iota(jnp.int32, (256, 256), 0)
    n = lax.broadcasted_iota(jnp.int32, (256, 256), 1)
    out = jnp.where(n < 128, n, jnp.where(n == 128, 128, jnp.where(n == 255, -1, 1000)))
    tap = k - 2 * out + 2
    value = jnp.where(tap == 2, 6.0, jnp.where((tap == 1) | (tap == 3), 4.0, jnp.where((tap == 0) | (tap == 4), 1.0, 0.0)))
    band[...] = (value * (1.0 / 4096.0)).astype(BF16)
    k = lax.broadcasted_iota(jnp.int32, (128, 256), 0)
    n = lax.broadcasted_iota(jnp.int32, (128, 256), 1)
    place = jnp.where(k < 2, k, jnp.where(k == 127, -1, 1000))
    out = jnp.where(n < 2, n, jnp.where(n == 127, -1, jnp.where(n == 255, -1, jnp.where(n == 128, 0, -1000))))
    high_in, low_in = k < 2, k == 127
    high_out = (n < 2) | (n == 255)
    low_out = (n == 127) | (n == 128)
    tap = place - 2 * out + 2
    legal = (high_in & high_out) | (low_in & low_out)
    value = jnp.where(tap == 2, 6.0, jnp.where((tap == 1) | (tap == 3), 4.0, jnp.where((tap == 0) | (tap == 4), 1.0, 0.0)))
    edge[...] = jnp.where(legal, value * (1.0 / 4096.0), 0.0).astype(BF16)


def build_end_weights(ends1, ends2, ends3):
    tap1 = [6, 4, 1]
    tap2 = [44, 40, 31, 20, 10, 4, 1]
    tap3 = [344, 336, 315, 284, 246, 204, 161, 120, 84, 56, 35, 20, 10, 4, 1]
    k = lax.broadcasted_iota(jnp.int32, (32, LANES), 0) - 16
    lane = lax.broadcasted_iota(jnp.int32, (32, LANES), 1)
    zero = jnp.zeros((112, LANES), BF16)

    def fill(ref, value):
        ref[0:112, :] = zero
        ref[112:144, :] = value.astype(BF16)
        ref[144:256, :] = zero

    for level, taps_of in enumerate((tap1, tap2, tap3)):
        step = 2 << level
        high = jnp.where((k < 0) & (lane < 2), step * lane - k, 99)
        distance = jnp.where((k >= 0) & (lane == 127), k + step, high)
        scale = 1.0 / 4096.0 ** (level + 1)
        value = jnp.zeros((32, LANES), F32)
        for offset, tap in enumerate(taps_of):
            value = jnp.where(distance == offset, (316 if tap == 315 else tap) * scale, value)
        if level == 0:
            fill(ends1, value)
        elif level == 1:
            fill(ends2, value)
        else:
            fill(ends3.at[0], value)
            fill(ends3.at[1], jnp.where(distance == 2, -scale, 0.0))


def pyramid(counts, vol, out1, out2, out3, v, zs1, as1, cut1, p1, l1, ye1, zs2, as2, p2, l2, ye2, zs3, as3, p3, l3,
            band, edge, ends1, ends2, ends3, x1, x2, x3, xp, yf, q, rz1, rz2u, rz2d, rz3u, rz3d, ry1, ryf, rq, rx, ru, rru, rrd,
            load_sem, send_sem, recv_sem, ready):
    me = {axis: lax.axis_index(axis) for axis in ("gz", "gy", "gx")}
    has = {(axis, 1): me[axis] < counts[axis] - 1 for axis in me}
    has.update({(axis, -1): me[axis] > 0 for axis in me})

    def exists(d):
        ok = None
        for axis, step in zip(("gz", "gy", "gx"), d):
            if step:
                ok = has[axis, step] if ok is None else ok & has[axis, step]
        return ok

    def device(d):
        return {axis: me[axis] + step for axis, step in zip(("gz", "gy", "gx"), d) if step}

    def blank(d):
        dz, dy, dx = d
        zeros = jnp.zeros((8, LANES), F32)
        if d == NEXT:
            rx[0] = zeros
            for i in range(8):
                rru[i] = zeros
            return
        if dx:
            target = rrd.at[SIDE[dz, dy]] if dz or dy else rx.at[1]
            target[...] = zeros
            return
        ru[SIDE[dz, dy]] = zeros
        side = 0 if dy == 1 else 1
        if dz and dy:
            targets = [rq.at[CORNER[dz, dy]]]
        elif dy:
            targets = [ry1.at[side, t] for t in range(4)] + [ryf.at[side, t] for t in range(3)]
        elif dz == 1:
            targets = [rz1.at[0, t] for t in range(4)] + [rz2u.at[t] for t in range(2)] + [rz3u.at[0]]
        else:
            targets = [rz1.at[1, t] for t in range(4)] + [rz2d.at[t] for t in range(2)] + [rz3d.at[0]]
        for target in targets:
            for r in range(0, target.shape[0], 8):
                target[r:r + 8, :] = zeros

    pieces = ((0, 1), (7, 1), (1, 1), (6, 1), (2, 2), (4, 2))
    loads = [
        pltpu.make_async_copy(
            vol.at[:, :, pl.ds(LANES * c, LANES * n)], v.at[:, :, pl.ds(LANES * c, LANES * n)], load_sem.at[i]
        )
        for i, (c, n) in enumerate(pieces)
    ]
    for load in loads:
        load.start()

    barrier = pltpu.get_barrier_semaphore()
    interior = functools.reduce(lambda x, y: x & y, has.values())

    def signal(semaphore, d):
        pl.semaphore_signal(semaphore, inc=1, device_id=device(d), device_id_type=MESH)

    @pl.when(interior)
    def _():
        for d in UPPER:
            signal(barrier, d)

    @pl.when(jnp.logical_not(interior))
    def _():
        for d in UPPER:
            @pl.when(exists(d))
            def _():
                signal(barrier, d)

        for d in TARGETS:
            @pl.when(jnp.logical_not(exists(tuple(-k for k in d))))
            def _():
                blank(d)

    build_weights(band, edge)
    build_end_weights(ends1, ends2, ends3)
    zero8 = jnp.zeros((8, LANES), F32)
    for c in range(8):
        for p in range(11):
            zs1[c, p * PITCH1:p * PITCH1 + 8, :] = zero8
        as1[c, 328:336, :] = zero8
        as1[c, 344:352, :] = zero8
    for c in range(4):
        q[c, 0:8, :] = zero8
        q[c, 8:16, :] = zero8
    for side in range(2):
        for t in range(3):
            yf[side, t] = zero8
    for t in range(7):
        for e in range(2):
            for r in range(0, 24, 8):
                ye1[t, e, r:r + 8, :] = zero8
        for p in range(8):
            zs2[t, p * PITCH2:p * PITCH2 + 8, :] = zero8
            zs2[t, p * PITCH2 + 40:p * PITCH2 + 48, :] = zero8
        for r in range(8, 40, 8):
            zs2[t, 7 * PITCH2 + r:7 * PITCH2 + r + 8, :] = zero8
        as2[t, 136:144, :] = zero8
    for t in range(5):
        for e in range(3):
            for r in range(0, 24, 8):
                ye2[t, e, r:r + 8, :] = zero8
        for p in range(8):
            zs3[t, p * PITCH3:p * PITCH3 + 8, :] = zero8
            zs3[t, p * PITCH3 + 24:p * PITCH3 + 32, :] = zero8
        for p in range(5, 8):
            for r in (8, 16):
                zs3[t, p * PITCH3 + r:p * PITCH3 + r + 8, :] = zero8

    flag = {key: jnp.where(value, 1.0, 0.0).astype(F32) for key, value in has.items()}
    zlo, zhi = flag["gz", -1], flag["gz", 1]
    ylo, yhi = flag["gy", -1], flag["gy", 1]
    lane = lax.broadcasted_iota(jnp.int32, (8, LANES), 1)
    sub = lax.broadcasted_iota(jnp.int32, (8, LANES), 0)
    xflag = jnp.where(lane < 64, flag["gx", 1], flag["gx", -1])

    def transfers(d):
        dz, dy, dx = d
        if dx == 1:
            return {
                2: (xp.at[0], rx.at[0]),
                4: (ru.at[pl.ds(0, 4)], rru.at[pl.ds(0, 4)]),
                5: (ru.at[pl.ds(4, 4)], rru.at[pl.ds(4, 4)]),
            }
        if dx == -1:
            return {2: (xp.at[1], rrd.at[SIDE[dz, dy]]) if dz or dy else (xp.at[0], rx.at[1])}
        along = (xp.at[1], ru.at[SIDE[dz, dy]])
        if dy == 0:
            if dz == 1:
                return {
                    0: (l1.at[pl.ds(0, 4), pl.ds(288, 32), :], rz1.at[0]),
                    1: (l2.at[pl.ds(0, 2), pl.ds(80, 32), :], rz2u),
                    2: (l3.at[pl.ds(0, 1), pl.ds(24, 16), :], rz3u),
                    3: along,
                }
            return {
                0: (l1.at[pl.ds(0, 4), pl.ds(256, 32), :], rz1.at[1]),
                1: (l2.at[pl.ds(0, 2), pl.ds(64, 16), :], rz2d),
                2: (l3.at[pl.ds(0, 1), pl.ds(16, 8), :], rz3d),
                3: along,
            }
        if dz == 0:
            side = 0 if dy == 1 else 1
            return {
                0: (l1.at[pl.ds(0, 4), pl.ds(336 if dy == 1 else 320, 8), :], ry1.at[side]),
                2: (yf.at[side], ryf.at[side]),
                3: along,
            }
        corner = CORNER[dz, dy]
        return {2: (q.at[corner], rq.at[corner]), 3: along}

    def awaited_with(d, stage):
        if d[2]:
            return 0
        if stage == 3:
            return 1 if d in NEAR_LOWER else 2
        return 3 if d[1] else 4

    def copies(d, stages=(0, 1, 2, 3, 4, 5)):
        return [
            pltpu.make_async_remote_copy(
                src_ref=pair[0],
                dst_ref=pair[1],
                send_sem=send_sem.at[0 if d[2] or i == 3 else 1],
                recv_sem=recv_sem.at[awaited_with(d, i)],
                device_id=device(d),
                device_id_type=MESH,
            )
            for i, pair in transfers(d).items()
            if i in stages
        ]

    def for_neighbours(act, stages=(0, 1, 2, 3, 4, 5), back=False, only=None):
        chosen = [d for d in (only or TARGETS) if any(i in stages for i in transfers(d))]

        @pl.when(interior)
        def _():
            for d in chosen:
                for copy in copies(d, stages):
                    act(copy)

        @pl.when(jnp.logical_not(interior))
        def _():
            for d in chosen:
                @pl.when(exists(tuple(-k for k in d) if back else d))
                def _():
                    for copy in copies(d, stages):
                        act(copy)

    start = lambda c: c.start()

    def settle(semaphore, only, stages, back):
        parts = []
        for d in only:
            units = sum(
                math.prod(pair[0].shape) // 1024
                for i, pair in transfers(d).items()
                if (i in stages if stages else d[2] or i == 3)
            )
            parts.append((tuple(-k for k in d) if back else d, units))
        axes = [a for j, a in enumerate(AXES) if any(d[j] for d, _ in parts)]

        def wait(state):
            units = sum(u for d, u in parts if all(state[a, k] for a, k in zip(AXES, d) if k))
            if units:
                rows = pl.ds(0, 8 * units)
                pltpu.make_async_copy(zs1.at[0, rows, :], zs1.at[1, rows, :], semaphore).wait()

        def choose(left, state):
            if not left:
                wait(state)
                return
            axis = left[0]
            for low, high in ((True, True), (True, False), (False, True)):
                fits = has[axis, -1] if low else jnp.logical_not(has[axis, -1])
                fits &= has[axis, 1] if high else jnp.logical_not(has[axis, 1])

                @pl.when(fits)
                def _():
                    choose(left[1:], {**state, (axis, -1): low, (axis, 1): high})

        @pl.when(interior)
        def _():
            wait({(a, k): True for a in AXES for k in (-1, 1)})

        @pl.when(jnp.logical_not(interior))
        def _():
            choose(axes, {})

    zflag2 = jnp.where(sub == 0, zlo, jnp.where(sub < 5, 1.0, zhi))
    plane_row1 = lambda s: 256 if s == -1 else (288 if s == 8 else 32 * s)
    plane_row2 = lambda s: 64 if s == -1 else (80 + 16 * (s - 4) if s >= 4 else 16 * s)
    plane_row3 = lambda s: 16 if s == -1 else (24 + 8 * (s - 2) if s >= 2 else 8 * s)
    zscale2 = lambda i: zlo if i == -1 else (zhi if i >= 4 else None)

    def cut(c, row, block):
        group, place = GROUP[c // 2]
        at = place * ROWS1 + row
        for piece, value in enumerate(split(block)):
            cut1[group, piece, at:at + block.shape[0], LANES * (c % 2):LANES * (c % 2) + LANES] = value

    def level_one_tiles(c, n):
        for r in range(0, 64, 8):
            planes = [v[s, r:r + 8, LANES * c:LANES * (c + n)] for s in range(16)]
            for i in range(-1, 9):
                plane = reduce_planes(lambda s: planes[s], 0, 15, i)
                row = (i + 1) * PITCH1 + 8 + r
                for h in range(n):
                    zs1[c + h, row:row + 8, :] = plane[:, LANES * h:LANES * h + LANES]
        for c in range(c, c + n):
            for i in range(-1, 9):
                base = (i + 1) * PITCH1 + 8
                plane = weighted({k: zs1[c, pl.ds(base + k - 2, 32, stride=2), :] for k in range(5)})
                if i == -1:
                    plane = plane * zlo
                elif i == 8:
                    plane = plane * zhi
                row = plane_row1(i)
                if c in (0, 7):
                    as1[c, row:row + 32, :] = plane
                cut(c, row, plane)

            def column(y, p, size):
                return zs1[c, pl.ds(p * PITCH1 + 8 + y, size, stride=PITCH1), :]

            as1[c, 320:328, :] = column(0, 1, 8) * ylo
            as1[c, 336:344, :] = weighted({0: column(62, 1, 8), 1: column(63, 1, 8)}) * yhi
            for s, p, zflag in ((0, 0, zlo), (1, 9, zhi)):
                first = p * PITCH1 + 8
                as1[c, 328 + s:329 + s, :] = zs1[c, first:first + 1, :] * (ylo * zflag)
                as1[c, 344 + s:345 + s, :] = weighted(
                    {0: zs1[c, first + 62:first + 63, :], 1: zs1[c, first + 63:first + 64, :]}
                ) * (yhi * zflag)
            cut(c, 320, as1[c, 320:352, :])

    def level_one_product(blocks):
        group = GROUP[blocks[0]][0]
        total = None
        for piece in range(3):
            part = jnp.dot(cut1[group, piece], band[...], preferred_element_type=F32)
            total = part if total is None else total + part
        for b in blocks:
            at = GROUP[b][1] * ROWS1
            p1[b] = total[at:at + ROWS1]

    def level_two_tile(source, t):
        for e, first in ((0, 320), (1, 336)):
            ye1[t, e, 8:16, :] = source[first:first + 8, :]
            ye1[t, e, 7:8, :] = source[first + 8:first + 9, :]
            ye1[t, e, 16:17, :] = source[first + 9:first + 10, :]
        for i in range(-1, 6):
            plane = reduce_planes(lambda s: source[plane_row1(s):plane_row1(s) + 32, :], -1, 8, i)
            if zscale2(i) is not None:
                plane = plane * zscale2(i)
            row = (i + 1) * PITCH2 + 8
            zs2[t, row:row + 32, :] = plane
        for e, y in ((0, -1), (1, 32)):
            block = weighted({k: ye1[t, e, pl.ds(4 + k, 8, stride=2), :] for k in range(5)})
            zs2[t, pl.ds(8 + y, 8, stride=PITCH2), :] = block * zflag2
        for i in range(-1, 6):
            base = (i + 1) * PITCH2 + 8
            row = plane_row2(i)
            as2[t, row:row + 16, :] = weighted(
                {k: zs2[t, pl.ds(base + k - 2, 16, stride=2), :] for k in range(5)}
            )

        def column2(y):
            return zs2[t, pl.ds(8 + y, 8, stride=PITCH2), :]

        as2[t, 112:120, :] = weighted({3: column2(-1), 4: column2(0)}) * ylo
        as2[t, 120:128, :] = weighted({0: column2(30), 1: column2(31), 2: column2(32)}) * yhi
        as2[t, 128:136, :] = column2(32) * yhi

    def level_three_tile(source, t):
        for e, first in ((0, 112), (1, 120), (2, 128)):
            ye2[t, e, 7:15, :] = source[first:first + 8, :]
        for i in range(-1, 4):
            row = (i + 1) * PITCH3 + 8
            zs3[t, row:row + 16, :] = reduce_planes(
                lambda s: source[plane_row2(s):plane_row2(s) + 16, :], -1, 5, i
            )
        for e, y in ((0, -1), (1, 16), (2, 17)):
            block = weighted({k: ye2[t, e, pl.ds(4 + k, 8, stride=2), :] for k in range(5)})
            zs3[t, pl.ds(8 + y, 8, stride=PITCH3), :] = block
        for i in range(-1, 4):
            base = (i + 1) * PITCH3 + 8
            row = plane_row3(i)
            as3[t, row:row + 8, :] = weighted(
                {k: zs3[t, pl.ds(base + k - 2, 8, stride=2), :] for k in range(5)}
            )

        def column3(y):
            return zs3[t, pl.ds(8 + y, 8, stride=PITCH3), :]

        as3[t, 40:48, :] = weighted({3: column3(-1), 4: column3(0)})
        as3[t, 48:56, :] = weighted({k: column3(14 + k) for k in range(4)})
        as3[t, 56:64, :] = weighted({0: column3(16), 1: column3(17)})

    def combine(parts, result, tiles, rows, mask):
        size = 16
        low = lax.broadcasted_iota(jnp.int32, (size, LANES), 1) < 64
        wide = None if mask is None else jnp.broadcast_to(mask[0:1], (size, LANES))
        total = tiles + 1
        for r in range(0, rows, size):
            over = [parts(t, r, size, 1) for t in range(total)]
            for t in range(total):
                before, after = over[(t - 1) % total], over[(t + 1) % total]
                if before is None:
                    spill = jnp.where(low, 0.0, after)
                elif after is None:
                    spill = jnp.where(low, before, 0.0)
                else:
                    spill = jnp.where(low, before, after)
                main = parts(t, r, size, 0)
                value = spill if main is None else main + spill
                if t == tiles and wide is not None:
                    value = value * wide
                result[t, r:r + size, :] = value

    main_groups = [(l1, 4, 8 * g) for g in range(32)] + [(l2, 2, 8 * g) for g in range(8)] + [(l3, 1, 8 * g) for g in range(2)]
    main_rows = [(x1, 8 * g) for g in range(32)] + [(x2, 8 * g) for g in range(8)] + [(x3, 8 * g) for g in range(2)]
    side_rows = (
        [(x1, 256 + 8 * g) for g in range(12)] + [(x2, 64 + 8 * g) for g in range(9)] + [(x3, 16 + 8 * g) for g in range(6)]
    )

    def pack(groups):
        total = None
        for g, (ref, row) in enumerate(groups):
            piece = ref[row:row + 8, :]
            piece = piece if g == 0 else pltpu.roll(piece, 3 * g, 1)
            total = piece if total is None else total + piece
        return total

    def ends(source, high, low):
        return jnp.concatenate([source[high], source[low]], axis=1)

    for i in range(2):
        loads[i].wait()
        level_one_tiles(*pieces[i])
    for i in range(2, 4):
        loads[i].wait()
    level_one_tiles(*pieces[2])
    level_one_tiles(*pieces[3])
    level_one_product((0, 3))
    level_two_tile(as1.at[0], 5)
    level_two_tile(as1.at[7], 6)
    level_three_tile(as2.at[5], 3)
    level_three_tile(as2.at[6], 4)
    x1[...] = product(ends(as1, 7, 0), ends1[...])
    x2[...] = product(ends(as2, 6, 5), ends2[...])
    block = ends(as3, 4, 3)
    x3[...] = product(block, ends3[0]) + product(block, ends3[1])
    xp[0] = pack(main_rows)
    xp[1] = pack(side_rows)
    one = {key: value.astype(jnp.int32) for key, value in has.items()}
    across_z = 1 + one["gz", 1] + one["gz", -1]
    across = across_z * (1 + one["gy", 1] + one["gy", -1])
    near_lower, near_upper = (one["gy", k] * across_z + one["gz", k] for k in (-1, 1))
    far_lower, far_upper = one["gx", -1] * across, one["gx", 1]

    def wait_for(semaphore, number):
        @pl.when(number > 0)
        def _():
            pl.semaphore_wait(semaphore, number)

    def answer(d):
        signal(ready.at[1 if d[2] else 0], d)


    def enter():
        wait_for(barrier, near_lower + far_lower)

        @pl.when(interior)
        def _():
            for d in [BEFORE] + NEAR_LOWER:
                answer(d)

        @pl.when(jnp.logical_not(interior))
        def _():
            for d in [BEFORE] + NEAR_LOWER:
                @pl.when(exists(d))
                def _():
                    answer(d)

        for_neighbours(start, (2,), only=FAR_LOWER)
        for_neighbours(start, (3,), only=NEAR_LOWER)

    last_column = jnp.logical_not(has["gx", 1])

    @pl.when(jnp.logical_not(last_column))
    def _():
        enter()

    for i in range(4, 6):
        loads[i].wait()
    level_one_tiles(*pieces[4])
    @pl.when(last_column)
    def _():
        enter()

    level_one_tiles(*pieces[5])
    level_one_product((1, 2))

    def parts1(t, r, size, half):
        return None if t == 4 else p1[t, r:r + size, 128 * half:128 * half + 128]

    combine(parts1, l1, 4, ROWS1, xflag)
    for_neighbours(start, (0,), only=LOWER)
    for t in range(5):
        level_two_tile(l1.at[t], t)
    for b in range(2):
        block = jnp.concatenate([as2[2 * b], as2[2 * b + 1]], axis=1)
        p2[b] = product(block, band[...])
    p2[2] = product(as2[4], edge[...])

    def parts2(t, r, size, half):
        return p2[t, r:r + size, 128 * half:128 * half + 128]

    combine(parts2, l2, 2, ROWS2, xflag)
    for_neighbours(start, (1,), only=LOWER)

    for t in range(3):
        level_three_tile(l2.at[t], t)
    p3[0] = product(jnp.concatenate([as3[0], as3[1]], axis=1), band[...])
    p3[1] = product(as3[2], edge[...])

    def parts3(t, r, size, half):
        return p3[t, r:r + size, 128 * half:128 * half + 128]

    combine(parts3, l3, 1, ROWS3, None)

    for side, blocks2, blocks3 in ((0, (120, 128), (48, 56)), (1, (112,), (40,))):
        for t in range(2):
            for j, row in enumerate(blocks2):
                yf[side, t, 4 * j:4 * j + 4, :] = l2[t, row + 1:row + 5, :]
        for j, row in enumerate(blocks3):
            yf[side, 2, 2 * j:2 * j + 2, :] = l3[0, row + 1:row + 3, :]
        for dz in (1, -1):
            corner = CORNER[dz, 1 - 2 * side]
            row1 = (344 if side == 0 else 328) + (1 if dz == 1 else 0)
            first2, first3, size = (5, 3, 2) if dz == 1 else (0, 0, 1)
            for t in range(4):
                q[corner, t:t + 1, :] = l1[t, row1:row1 + 1, :]
            for t in range(2):
                for j, row in enumerate(blocks2):
                    to = 8 + 4 * t + 2 * j
                    q[corner, to:to + size, :] = l2[t, row + first2:row + first2 + size, :]
            for j, row in enumerate(blocks3):
                q[corner, 4 + 2 * j:4 + 2 * j + size, :] = l3[0, row + first3:row + first3 + size, :]


    for_neighbours(start, (2,), only=NEAR_LOWER)
    wait_for(ready.at[0], near_upper)
    for_neighbours(start, (3,), only=NEAR_UPPER)
    for_neighbours(start, (0, 1, 2), only=NEAR_UPPER)
    wait_for(ready.at[1], far_upper)
    for_neighbours(start, (2,), only=[NEXT])
    settle(recv_sem.at[1], NEAR_LOWER, (3,), True)
    for_neighbours(start, (4,), only=[NEXT])
    settle(recv_sem.at[2], NEAR_UPPER, (3,), True)
    for_neighbours(start, (5,), only=[NEXT])

    heights, depths = (32, 16, 8), (8, 4, 2)
    levels = (l1, l2, l3)

    def add(level, t, rows, value):
        ref = levels[level]
        ref[t, rows, :] = ref[t, rows, :] + value

    def add_y(dy, level, t, get):
        height, depth = heights[level], depths[level]
        for j in range(2 if dy == 1 and level else 1):
            add(level, t, pl.ds(j if dy == 1 else height - 1, depth, stride=height), get(j))

    def add_z(dz, level, t, get):
        height, depth = heights[level], depths[level]
        planes = 2 if dz == 1 and level else 1
        to = 0 if dz == 1 else (depth - 1) * height
        for r in range(0, planes * height, 8):
            add(level, t, slice(to + r, to + r + 8), get(r))

    def add_corner(dz, dy, level, t, get):
        height, depth = heights[level], depths[level]
        planes = 2 if dz == 1 and level else 1
        for j in range(2 if dy == 1 and level else 1):
            value = get(j)
            for p in range(planes):
                row = (p if dz == 1 else depth - 1) * height + (j if dy == 1 else height - 1)
                add(level, t, slice(row, row + 1), value[p:p + 1])

    settle(recv_sem.at[3], [d for d in DIRECTIONS if d[1] and not d[2]], (0, 1, 2), True)
    for dy in (1, -1):
        side = 0 if dy == 1 else 1
        for t in range(4):
            add_y(dy, 0, t, lambda j: ry1[side, t])
        for t in range(2):
            add_y(dy, 1, t, lambda j: ryf[side, t, 4 * j:4 * j + 4, :])
        add_y(dy, 2, 0, lambda j: ryf[side, 2, 2 * j:2 * j + 2, :])
        for dz in (1, -1):
            c = CORNER[dz, dy]
            for t in range(4):
                add_corner(dz, dy, 0, t, lambda j: rq[c, t:t + 1, :])
            for t in range(2):
                add_corner(dz, dy, 1, t, lambda j: rq[c, 8 + 4 * t + 2 * j:10 + 4 * t + 2 * j, :])
            add_corner(dz, dy, 2, 0, lambda j: rq[c, 4 + 2 * j:6 + 2 * j, :])
    settle(recv_sem.at[4], FACES[:2], (0, 1, 2), True)
    for t in range(4):
        add_z(1, 0, t, lambda r: rz1[0, t, r:r + 8, :])
        add_z(-1, 0, t, lambda r: rz1[1, t, r:r + 8, :])
    for t in range(2):
        add_z(1, 1, t, lambda r: rz2u[t, r:r + 8, :])
        add_z(-1, 1, t, lambda r: rz2d[t, r:r + 8, :])
    add_z(1, 2, 0, lambda r: rz3u[0, r:r + 8, :])
    add_z(-1, 2, 0, lambda r: rz3d[0, r:r + 8, :])
    settle(send_sem.at[0], TARGETS, None, False)
    settle(send_sem.at[1], NEAR_LOWER + NEAR_UPPER, (0, 1, 2), False)
    settle(recv_sem.at[0], [NEXT] + FAR_LOWER, (2, 4, 5), True)
    third = lax.rem(lane, 3)
    low_lanes, high_lane = lane < 2, lane == 127

    def both(low_side, high_side):
        return jnp.where((third == 2) | high_lane, high_side, low_side)

    def spread(value, g):
        moved = value if g == 0 else pltpu.roll(value, LANES - 3 * g, 1)
        return jnp.where(low_lanes, moved, 0.0), jnp.where(high_lane, moved, 0.0)

    def add_columns(level, pairs):
        last = (3, 1, 0)[level]
        for rows, (low_value, high_value) in pairs:
            if last == 0:
                add(level, 0, rows, low_value + high_value)
            else:
                add(level, 0, rows, low_value)
                add(level, last, rows, high_value)

    value = both(rx[0], rx[1])
    for g, (ref, _, row) in enumerate(main_groups):
        level = 0 if g < 32 else (1 if g < 40 else 2)
        add_columns(level, [(slice(row, row + 8), spread(value, g))])
    firsts = {0: 0, 1: 12, 2: 21}
    for dz, dy in SIDES:
        value = both(rru[SIDE[dz, dy]], rrd[SIDE[dz, dy]])
        for level in range(3):
            height, depth = heights[level], depths[level]
            if dy == 0:
                first = firsts[level] + (height // 8 if dz == 1 else 0)
                planes = 2 if dz == 1 and level else 1
                to = 0 if dz == 1 else (depth - 1) * height
                for r in range(planes * height // 8):
                    add_columns(level, [(slice(to + 8 * r, to + 8 * r + 8), spread(value, first + r))])
                continue
            for j in range(2 if dy == 1 and level else 1):
                y = j if dy == 1 else height - 1
                if level == 0:
                    group = (10 if dy == 1 else 8) + (1 if dz else 0)
                else:
                    group = {1: (18, 19), 2: (24, 25)}[level][1 if dy == 1 else 0] + j
                parts = spread(value, group)
                if dz == 0:
                    if level:
                        parts = tuple(x[1:1 + depth] for x in parts)
                    add_columns(level, [(pl.ds(y, depth, stride=height), parts)])
                    continue
                for p in range(2 if dz == 1 and level else 1):
                    if level == 0:
                        s = 1 if dz == 1 else 0
                    else:
                        s = depth + 1 + p if dz == 1 else 0
                    z = p if dz == 1 else depth - 1
                    row = slice(z * height + y, z * height + y + 1)
                    add_columns(level, [(row, tuple(x[s:s + 1] for x in parts))])

    for z in range(8):
        for t in range(4):
            out1[z, :, LANES * t:LANES * t + LANES] = l1[t, 32 * z:32 * z + 32, :]
    for z in range(4):
        for t in range(2):
            out2[z, :, LANES * t:LANES * t + LANES] = l2[t, 16 * z:16 * z + 16, :]
    for z in range(2):
        out3[z, :, :] = l3[0, 8 * z:8 * z + 8, :]


def store(in1, in2, in3, out1, out2, out3, sem):
    copies = [
        pltpu.make_async_copy(source, target, sem.at[i])
        for i, (source, target) in enumerate(((in1, out1), (in2, out2), (in3, out3)))
    ]
    for copy in copies:
        copy.start()
    for copy in copies:
        copy.wait()


def on_device(counts, volume):
    shapes = tuple(jax.ShapeDtypeStruct(s, F32) for s in ((8, 32, 512), (4, 16, 256), (2, 8, 128)))
    levels = levels_of(counts, shapes, volume)
    return pl.pallas_call(
        store,
        out_shape=shapes,
        in_specs=[pl.BlockSpec(memory_space=pltpu.VMEM)] * 3,
        out_specs=[pl.BlockSpec(memory_space=pltpu.HBM)] * 3,
        scratch_shapes=[pltpu.SemaphoreType.DMA((3,))],
        compiler_params=pltpu.CompilerParams(vmem_limit_bytes=52 * 1024 * 1024),
        name="store",
    )(*levels)


def levels_of(counts, shapes, volume):
    vmem = lambda *shape: pltpu.VMEM(shape, F32)
    return pl.pallas_call(
        functools.partial(pyramid, counts),
        out_shape=shapes,
        in_specs=[pl.BlockSpec(memory_space=pltpu.HBM)],
        out_specs=[pl.BlockSpec(memory_space=pltpu.VMEM)] * 3,
        scratch_shapes=[
            vmem(16, 64, 1024),
            vmem(8, 10 * PITCH1 + 8, LANES), vmem(8, ROWS1, LANES),
            pltpu.VMEM((2, 3, 2 * ROWS1, 256), BF16), vmem(4, ROWS1, 256), vmem(5, ROWS1, LANES),
            vmem(7, 2, 24, LANES), vmem(7, 8 * PITCH2, LANES), vmem(7, ROWS2, LANES), vmem(3, ROWS2, 256),
            vmem(3, ROWS2, LANES),
            vmem(5, 3, 24, LANES), vmem(5, 8 * PITCH3, LANES), vmem(5, ROWS3, LANES), vmem(2, ROWS3, 256),
            vmem(2, ROWS3, LANES),
            pltpu.VMEM((256, 256), BF16), pltpu.VMEM((128, 256), BF16),
            pltpu.VMEM((256, LANES), BF16), pltpu.VMEM((256, LANES), BF16), pltpu.VMEM((2, 256, LANES), BF16),
            vmem(ROWS1, LANES), vmem(ROWS2, LANES), vmem(ROWS3, LANES),
            vmem(2, 8, LANES), vmem(2, 3, 8, LANES), vmem(4, 16, LANES),
            vmem(2, 4, 32, LANES), vmem(2, 32, LANES), vmem(2, 16, LANES), vmem(1, 16, LANES), vmem(1, 8, LANES),
            vmem(2, 4, 8, LANES), vmem(2, 3, 8, LANES), vmem(4, 16, LANES),
            vmem(2, 8, LANES), vmem(8, 8, LANES), vmem(8, 8, LANES), vmem(8, 8, LANES),
            pltpu.SemaphoreType.DMA((6,)),
            pltpu.SemaphoreType.DMA((2,)),
            pltpu.SemaphoreType.DMA((5,)),
            pltpu.SemaphoreType.REGULAR((2,)),
        ],
        compiler_params=pltpu.CompilerParams(
            collective_id=0, has_side_effects=True, vmem_limit_bytes=52 * 1024 * 1024
        ),
        name="pyramid",
    )(volume)


def solution(mesh):
    spec = P("gz", "gy", "gx")
    return jax.shard_map(
        functools.partial(on_device, dict(mesh.shape)),
        mesh=mesh,
        in_specs=(spec,),
        out_specs=(spec, spec, spec),
        check_vma=False,
    )
```

```python
import functools
import math

import jax
import jax.numpy as jnp
from jax import lax
from jax.experimental import pallas as pl
from jax.experimental.pallas import tpu as pltpu
from jax.sharding import PartitionSpec as P

MESH = pl.DeviceIdType.MESH
F32 = jnp.float32
BF16 = jnp.bfloat16
LANES = 128
AXES = ("gz", "gy", "gx")
taps = (1.0, 4.0, 6.0, 4.0, 1.0)

ROWS1, ROWS2, ROWS3 = 352, 144, 64
PITCH1, PITCH2, PITCH3 = 72, 48, 32
DIRECTIONS = [
    (dz, dy, dx)
    for dx in (-1, 1, 0)
    for dz in (1, -1, 0)
    for dy in (-1, 1, 0)
    if (dz, dy, dx) != (0, 0, 0)
]
SIDES = [(1, -1), (-1, -1), (0, -1), (-1, 0), (1, 1), (-1, 1), (0, 1), (1, 0)]
SIDE = {d: i for i, d in enumerate(SIDES)}
UPPER = [d for d in DIRECTIONS if (d[2], d[1], d[0]) > (0, 0, 0)]
LOWER = [d for d in DIRECTIONS if (d[2], d[1], d[0]) < (0, 0, 0)]
TARGETS = [d for d in DIRECTIONS if d[2] < 1 or d == (0, 0, 1)]
NEAR_LOWER, NEAR_UPPER = ([d for d in half if not d[2]] for half in (LOWER, UPPER))
FAR_LOWER, NEXT, BEFORE = [d for d in LOWER if d[2]], (0, 0, 1), (0, 0, -1)
FACES = [(1, 0, 0), (-1, 0, 0), (0, 1, 0), (0, -1, 0)]
GROUP = {0: (0, 0), 3: (0, 1), 1: (1, 0), 2: (1, 1)}
CORNER = {(1, 1): 0, (1, -1): 1, (-1, 1): 2, (-1, -1): 3}


def weighted(pieces):
    groups = {}
    for k, piece in pieces.items():
        groups.setdefault(taps[k], []).append(piece)
    total = None
    for tap, members in groups.items():
        part = members[0] if len(members) == 1 else members[0] + members[1]
        part = part if tap == 1.0 else tap * part
        total = part if total is None else total + part
    return total


def reduce_planes(load, low, high, out):
    return weighted(
        {k: load(2 * out + k - 2) for k in range(5) if low <= 2 * out + k - 2 <= high}
    )


def split(block):
    first = block.astype(BF16)
    rest = block - first.astype(F32)
    second = rest.astype(BF16)
    third = (rest - second.astype(F32)).astype(BF16)
    return third, second, first


def product(block, weights):
    total = None
    for piece in split(block):
        part = jnp.dot(piece, weights, preferred_element_type=F32)
        total = part if total is None else total + part
    return total


def build_weights(band, edge):
    k = lax.broadcasted_iota(jnp.int32, (256, 256), 0)
    n = lax.broadcasted_iota(jnp.int32, (256, 256), 1)
    out = jnp.where(n < 128, n, jnp.where(n == 128, 128, jnp.where(n == 255, -1, 1000)))
    tap = k - 2 * out + 2
    value = jnp.where(tap == 2, 6.0, jnp.where((tap == 1) | (tap == 3), 4.0, jnp.where((tap == 0) | (tap == 4), 1.0, 0.0)))
    band[...] = (value * (1.0 / 4096.0)).astype(BF16)
    k = lax.broadcasted_iota(jnp.int32, (128, 256), 0)
    n = lax.broadcasted_iota(jnp.int32, (128, 256), 1)
    place = jnp.where(k < 2, k, jnp.where(k == 127, -1, 1000))
    out = jnp.where(n < 2, n, jnp.where(n == 127, -1, jnp.where(n == 255, -1, jnp.where(n == 128, 0, -1000))))
    high_in, low_in = k < 2, k == 127
    high_out = (n < 2) | (n == 255)
    low_out = (n == 127) | (n == 128)
    tap = place - 2 * out + 2
    legal = (high_in & high_out) | (low_in & low_out)
    value = jnp.where(tap == 2, 6.0, jnp.where((tap == 1) | (tap == 3), 4.0, jnp.where((tap == 0) | (tap == 4), 1.0, 0.0)))
    edge[...] = jnp.where(legal, value * (1.0 / 4096.0), 0.0).astype(BF16)


def build_end_weights(ends1, ends2, ends3):
    tap1 = [6, 4, 1]
    tap2 = [44, 40, 31, 20, 10, 4, 1]
    tap3 = [344, 336, 315, 284, 246, 204, 161, 120, 84, 56, 35, 20, 10, 4, 1]
    k = lax.broadcasted_iota(jnp.int32, (32, LANES), 0) - 16
    lane = lax.broadcasted_iota(jnp.int32, (32, LANES), 1)
    zero = jnp.zeros((112, LANES), BF16)

    def fill(ref, value):
        ref[0:112, :] = zero
        ref[112:144, :] = value.astype(BF16)
        ref[144:256, :] = zero

    for level, taps_of in enumerate((tap1, tap2, tap3)):
        step = 2 << level
        high = jnp.where((k < 0) & (lane < 2), step * lane - k, 99)
        distance = jnp.where((k >= 0) & (lane == 127), k + step, high)
        scale = 1.0 / 4096.0 ** (level + 1)
        value = jnp.zeros((32, LANES), F32)
        for offset, tap in enumerate(taps_of):
            value = jnp.where(distance == offset, (316 if tap == 315 else tap) * scale, value)
        if level == 0:
            fill(ends1, value)
        elif level == 1:
            fill(ends2, value)
        else:
            fill(ends3.at[0], value)
            fill(ends3.at[1], jnp.where(distance == 2, -scale, 0.0))


def pyramid(counts, vol, out1, out2, out3, v, zs1, as1, cut1, p1, l1, ye1, zs2, as2, p2, l2, ye2, zs3, as3, p3, l3,
            band, edge, ends1, ends2, ends3, x1, x2, x3, xp, yf, q, rz1, rz2u, rz2d, rz3u, rz3d, ry1, ryf, rq, rx, ru, rru, rrd,
            load_sem, send_sem, recv_sem, ready):
    me = {axis: lax.axis_index(axis) for axis in ("gz", "gy", "gx")}
    has = {(axis, 1): me[axis] < counts[axis] - 1 for axis in me}
    has.update({(axis, -1): me[axis] > 0 for axis in me})

    def exists(d):
        ok = None
        for axis, step in zip(("gz", "gy", "gx"), d):
            if step:
                ok = has[axis, step] if ok is None else ok & has[axis, step]
        return ok

    def device(d):
        return {axis: me[axis] + step for axis, step in zip(("gz", "gy", "gx"), d) if step}

    def blank(d):
        dz, dy, dx = d
        zeros = jnp.zeros((8, LANES), F32)
        if d == NEXT:
            rx[0] = zeros
            for i in range(8):
                rru[i] = zeros
            return
        if dx:
            target = rrd.at[SIDE[dz, dy]] if dz or dy else rx.at[1]
            target[...] = zeros
            return
        ru[SIDE[dz, dy]] = zeros
        side = 0 if dy == 1 else 1
        if dz and dy:
            targets = [rq.at[CORNER[dz, dy]]]
        elif dy:
            targets = [ry1.at[side, t] for t in range(4)] + [ryf.at[side, t] for t in range(3)]
        elif dz == 1:
            targets = [rz1.at[0, t] for t in range(4)] + [rz2u.at[t] for t in range(2)] + [rz3u.at[0]]
        else:
            targets = [rz1.at[1, t] for t in range(4)] + [rz2d.at[t] for t in range(2)] + [rz3d.at[0]]
        for target in targets:
            for r in range(0, target.shape[0], 8):
                target[r:r + 8, :] = zeros

    pieces = ((0, 1), (7, 1), (1, 1), (6, 1), (2, 2), (4, 2))
    loads = [
        pltpu.make_async_copy(
            vol.at[:, :, pl.ds(LANES * c, LANES * n)], v.at[:, :, pl.ds(LANES * c, LANES * n)], load_sem.at[i]
        )
        for i, (c, n) in enumerate(pieces)
    ]
    for load in loads:
        load.start()

    barrier = pltpu.get_barrier_semaphore()
    interior = functools.reduce(lambda x, y: x & y, has.values())

    def signal(semaphore, d):
        pl.semaphore_signal(semaphore, inc=1, device_id=device(d), device_id_type=MESH)

    @pl.when(interior)
    def _():
        for d in UPPER:
            signal(barrier, d)

    @pl.when(jnp.logical_not(interior))
    def _():
        for d in UPPER:
            @pl.when(exists(d))
            def _():
                signal(barrier, d)

        for d in TARGETS:
            @pl.when(jnp.logical_not(exists(tuple(-k for k in d))))
            def _():
                blank(d)

    build_weights(band, edge)
    build_end_weights(ends1, ends2, ends3)
    zero8 = jnp.zeros((8, LANES), F32)
    for c in range(8):
        for p in range(11):
            zs1[c, p * PITCH1:p * PITCH1 + 8, :] = zero8
        as1[c, 328:336, :] = zero8
        as1[c, 344:352, :] = zero8
    for c in range(4):
        q[c, 0:8, :] = zero8
        q[c, 8:16, :] = zero8
    for side in range(2):
        for t in range(3):
            yf[side, t] = zero8
    for t in range(7):
        for e in range(2):
            for r in range(0, 24, 8):
                ye1[t, e, r:r + 8, :] = zero8
        for p in range(8):
            zs2[t, p * PITCH2:p * PITCH2 + 8, :] = zero8
            zs2[t, p * PITCH2 + 40:p * PITCH2 + 48, :] = zero8
        for r in range(8, 40, 8):
            zs2[t, 7 * PITCH2 + r:7 * PITCH2 + r + 8, :] = zero8
        as2[t, 136:144, :] = zero8
    for t in range(5):
        for e in range(3):
            for r in range(0, 24, 8):
                ye2[t, e, r:r + 8, :] = zero8
        for p in range(8):
            zs3[t, p * PITCH3:p * PITCH3 + 8, :] = zero8
            zs3[t, p * PITCH3 + 24:p * PITCH3 + 32, :] = zero8
        for p in range(5, 8):
            for r in (8, 16):
                zs3[t, p * PITCH3 + r:p * PITCH3 + r + 8, :] = zero8

    flag = {key: jnp.where(value, 1.0, 0.0).astype(F32) for key, value in has.items()}
    zlo, zhi = flag["gz", -1], flag["gz", 1]
    ylo, yhi = flag["gy", -1], flag["gy", 1]
    lane = lax.broadcasted_iota(jnp.int32, (8, LANES), 1)
    sub = lax.broadcasted_iota(jnp.int32, (8, LANES), 0)
    xflag = jnp.where(lane < 64, flag["gx", 1], flag["gx", -1])

    def transfers(d):
        dz, dy, dx = d
        if dx == 1:
            return {
                2: (xp.at[0], rx.at[0]),
                4: (ru.at[pl.ds(0, 4)], rru.at[pl.ds(0, 4)]),
                5: (ru.at[pl.ds(4, 4)], rru.at[pl.ds(4, 4)]),
            }
        if dx == -1:
            return {2: (xp.at[1], rrd.at[SIDE[dz, dy]]) if dz or dy else (xp.at[0], rx.at[1])}
        along = (xp.at[1], ru.at[SIDE[dz, dy]])
        if dy == 0:
            if dz == 1:
                return {
                    0: (l1.at[pl.ds(0, 4), pl.ds(288, 32), :], rz1.at[0]),
                    1: (l2.at[pl.ds(0, 2), pl.ds(80, 32), :], rz2u),
                    2: (l3.at[pl.ds(0, 1), pl.ds(24, 16), :], rz3u),
                    3: along,
                }
            return {
                0: (l1.at[pl.ds(0, 4), pl.ds(256, 32), :], rz1.at[1]),
                1: (l2.at[pl.ds(0, 2), pl.ds(64, 16), :], rz2d),
                2: (l3.at[pl.ds(0, 1), pl.ds(16, 8), :], rz3d),
                3: along,
            }
        if dz == 0:
            side = 0 if dy == 1 else 1
            return {
                0: (l1.at[pl.ds(0, 4), pl.ds(336 if dy == 1 else 320, 8), :], ry1.at[side]),
                2: (yf.at[side], ryf.at[side]),
                3: along,
            }
        corner = CORNER[dz, dy]
        return {2: (q.at[corner], rq.at[corner]), 3: along}

    def awaited_with(d, stage):
        if d[2]:
            return 5 if stage == 5 else 0
        if stage == 3:
            return 1 if d in NEAR_LOWER else 2
        return 3 if d[1] else 4

    def copies(d, stages=(0, 1, 2, 3, 4, 5)):
        return [
            pltpu.make_async_remote_copy(
                src_ref=pair[0],
                dst_ref=pair[1],
                send_sem=send_sem.at[0 if d[2] or i == 3 else 1],
                recv_sem=recv_sem.at[awaited_with(d, i)],
                device_id=device(d),
                device_id_type=MESH,
            )
            for i, pair in transfers(d).items()
            if i in stages
        ]

    def for_neighbours(act, stages=(0, 1, 2, 3, 4, 5), back=False, only=None):
        chosen = [d for d in (only or TARGETS) if any(i in stages for i in transfers(d))]

        @pl.when(interior)
        def _():
            for d in chosen:
                for copy in copies(d, stages):
                    act(copy)

        @pl.when(jnp.logical_not(interior))
        def _():
            for d in chosen:
                @pl.when(exists(tuple(-k for k in d) if back else d))
                def _():
                    for copy in copies(d, stages):
                        act(copy)

    start = lambda c: c.start()

    def settle(semaphore, only, stages, back):
        parts = []
        for d in only:
            units = sum(
                math.prod(pair[0].shape) // 1024
                for i, pair in transfers(d).items()
                if (i in stages if stages else d[2] or i == 3)
            )
            parts.append((tuple(-k for k in d) if back else d, units))
        axes = [a for j, a in enumerate(AXES) if any(d[j] for d, _ in parts)]

        def wait(state):
            units = sum(u for d, u in parts if all(state[a, k] for a, k in zip(AXES, d) if k))
            if units:
                rows = pl.ds(0, 8 * units)
                pltpu.make_async_copy(zs1.at[0, rows, :], zs1.at[1, rows, :], semaphore).wait()

        def choose(left, state):
            if not left:
                wait(state)
                return
            axis = left[0]
            for low, high in ((True, True), (True, False), (False, True)):
                fits = has[axis, -1] if low else jnp.logical_not(has[axis, -1])
                fits &= has[axis, 1] if high else jnp.logical_not(has[axis, 1])

                @pl.when(fits)
                def _():
                    choose(left[1:], {**state, (axis, -1): low, (axis, 1): high})

        @pl.when(interior)
        def _():
            wait({(a, k): True for a in AXES for k in (-1, 1)})

        @pl.when(jnp.logical_not(interior))
        def _():
            choose(axes, {})

    zflag2 = jnp.where(sub == 0, zlo, jnp.where(sub < 5, 1.0, zhi))
    plane_row1 = lambda s: 256 if s == -1 else (288 if s == 8 else 32 * s)
    plane_row2 = lambda s: 64 if s == -1 else (80 + 16 * (s - 4) if s >= 4 else 16 * s)
    plane_row3 = lambda s: 16 if s == -1 else (24 + 8 * (s - 2) if s >= 2 else 8 * s)
    zscale2 = lambda i: zlo if i == -1 else (zhi if i >= 4 else None)

    def cut(c, row, block):
        group, place = GROUP[c // 2]
        at = place * ROWS1 + row
        for piece, value in enumerate(split(block)):
            cut1[group, piece, at:at + block.shape[0], LANES * (c % 2):LANES * (c % 2) + LANES] = value

    def level_one_tiles(c, n):
        for r in range(0, 64, 8):
            planes = [v[s, r:r + 8, LANES * c:LANES * (c + n)] for s in range(16)]
            for i in range(-1, 9):
                plane = reduce_planes(lambda s: planes[s], 0, 15, i)
                row = (i + 1) * PITCH1 + 8 + r
                for h in range(n):
                    zs1[c + h, row:row + 8, :] = plane[:, LANES * h:LANES * h + LANES]
        for c in range(c, c + n):
            for i in range(-1, 9):
                base = (i + 1) * PITCH1 + 8
                plane = weighted({k: zs1[c, pl.ds(base + k - 2, 32, stride=2), :] for k in range(5)})
                if i == -1:
                    plane = plane * zlo
                elif i == 8:
                    plane = plane * zhi
                row = plane_row1(i)
                if c in (0, 7):
                    as1[c, row:row + 32, :] = plane
                cut(c, row, plane)

            def column(y, p, size):
                return zs1[c, pl.ds(p * PITCH1 + 8 + y, size, stride=PITCH1), :]

            as1[c, 320:328, :] = column(0, 1, 8) * ylo
            as1[c, 336:344, :] = weighted({0: column(62, 1, 8), 1: column(63, 1, 8)}) * yhi
            for s, p, zflag in ((0, 0, zlo), (1, 9, zhi)):
                first = p * PITCH1 + 8
                as1[c, 328 + s:329 + s, :] = zs1[c, first:first + 1, :] * (ylo * zflag)
                as1[c, 344 + s:345 + s, :] = weighted(
                    {0: zs1[c, first + 62:first + 63, :], 1: zs1[c, first + 63:first + 64, :]}
                ) * (yhi * zflag)
            cut(c, 320, as1[c, 320:352, :])

    def level_one_product(blocks):
        group = GROUP[blocks[0]][0]
        total = None
        for piece in range(3):
            part = jnp.dot(cut1[group, piece], band[...], preferred_element_type=F32)
            total = part if total is None else total + part
        for b in blocks:
            at = GROUP[b][1] * ROWS1
            p1[b] = total[at:at + ROWS1]

    def level_two_tile(source, t):
        for e, first in ((0, 320), (1, 336)):
            ye1[t, e, 8:16, :] = source[first:first + 8, :]
            ye1[t, e, 7:8, :] = source[first + 8:first + 9, :]
            ye1[t, e, 16:17, :] = source[first + 9:first + 10, :]
        for i in range(-1, 6):
            plane = reduce_planes(lambda s: source[plane_row1(s):plane_row1(s) + 32, :], -1, 8, i)
            if zscale2(i) is not None:
                plane = plane * zscale2(i)
            row = (i + 1) * PITCH2 + 8
            zs2[t, row:row + 32, :] = plane
        for e, y in ((0, -1), (1, 32)):
            block = weighted({k: ye1[t, e, pl.ds(4 + k, 8, stride=2), :] for k in range(5)})
            zs2[t, pl.ds(8 + y, 8, stride=PITCH2), :] = block * zflag2
        for i in range(-1, 6):
            base = (i + 1) * PITCH2 + 8
            row = plane_row2(i)
            as2[t, row:row + 16, :] = weighted(
                {k: zs2[t, pl.ds(base + k - 2, 16, stride=2), :] for k in range(5)}
            )

        def column2(y):
            return zs2[t, pl.ds(8 + y, 8, stride=PITCH2), :]

        as2[t, 112:120, :] = weighted({3: column2(-1), 4: column2(0)}) * ylo
        as2[t, 120:128, :] = weighted({0: column2(30), 1: column2(31), 2: column2(32)}) * yhi
        as2[t, 128:136, :] = column2(32) * yhi

    def level_three_tile(source, t):
        for e, first in ((0, 112), (1, 120), (2, 128)):
            ye2[t, e, 7:15, :] = source[first:first + 8, :]
        for i in range(-1, 4):
            row = (i + 1) * PITCH3 + 8
            zs3[t, row:row + 16, :] = reduce_planes(
                lambda s: source[plane_row2(s):plane_row2(s) + 16, :], -1, 5, i
            )
        for e, y in ((0, -1), (1, 16), (2, 17)):
            block = weighted({k: ye2[t, e, pl.ds(4 + k, 8, stride=2), :] for k in range(5)})
            zs3[t, pl.ds(8 + y, 8, stride=PITCH3), :] = block
        for i in range(-1, 4):
            base = (i + 1) * PITCH3 + 8
            row = plane_row3(i)
            as3[t, row:row + 8, :] = weighted(
                {k: zs3[t, pl.ds(base + k - 2, 8, stride=2), :] for k in range(5)}
            )

        def column3(y):
            return zs3[t, pl.ds(8 + y, 8, stride=PITCH3), :]

        as3[t, 40:48, :] = weighted({3: column3(-1), 4: column3(0)})
        as3[t, 48:56, :] = weighted({k: column3(14 + k) for k in range(4)})
        as3[t, 56:64, :] = weighted({0: column3(16), 1: column3(17)})

    def combine(parts, result, tiles, rows, mask):
        size = 16
        low = lax.broadcasted_iota(jnp.int32, (size, LANES), 1) < 64
        wide = None if mask is None else jnp.broadcast_to(mask[0:1], (size, LANES))
        total = tiles + 1
        for r in range(0, rows, size):
            over = [parts(t, r, size, 1) for t in range(total)]
            for t in range(total):
                before, after = over[(t - 1) % total], over[(t + 1) % total]
                if before is None:
                    spill = jnp.where(low, 0.0, after)
                elif after is None:
                    spill = jnp.where(low, before, 0.0)
                else:
                    spill = jnp.where(low, before, after)
                main = parts(t, r, size, 0)
                value = spill if main is None else main + spill
                if t == tiles and wide is not None:
                    value = value * wide
                result[t, r:r + size, :] = value

    main_groups = [(l1, 4, 8 * g) for g in range(32)] + [(l2, 2, 8 * g) for g in range(8)] + [(l3, 1, 8 * g) for g in range(2)]
    main_rows = [(x1, 8 * g) for g in range(32)] + [(x2, 8 * g) for g in range(8)] + [(x3, 8 * g) for g in range(2)]
    side_rows = (
        [(x1, 256 + 8 * g) for g in range(12)] + [(x2, 64 + 8 * g) for g in range(9)] + [(x3, 16 + 8 * g) for g in range(6)]
    )

    def pack(groups):
        total = None
        for g, (ref, row) in enumerate(groups):
            piece = ref[row:row + 8, :]
            piece = piece if g == 0 else pltpu.roll(piece, 3 * g, 1)
            total = piece if total is None else total + piece
        return total

    def ends(source, high, low):
        return jnp.concatenate([source[high], source[low]], axis=1)

    for i in range(2):
        loads[i].wait()
        level_one_tiles(*pieces[i])
    for i in range(2, 4):
        loads[i].wait()
    level_one_tiles(*pieces[2])
    level_one_tiles(*pieces[3])
    level_one_product((0, 3))
    level_two_tile(as1.at[0], 5)
    level_two_tile(as1.at[7], 6)
    level_three_tile(as2.at[5], 3)
    level_three_tile(as2.at[6], 4)
    x1[...] = product(ends(as1, 7, 0), ends1[...])
    x2[...] = product(ends(as2, 6, 5), ends2[...])
    block = ends(as3, 4, 3)
    x3[...] = product(block, ends3[0]) + product(block, ends3[1])
    xp[0] = pack(main_rows)
    xp[1] = pack(side_rows)
    one = {key: value.astype(jnp.int32) for key, value in has.items()}
    across_z = 1 + one["gz", 1] + one["gz", -1]
    across = across_z * (1 + one["gy", 1] + one["gy", -1])
    near_lower, near_upper = (one["gy", k] * across_z + one["gz", k] for k in (-1, 1))
    far_lower, far_upper = one["gx", -1] * across, one["gx", 1]

    def wait_for(semaphore, number):
        @pl.when(number > 0)
        def _():
            pl.semaphore_wait(semaphore, number)

    def answer(d):
        signal(ready.at[1 if d[2] else 0], d)


    def enter():
        wait_for(barrier, near_lower + far_lower)

        @pl.when(interior)
        def _():
            for d in [BEFORE] + NEAR_LOWER:
                answer(d)

        @pl.when(jnp.logical_not(interior))
        def _():
            for d in [BEFORE] + NEAR_LOWER:
                @pl.when(exists(d))
                def _():
                    answer(d)

        for_neighbours(start, (2,), only=FAR_LOWER)
        for_neighbours(start, (3,), only=NEAR_LOWER)

    last_column = jnp.logical_not(has["gx", 1])

    @pl.when(jnp.logical_not(last_column))
    def _():
        enter()

    for i in range(4, 6):
        loads[i].wait()
    level_one_tiles(*pieces[4])
    @pl.when(last_column)
    def _():
        enter()

    level_one_tiles(*pieces[5])
    level_one_product((1, 2))

    def parts1(t, r, size, half):
        return None if t == 4 else p1[t, r:r + size, 128 * half:128 * half + 128]

    combine(parts1, l1, 4, ROWS1, xflag)
    for_neighbours(start, (0,), only=LOWER)
    for t in range(5):
        level_two_tile(l1.at[t], t)
    for b in range(2):
        block = jnp.concatenate([as2[2 * b], as2[2 * b + 1]], axis=1)
        p2[b] = product(block, band[...])
    p2[2] = product(as2[4], edge[...])

    def parts2(t, r, size, half):
        return p2[t, r:r + size, 128 * half:128 * half + 128]

    combine(parts2, l2, 2, ROWS2, xflag)
    for_neighbours(start, (1,), only=LOWER)
    prompt = (me["gx"] == counts["gx"] - 2) & (lax.rem(me["gz"], 2) == 0)

    def pass_on():
        wait_for(ready.at[0], near_upper)
        for_neighbours(start, (3,), only=NEAR_UPPER)

    @pl.when(prompt)
    def _():
        pass_on()


    for t in range(3):
        level_three_tile(l2.at[t], t)
    p3[0] = product(jnp.concatenate([as3[0], as3[1]], axis=1), band[...])
    p3[1] = product(as3[2], edge[...])

    def parts3(t, r, size, half):
        return p3[t, r:r + size, 128 * half:128 * half + 128]

    combine(parts3, l3, 1, ROWS3, None)

    for side, blocks2, blocks3 in ((0, (120, 128), (48, 56)), (1, (112,), (40,))):
        for t in range(2):
            for j, row in enumerate(blocks2):
                yf[side, t, 4 * j:4 * j + 4, :] = l2[t, row + 1:row + 5, :]
        for j, row in enumerate(blocks3):
            yf[side, 2, 2 * j:2 * j + 2, :] = l3[0, row + 1:row + 3, :]
        for dz in (1, -1):
            corner = CORNER[dz, 1 - 2 * side]
            row1 = (344 if side == 0 else 328) + (1 if dz == 1 else 0)
            first2, first3, size = (5, 3, 2) if dz == 1 else (0, 0, 1)
            for t in range(4):
                q[corner, t:t + 1, :] = l1[t, row1:row1 + 1, :]
            for t in range(2):
                for j, row in enumerate(blocks2):
                    to = 8 + 4 * t + 2 * j
                    q[corner, to:to + size, :] = l2[t, row + first2:row + first2 + size, :]
            for j, row in enumerate(blocks3):
                q[corner, 4 + 2 * j:4 + 2 * j + size, :] = l3[0, row + first3:row + first3 + size, :]


    for_neighbours(start, (2,), only=NEAR_LOWER)
    @pl.when(jnp.logical_not(prompt))
    def _():
        pass_on()

    for_neighbours(start, (0, 1, 2), only=NEAR_UPPER)
    wait_for(ready.at[1], far_upper)
    for_neighbours(start, (2,), only=[NEXT])
    settle(recv_sem.at[1], NEAR_LOWER, (3,), True)
    for_neighbours(start, (4,), only=[NEXT])
    settle(recv_sem.at[2], NEAR_UPPER, (3,), True)
    for_neighbours(start, (5,), only=[NEXT])

    heights, depths = (32, 16, 8), (8, 4, 2)
    levels = (l1, l2, l3)

    def add(level, t, rows, value):
        ref = levels[level]
        ref[t, rows, :] = ref[t, rows, :] + value

    def add_y(dy, level, t, get):
        height, depth = heights[level], depths[level]
        for j in range(2 if dy == 1 and level else 1):
            add(level, t, pl.ds(j if dy == 1 else height - 1, depth, stride=height), get(j))

    def add_z(dz, level, t, get):
        height, depth = heights[level], depths[level]
        planes = 2 if dz == 1 and level else 1
        to = 0 if dz == 1 else (depth - 1) * height
        for r in range(0, planes * height, 8):
            add(level, t, slice(to + r, to + r + 8), get(r))

    def add_corner(dz, dy, level, t, get):
        height, depth = heights[level], depths[level]
        planes = 2 if dz == 1 and level else 1
        for j in range(2 if dy == 1 and level else 1):
            value = get(j)
            for p in range(planes):
                row = (p if dz == 1 else depth - 1) * height + (j if dy == 1 else height - 1)
                add(level, t, slice(row, row + 1), value[p:p + 1])

    settle(recv_sem.at[3], [d for d in DIRECTIONS if d[1] and not d[2]], (0, 1, 2), True)
    for dy in (1, -1):
        side = 0 if dy == 1 else 1
        for t in range(4):
            add_y(dy, 0, t, lambda j: ry1[side, t])
        for t in range(2):
            add_y(dy, 1, t, lambda j: ryf[side, t, 4 * j:4 * j + 4, :])
        add_y(dy, 2, 0, lambda j: ryf[side, 2, 2 * j:2 * j + 2, :])
        for dz in (1, -1):
            c = CORNER[dz, dy]
            for t in range(4):
                add_corner(dz, dy, 0, t, lambda j: rq[c, t:t + 1, :])
            for t in range(2):
                add_corner(dz, dy, 1, t, lambda j: rq[c, 8 + 4 * t + 2 * j:10 + 4 * t + 2 * j, :])
            add_corner(dz, dy, 2, 0, lambda j: rq[c, 4 + 2 * j:6 + 2 * j, :])
    settle(recv_sem.at[4], FACES[:2], (0, 1, 2), True)
    for t in range(4):
        add_z(1, 0, t, lambda r: rz1[0, t, r:r + 8, :])
        add_z(-1, 0, t, lambda r: rz1[1, t, r:r + 8, :])
    for t in range(2):
        add_z(1, 1, t, lambda r: rz2u[t, r:r + 8, :])
        add_z(-1, 1, t, lambda r: rz2d[t, r:r + 8, :])
    add_z(1, 2, 0, lambda r: rz3u[0, r:r + 8, :])
    add_z(-1, 2, 0, lambda r: rz3d[0, r:r + 8, :])
    settle(send_sem.at[0], TARGETS, None, False)
    settle(send_sem.at[1], NEAR_LOWER + NEAR_UPPER, (0, 1, 2), False)
    settle(recv_sem.at[0], [NEXT] + FAR_LOWER, (2, 4), True)
    third = lax.rem(lane, 3)
    low_lanes, high_lane = lane < 2, lane == 127

    def both(low_side, high_side):
        return jnp.where((third == 2) | high_lane, high_side, low_side)

    def spread(value, g):
        moved = value if g == 0 else pltpu.roll(value, LANES - 3 * g, 1)
        return jnp.where(low_lanes, moved, 0.0), jnp.where(high_lane, moved, 0.0)

    def add_columns(level, pairs, keep=(True, True)):
        last = (3, 1, 0)[level]
        for rows, (low_value, high_value) in pairs:
            if last == 0 and keep == (True, True):
                add(level, 0, rows, low_value + high_value)
                continue
            if keep[0]:
                add(level, 0, rows, low_value)
            if keep[1]:
                add(level, last, rows, high_value)

    value = both(rx[0], rx[1])
    for g, (ref, _, row) in enumerate(main_groups):
        level = 0 if g < 32 else (1 if g < 40 else 2)
        add_columns(level, [(slice(row, row + 8), spread(value, g))])
    firsts = {0: 0, 1: 12, 2: 21}

    def add_sides(sides, values, keep):
        for dz, dy in sides:
            value = values(SIDE[dz, dy])
            for level in range(3):
                height, depth = heights[level], depths[level]
                if dy == 0:
                    first = firsts[level] + (height // 8 if dz == 1 else 0)
                    planes = 2 if dz == 1 and level else 1
                    to = 0 if dz == 1 else (depth - 1) * height
                    for r in range(planes * height // 8):
                        add_columns(level, [(slice(to + 8 * r, to + 8 * r + 8), spread(value, first + r))], keep)
                    continue
                for j in range(2 if dy == 1 and level else 1):
                    y = j if dy == 1 else height - 1
                    if level == 0:
                        group = (10 if dy == 1 else 8) + (1 if dz else 0)
                    else:
                        group = {1: (18, 19), 2: (24, 25)}[level][1 if dy == 1 else 0] + j
                    parts = spread(value, group)
                    if dz == 0:
                        if level:
                            parts = tuple(x[1:1 + depth] for x in parts)
                        add_columns(level, [(pl.ds(y, depth, stride=height), parts)], keep)
                        continue
                    for p in range(2 if dz == 1 and level else 1):
                        if level == 0:
                            s = 1 if dz == 1 else 0
                        else:
                            s = depth + 1 + p if dz == 1 else 0
                        z = p if dz == 1 else depth - 1
                        row = slice(z * height + y, z * height + y + 1)
                        add_columns(level, [(row, tuple(x[s:s + 1] for x in parts))], keep)

    add_sides(SIDES[:4], lambda i: both(rru[i], rrd[i]), (True, True))
    add_sides(SIDES[4:], lambda i: rrd[i], (False, True))
    settle(recv_sem.at[5], [NEXT], (5,), True)
    add_sides(SIDES[4:], lambda i: rru[i], (True, False))

    for z in range(8):
        for t in range(4):
            out1[z, :, LANES * t:LANES * t + LANES] = l1[t, 32 * z:32 * z + 32, :]
    for z in range(4):
        for t in range(2):
            out2[z, :, LANES * t:LANES * t + LANES] = l2[t, 16 * z:16 * z + 16, :]
    for z in range(2):
        out3[z, :, :] = l3[0, 8 * z:8 * z + 8, :]


def store(in1, in2, in3, out1, out2, out3, sem):
    copies = [
        pltpu.make_async_copy(source, target, sem.at[i])
        for i, (source, target) in enumerate(((in1, out1), (in2, out2), (in3, out3)))
    ]
    for copy in copies:
        copy.start()
    for copy in copies:
        copy.wait()


def on_device(counts, volume):
    shapes = tuple(jax.ShapeDtypeStruct(s, F32) for s in ((8, 32, 512), (4, 16, 256), (2, 8, 128)))
    levels = levels_of(counts, shapes, volume)
    return pl.pallas_call(
        store,
        out_shape=shapes,
        in_specs=[pl.BlockSpec(memory_space=pltpu.VMEM)] * 3,
        out_specs=[pl.BlockSpec(memory_space=pltpu.HBM)] * 3,
        scratch_shapes=[pltpu.SemaphoreType.DMA((3,))],
        compiler_params=pltpu.CompilerParams(vmem_limit_bytes=52 * 1024 * 1024),
        name="store",
    )(*levels)


def levels_of(counts, shapes, volume):
    vmem = lambda *shape: pltpu.VMEM(shape, F32)
    return pl.pallas_call(
        functools.partial(pyramid, counts),
        out_shape=shapes,
        in_specs=[pl.BlockSpec(memory_space=pltpu.HBM)],
        out_specs=[pl.BlockSpec(memory_space=pltpu.VMEM)] * 3,
        scratch_shapes=[
            vmem(16, 64, 1024),
            vmem(8, 10 * PITCH1 + 8, LANES), vmem(8, ROWS1, LANES),
            pltpu.VMEM((2, 3, 2 * ROWS1, 256), BF16), vmem(4, ROWS1, 256), vmem(5, ROWS1, LANES),
            vmem(7, 2, 24, LANES), vmem(7, 8 * PITCH2, LANES), vmem(7, ROWS2, LANES), vmem(3, ROWS2, 256),
            vmem(3, ROWS2, LANES),
            vmem(5, 3, 24, LANES), vmem(5, 8 * PITCH3, LANES), vmem(5, ROWS3, LANES), vmem(2, ROWS3, 256),
            vmem(2, ROWS3, LANES),
            pltpu.VMEM((256, 256), BF16), pltpu.VMEM((128, 256), BF16),
            pltpu.VMEM((256, LANES), BF16), pltpu.VMEM((256, LANES), BF16), pltpu.VMEM((2, 256, LANES), BF16),
            vmem(ROWS1, LANES), vmem(ROWS2, LANES), vmem(ROWS3, LANES),
            vmem(2, 8, LANES), vmem(2, 3, 8, LANES), vmem(4, 16, LANES),
            vmem(2, 4, 32, LANES), vmem(2, 32, LANES), vmem(2, 16, LANES), vmem(1, 16, LANES), vmem(1, 8, LANES),
            vmem(2, 4, 8, LANES), vmem(2, 3, 8, LANES), vmem(4, 16, LANES),
            vmem(2, 8, LANES), vmem(8, 8, LANES), vmem(8, 8, LANES), vmem(8, 8, LANES),
            pltpu.SemaphoreType.DMA((6,)),
            pltpu.SemaphoreType.DMA((2,)),
            pltpu.SemaphoreType.DMA((6,)),
            pltpu.SemaphoreType.REGULAR((2,)),
        ],
        compiler_params=pltpu.CompilerParams(
            collective_id=0, has_side_effects=True, vmem_limit_bytes=52 * 1024 * 1024
        ),
        name="pyramid",
    )(volume)


def solution(mesh):
    spec = P("gz", "gy", "gx")
    return jax.shard_map(
        functools.partial(on_device, dict(mesh.shape)),
        mesh=mesh,
        in_specs=(spec,),
        out_specs=(spec, spec, spec),
        check_vma=False,
    )
```

```python
import functools
import math

import jax
import jax.numpy as jnp
from jax import lax
from jax.experimental import pallas as pl
from jax.experimental.pallas import tpu as pltpu
from jax.sharding import PartitionSpec as P

MESH = pl.DeviceIdType.MESH
F32 = jnp.float32
BF16 = jnp.bfloat16
LANES = 128
AXES = ("gz", "gy", "gx")
taps = (1.0, 4.0, 6.0, 4.0, 1.0)

ROWS1, ROWS2, ROWS3 = 352, 144, 64
PITCH1, PITCH2, PITCH3 = 72, 48, 32
DIRECTIONS = [
    (dz, dy, dx)
    for dx in (-1, 1, 0)
    for dz in (1, -1, 0)
    for dy in (-1, 1, 0)
    if (dz, dy, dx) != (0, 0, 0)
]
SIDES = [(1, -1), (-1, -1), (0, -1), (-1, 0), (1, 1), (-1, 1), (0, 1), (1, 0)]
SIDE = {d: i for i, d in enumerate(SIDES)}
UPPER = [d for d in DIRECTIONS if (d[2], d[1], d[0]) > (0, 0, 0)]
LOWER = [d for d in DIRECTIONS if (d[2], d[1], d[0]) < (0, 0, 0)]
TARGETS = [d for d in DIRECTIONS if d[2] < 1 or d == (0, 0, 1)]
NEAR_LOWER, NEAR_UPPER = ([d for d in half if not d[2]] for half in (LOWER, UPPER))
FAR_LOWER, NEXT, BEFORE = [d for d in LOWER if d[2]], (0, 0, 1), (0, 0, -1)
FACES = [(1, 0, 0), (-1, 0, 0), (0, 1, 0), (0, -1, 0)]
GROUP = {0: (0, 0), 3: (0, 1), 1: (1, 0), 2: (1, 1)}
CORNER = {(1, 1): 0, (1, -1): 1, (-1, 1): 2, (-1, -1): 3}


def weighted(pieces):
    groups = {}
    for k, piece in pieces.items():
        groups.setdefault(taps[k], []).append(piece)
    total = None
    for tap, members in groups.items():
        part = members[0] if len(members) == 1 else members[0] + members[1]
        part = part if tap == 1.0 else tap * part
        total = part if total is None else total + part
    return total


def reduce_planes(load, low, high, out):
    return weighted(
        {k: load(2 * out + k - 2) for k in range(5) if low <= 2 * out + k - 2 <= high}
    )


def split(block):
    first = block.astype(BF16)
    rest = block - first.astype(F32)
    second = rest.astype(BF16)
    third = (rest - second.astype(F32)).astype(BF16)
    return third, second, first


def product(block, weights):
    total = None
    for piece in split(block):
        part = jnp.dot(piece, weights, preferred_element_type=F32)
        total = part if total is None else total + part
    return total


def build_weights(band, edge):
    k = lax.broadcasted_iota(jnp.int32, (256, 256), 0)
    n = lax.broadcasted_iota(jnp.int32, (256, 256), 1)
    out = jnp.where(n < 128, n, jnp.where(n == 128, 128, jnp.where(n == 255, -1, 1000)))
    tap = k - 2 * out + 2
    value = jnp.where(tap == 2, 6.0, jnp.where((tap == 1) | (tap == 3), 4.0, jnp.where((tap == 0) | (tap == 4), 1.0, 0.0)))
    band[...] = (value * (1.0 / 4096.0)).astype(BF16)
    k = lax.broadcasted_iota(jnp.int32, (128, 256), 0)
    n = lax.broadcasted_iota(jnp.int32, (128, 256), 1)
    place = jnp.where(k < 2, k, jnp.where(k == 127, -1, 1000))
    out = jnp.where(n < 2, n, jnp.where(n == 127, -1, jnp.where(n == 255, -1, jnp.where(n == 128, 0, -1000))))
    high_in, low_in = k < 2, k == 127
    high_out = (n < 2) | (n == 255)
    low_out = (n == 127) | (n == 128)
    tap = place - 2 * out + 2
    legal = (high_in & high_out) | (low_in & low_out)
    value = jnp.where(tap == 2, 6.0, jnp.where((tap == 1) | (tap == 3), 4.0, jnp.where((tap == 0) | (tap == 4), 1.0, 0.0)))
    edge[...] = jnp.where(legal, value * (1.0 / 4096.0), 0.0).astype(BF16)


def build_end_weights(ends1, ends2, ends3):
    tap1 = [6, 4, 1]
    tap2 = [44, 40, 31, 20, 10, 4, 1]
    tap3 = [344, 336, 315, 284, 246, 204, 161, 120, 84, 56, 35, 20, 10, 4, 1]
    k = lax.broadcasted_iota(jnp.int32, (32, LANES), 0) - 16
    lane = lax.broadcasted_iota(jnp.int32, (32, LANES), 1)
    zero = jnp.zeros((112, LANES), BF16)

    def fill(ref, value):
        ref[0:112, :] = zero
        ref[112:144, :] = value.astype(BF16)
        ref[144:256, :] = zero

    for level, taps_of in enumerate((tap1, tap2, tap3)):
        step = 2 << level
        high = jnp.where((k < 0) & (lane < 2), step * lane - k, 99)
        distance = jnp.where((k >= 0) & (lane == 127), k + step, high)
        scale = 1.0 / 4096.0 ** (level + 1)
        value = jnp.zeros((32, LANES), F32)
        for offset, tap in enumerate(taps_of):
            value = jnp.where(distance == offset, (316 if tap == 315 else tap) * scale, value)
        if level == 0:
            fill(ends1, value)
        elif level == 1:
            fill(ends2, value)
        else:
            fill(ends3.at[0], value)
            fill(ends3.at[1], jnp.where(distance == 2, -scale, 0.0))


def pyramid(counts, vol, out1, out2, out3, v, zs1, as1, cut1, p1, l1, ye1, zs2, as2, p2, l2, ye2, zs3, as3, p3, l3,
            band, edge, ends1, ends2, ends3, x1, x2, x3, xp, yf, q, rz1, rz2u, rz2d, rz3u, rz3d, ry1, ryf, rq, rx, ru, rru, rrd,
            load_sem, send_sem, recv_sem, ready):
    me = {axis: lax.axis_index(axis) for axis in ("gz", "gy", "gx")}
    has = {(axis, 1): me[axis] < counts[axis] - 1 for axis in me}
    has.update({(axis, -1): me[axis] > 0 for axis in me})

    def exists(d):
        ok = None
        for axis, step in zip(("gz", "gy", "gx"), d):
            if step:
                ok = has[axis, step] if ok is None else ok & has[axis, step]
        return ok

    def device(d):
        return {axis: me[axis] + step for axis, step in zip(("gz", "gy", "gx"), d) if step}

    def blank(d):
        dz, dy, dx = d
        zeros = jnp.zeros((8, LANES), F32)
        if d == NEXT:
            rx[0] = zeros
            for i in range(8):
                rru[i] = zeros
            return
        if dx:
            target = rrd.at[SIDE[dz, dy]] if dz or dy else rx.at[1]
            target[...] = zeros
            return
        ru[SIDE[dz, dy]] = zeros
        side = 0 if dy == 1 else 1
        if dz and dy:
            targets = [rq.at[CORNER[dz, dy]]]
        elif dy:
            targets = [ry1.at[side, t] for t in range(4)] + [ryf.at[side, t] for t in range(3)]
        elif dz == 1:
            targets = [rz1.at[0, t] for t in range(4)] + [rz2u.at[t] for t in range(2)] + [rz3u.at[0]]
        else:
            targets = [rz1.at[1, t] for t in range(4)] + [rz2d.at[t] for t in range(2)] + [rz3d.at[0]]
        for target in targets:
            for r in range(0, target.shape[0], 8):
                target[r:r + 8, :] = zeros

    pieces = ((0, 1), (7, 1), (1, 1), (6, 1), (2, 2), (4, 2))
    loads = [
        pltpu.make_async_copy(
            vol.at[:, :, pl.ds(LANES * c, LANES * n)], v.at[:, :, pl.ds(LANES * c, LANES * n)], load_sem.at[i]
        )
        for i, (c, n) in enumerate(pieces)
    ]
    for load in loads:
        load.start()

    barrier = pltpu.get_barrier_semaphore()
    interior = functools.reduce(lambda x, y: x & y, has.values())

    def signal(semaphore, d):
        pl.semaphore_signal(semaphore, inc=1, device_id=device(d), device_id_type=MESH)

    @pl.when(interior)
    def _():
        for d in UPPER:
            signal(barrier, d)

    @pl.when(jnp.logical_not(interior))
    def _():
        for d in UPPER:
            @pl.when(exists(d))
            def _():
                signal(barrier, d)

        for d in TARGETS:
            @pl.when(jnp.logical_not(exists(tuple(-k for k in d))))
            def _():
                blank(d)

    build_weights(band, edge)
    build_end_weights(ends1, ends2, ends3)
    zero8 = jnp.zeros((8, LANES), F32)
    for c in range(8):
        for p in range(11):
            zs1[c, p * PITCH1:p * PITCH1 + 8, :] = zero8
        as1[c, 328:336, :] = zero8
        as1[c, 344:352, :] = zero8
    for c in range(4):
        q[c, 0:8, :] = zero8
        q[c, 8:16, :] = zero8
    for side in range(2):
        for t in range(3):
            yf[side, t] = zero8
    for t in range(7):
        for e in range(2):
            for r in range(0, 24, 8):
                ye1[t, e, r:r + 8, :] = zero8
        for p in range(8):
            zs2[t, p * PITCH2:p * PITCH2 + 8, :] = zero8
            zs2[t, p * PITCH2 + 40:p * PITCH2 + 48, :] = zero8
        for r in range(8, 40, 8):
            zs2[t, 7 * PITCH2 + r:7 * PITCH2 + r + 8, :] = zero8
        as2[t, 136:144, :] = zero8
    for t in range(5):
        for e in range(3):
            for r in range(0, 24, 8):
                ye2[t, e, r:r + 8, :] = zero8
        for p in range(8):
            zs3[t, p * PITCH3:p * PITCH3 + 8, :] = zero8
            zs3[t, p * PITCH3 + 24:p * PITCH3 + 32, :] = zero8
        for p in range(5, 8):
            for r in (8, 16):
                zs3[t, p * PITCH3 + r:p * PITCH3 + r + 8, :] = zero8

    flag = {key: jnp.where(value, 1.0, 0.0).astype(F32) for key, value in has.items()}
    zlo, zhi = flag["gz", -1], flag["gz", 1]
    ylo, yhi = flag["gy", -1], flag["gy", 1]
    lane = lax.broadcasted_iota(jnp.int32, (8, LANES), 1)
    sub = lax.broadcasted_iota(jnp.int32, (8, LANES), 0)
    xflag = jnp.where(lane < 64, flag["gx", 1], flag["gx", -1])

    def transfers(d):
        dz, dy, dx = d
        if dx == 1:
            return {
                2: (xp.at[0], rx.at[0]),
                4: (ru.at[pl.ds(0, 4)], rru.at[pl.ds(0, 4)]),
                5: (ru.at[pl.ds(4, 4)], rru.at[pl.ds(4, 4)]),
            }
        if dx == -1:
            return {2: (xp.at[1], rrd.at[SIDE[dz, dy]]) if dz or dy else (xp.at[0], rx.at[1])}
        along = (xp.at[1], ru.at[SIDE[dz, dy]])
        if dy == 0:
            if dz == 1:
                return {
                    0: (l1.at[pl.ds(0, 4), pl.ds(288, 32), :], rz1.at[0]),
                    1: (l2.at[pl.ds(0, 2), pl.ds(80, 32), :], rz2u),
                    2: (l3.at[pl.ds(0, 1), pl.ds(24, 16), :], rz3u),
                    3: along,
                }
            return {
                0: (l1.at[pl.ds(0, 4), pl.ds(256, 32), :], rz1.at[1]),
                1: (l2.at[pl.ds(0, 2), pl.ds(64, 16), :], rz2d),
                2: (l3.at[pl.ds(0, 1), pl.ds(16, 8), :], rz3d),
                3: along,
            }
        if dz == 0:
            side = 0 if dy == 1 else 1
            return {
                0: (l1.at[pl.ds(0, 4), pl.ds(336 if dy == 1 else 320, 8), :], ry1.at[side]),
                2: (yf.at[side], ryf.at[side]),
                3: along,
            }
        corner = CORNER[dz, dy]
        return {2: (q.at[corner], rq.at[corner]), 3: along}

    def awaited_with(d, stage):
        if d[2]:
            return 5 if stage == 5 else 0
        if stage == 3:
            return 1 if d in NEAR_LOWER else 2
        return (6 if d[0] else 3) if d[1] else 4

    def copies(d, stages=(0, 1, 2, 3, 4, 5)):
        return [
            pltpu.make_async_remote_copy(
                src_ref=pair[0],
                dst_ref=pair[1],
                send_sem=send_sem.at[0 if d[2] or i == 3 else 1],
                recv_sem=recv_sem.at[awaited_with(d, i)],
                device_id=device(d),
                device_id_type=MESH,
            )
            for i, pair in transfers(d).items()
            if i in stages
        ]

    def for_neighbours(act, stages=(0, 1, 2, 3, 4, 5), back=False, only=None):
        chosen = [d for d in (only or TARGETS) if any(i in stages for i in transfers(d))]

        @pl.when(interior)
        def _():
            for d in chosen:
                for copy in copies(d, stages):
                    act(copy)

        @pl.when(jnp.logical_not(interior))
        def _():
            for d in chosen:
                @pl.when(exists(tuple(-k for k in d) if back else d))
                def _():
                    for copy in copies(d, stages):
                        act(copy)

    start = lambda c: c.start()

    def settle(semaphore, only, stages, back):
        parts = []
        for d in only:
            units = sum(
                math.prod(pair[0].shape) // 1024
                for i, pair in transfers(d).items()
                if (i in stages if stages else d[2] or i == 3)
            )
            parts.append((tuple(-k for k in d) if back else d, units))
        axes = [a for j, a in enumerate(AXES) if any(d[j] for d, _ in parts)]

        def wait(state):
            units = sum(u for d, u in parts if all(state[a, k] for a, k in zip(AXES, d) if k))
            if units:
                rows = pl.ds(0, 8 * units)
                pltpu.make_async_copy(zs1.at[0, rows, :], zs1.at[1, rows, :], semaphore).wait()

        def choose(left, state):
            if not left:
                wait(state)
                return
            axis = left[0]
            for low, high in ((True, True), (True, False), (False, True)):
                fits = has[axis, -1] if low else jnp.logical_not(has[axis, -1])
                fits &= has[axis, 1] if high else jnp.logical_not(has[axis, 1])

                @pl.when(fits)
                def _():
                    choose(left[1:], {**state, (axis, -1): low, (axis, 1): high})

        @pl.when(interior)
        def _():
            wait({(a, k): True for a in AXES for k in (-1, 1)})

        @pl.when(jnp.logical_not(interior))
        def _():
            choose(axes, {})

    zflag2 = jnp.where(sub == 0, zlo, jnp.where(sub < 5, 1.0, zhi))
    plane_row1 = lambda s: 256 if s == -1 else (288 if s == 8 else 32 * s)
    plane_row2 = lambda s: 64 if s == -1 else (80 + 16 * (s - 4) if s >= 4 else 16 * s)
    plane_row3 = lambda s: 16 if s == -1 else (24 + 8 * (s - 2) if s >= 2 else 8 * s)
    zscale2 = lambda i: zlo if i == -1 else (zhi if i >= 4 else None)

    def cut(c, row, block):
        group, place = GROUP[c // 2]
        at = place * ROWS1 + row
        for piece, value in enumerate(split(block)):
            cut1[group, piece, at:at + block.shape[0], LANES * (c % 2):LANES * (c % 2) + LANES] = value

    def level_one_tiles(c, n):
        for r in range(0, 64, 8):
            planes = [v[s, r:r + 8, LANES * c:LANES * (c + n)] for s in range(16)]
            for i in range(-1, 9):
                plane = reduce_planes(lambda s: planes[s], 0, 15, i)
                row = (i + 1) * PITCH1 + 8 + r
                for h in range(n):
                    zs1[c + h, row:row + 8, :] = plane[:, LANES * h:LANES * h + LANES]
        for c in range(c, c + n):
            for i in range(-1, 9):
                base = (i + 1) * PITCH1 + 8
                plane = weighted({k: zs1[c, pl.ds(base + k - 2, 32, stride=2), :] for k in range(5)})
                if i == -1:
                    plane = plane * zlo
                elif i == 8:
                    plane = plane * zhi
                row = plane_row1(i)
                if c in (0, 7):
                    as1[c, row:row + 32, :] = plane
                cut(c, row, plane)

            def column(y, p, size):
                return zs1[c, pl.ds(p * PITCH1 + 8 + y, size, stride=PITCH1), :]

            as1[c, 320:328, :] = column(0, 1, 8) * ylo
            as1[c, 336:344, :] = weighted({0: column(62, 1, 8), 1: column(63, 1, 8)}) * yhi
            for s, p, zflag in ((0, 0, zlo), (1, 9, zhi)):
                first = p * PITCH1 + 8
                as1[c, 328 + s:329 + s, :] = zs1[c, first:first + 1, :] * (ylo * zflag)
                as1[c, 344 + s:345 + s, :] = weighted(
                    {0: zs1[c, first + 62:first + 63, :], 1: zs1[c, first + 63:first + 64, :]}
                ) * (yhi * zflag)
            cut(c, 320, as1[c, 320:352, :])

    def level_one_product(blocks):
        group = GROUP[blocks[0]][0]
        total = None
        for piece in range(3):
            part = jnp.dot(cut1[group, piece], band[...], preferred_element_type=F32)
            total = part if total is None else total + part
        for b in blocks:
            at = GROUP[b][1] * ROWS1
            p1[b] = total[at:at + ROWS1]

    def level_two_tile(source, t):
        for e, first in ((0, 320), (1, 336)):
            ye1[t, e, 8:16, :] = source[first:first + 8, :]
            ye1[t, e, 7:8, :] = source[first + 8:first + 9, :]
            ye1[t, e, 16:17, :] = source[first + 9:first + 10, :]
        for i in range(-1, 6):
            plane = reduce_planes(lambda s: source[plane_row1(s):plane_row1(s) + 32, :], -1, 8, i)
            if zscale2(i) is not None:
                plane = plane * zscale2(i)
            row = (i + 1) * PITCH2 + 8
            zs2[t, row:row + 32, :] = plane
        for e, y in ((0, -1), (1, 32)):
            block = weighted({k: ye1[t, e, pl.ds(4 + k, 8, stride=2), :] for k in range(5)})
            zs2[t, pl.ds(8 + y, 8, stride=PITCH2), :] = block * zflag2
        for i in range(-1, 6):
            base = (i + 1) * PITCH2 + 8
            row = plane_row2(i)
            as2[t, row:row + 16, :] = weighted(
                {k: zs2[t, pl.ds(base + k - 2, 16, stride=2), :] for k in range(5)}
            )

        def column2(y):
            return zs2[t, pl.ds(8 + y, 8, stride=PITCH2), :]

        as2[t, 112:120, :] = weighted({3: column2(-1), 4: column2(0)}) * ylo
        as2[t, 120:128, :] = weighted({0: column2(30), 1: column2(31), 2: column2(32)}) * yhi
        as2[t, 128:136, :] = column2(32) * yhi

    def level_three_tile(source, t):
        for e, first in ((0, 112), (1, 120), (2, 128)):
            ye2[t, e, 7:15, :] = source[first:first + 8, :]
        for i in range(-1, 4):
            row = (i + 1) * PITCH3 + 8
            zs3[t, row:row + 16, :] = reduce_planes(
                lambda s: source[plane_row2(s):plane_row2(s) + 16, :], -1, 5, i
            )
        for e, y in ((0, -1), (1, 16), (2, 17)):
            block = weighted({k: ye2[t, e, pl.ds(4 + k, 8, stride=2), :] for k in range(5)})
            zs3[t, pl.ds(8 + y, 8, stride=PITCH3), :] = block
        for i in range(-1, 4):
            base = (i + 1) * PITCH3 + 8
            row = plane_row3(i)
            as3[t, row:row + 8, :] = weighted(
                {k: zs3[t, pl.ds(base + k - 2, 8, stride=2), :] for k in range(5)}
            )

        def column3(y):
            return zs3[t, pl.ds(8 + y, 8, stride=PITCH3), :]

        as3[t, 40:48, :] = weighted({3: column3(-1), 4: column3(0)})
        as3[t, 48:56, :] = weighted({k: column3(14 + k) for k in range(4)})
        as3[t, 56:64, :] = weighted({0: column3(16), 1: column3(17)})

    def combine(parts, result, tiles, rows, mask):
        size = 16
        low = lax.broadcasted_iota(jnp.int32, (size, LANES), 1) < 64
        wide = None if mask is None else jnp.broadcast_to(mask[0:1], (size, LANES))
        total = tiles + 1
        for r in range(0, rows, size):
            over = [parts(t, r, size, 1) for t in range(total)]
            for t in range(total):
                before, after = over[(t - 1) % total], over[(t + 1) % total]
                if before is None:
                    spill = jnp.where(low, 0.0, after)
                elif after is None:
                    spill = jnp.where(low, before, 0.0)
                else:
                    spill = jnp.where(low, before, after)
                main = parts(t, r, size, 0)
                value = spill if main is None else main + spill
                if t == tiles and wide is not None:
                    value = value * wide
                result[t, r:r + size, :] = value

    main_groups = [(l1, 4, 8 * g) for g in range(32)] + [(l2, 2, 8 * g) for g in range(8)] + [(l3, 1, 8 * g) for g in range(2)]
    main_rows = [(x1, 8 * g) for g in range(32)] + [(x2, 8 * g) for g in range(8)] + [(x3, 8 * g) for g in range(2)]
    side_rows = (
        [(x1, 256 + 8 * g) for g in range(12)] + [(x2, 64 + 8 * g) for g in range(9)] + [(x3, 16 + 8 * g) for g in range(6)]
    )

    def pack(groups):
        total = None
        for g, (ref, row) in enumerate(groups):
            piece = ref[row:row + 8, :]
            piece = piece if g == 0 else pltpu.roll(piece, 3 * g, 1)
            total = piece if total is None else total + piece
        return total

    def ends(source, high, low):
        return jnp.concatenate([source[high], source[low]], axis=1)

    for i in range(2):
        loads[i].wait()
        level_one_tiles(*pieces[i])
    for i in range(2, 4):
        loads[i].wait()
    level_one_tiles(*pieces[2])
    level_one_tiles(*pieces[3])
    level_one_product((0, 3))
    level_two_tile(as1.at[0], 5)
    level_two_tile(as1.at[7], 6)
    level_three_tile(as2.at[5], 3)
    level_three_tile(as2.at[6], 4)
    x1[...] = product(ends(as1, 7, 0), ends1[...])
    x2[...] = product(ends(as2, 6, 5), ends2[...])
    block = ends(as3, 4, 3)
    x3[...] = product(block, ends3[0]) + product(block, ends3[1])
    xp[0] = pack(main_rows)
    xp[1] = pack(side_rows)
    one = {key: value.astype(jnp.int32) for key, value in has.items()}
    across_z = 1 + one["gz", 1] + one["gz", -1]
    across = across_z * (1 + one["gy", 1] + one["gy", -1])
    near_lower, near_upper = (one["gy", k] * across_z + one["gz", k] for k in (-1, 1))
    far_lower, far_upper = one["gx", -1] * across, one["gx", 1]

    def wait_for(semaphore, number):
        @pl.when(number > 0)
        def _():
            pl.semaphore_wait(semaphore, number)

    def answer(d):
        signal(ready.at[1 if d[2] else 0], d)


    def enter():
        wait_for(barrier, near_lower + far_lower)

        @pl.when(interior)
        def _():
            for d in [BEFORE] + NEAR_LOWER:
                answer(d)

        @pl.when(jnp.logical_not(interior))
        def _():
            for d in [BEFORE] + NEAR_LOWER:
                @pl.when(exists(d))
                def _():
                    answer(d)

        for_neighbours(start, (2,), only=FAR_LOWER)
        for_neighbours(start, (3,), only=NEAR_LOWER)

    last_column = jnp.logical_not(has["gx", 1])

    @pl.when(jnp.logical_not(last_column))
    def _():
        enter()

    for i in range(4, 6):
        loads[i].wait()
    level_one_tiles(*pieces[4])
    @pl.when(last_column)
    def _():
        enter()

    level_one_tiles(*pieces[5])
    level_one_product((1, 2))

    def parts1(t, r, size, half):
        return None if t == 4 else p1[t, r:r + size, 128 * half:128 * half + 128]

    combine(parts1, l1, 4, ROWS1, xflag)
    for_neighbours(start, (0,), only=LOWER)
    for t in range(5):
        level_two_tile(l1.at[t], t)
    for b in range(2):
        block = jnp.concatenate([as2[2 * b], as2[2 * b + 1]], axis=1)
        p2[b] = product(block, band[...])
    p2[2] = product(as2[4], edge[...])

    def parts2(t, r, size, half):
        return p2[t, r:r + size, 128 * half:128 * half + 128]

    combine(parts2, l2, 2, ROWS2, xflag)
    for_neighbours(start, (1,), only=LOWER)
    prompt = me["gx"] == counts["gx"] - 2

    def pass_on():
        wait_for(ready.at[0], near_upper)
        for_neighbours(start, (3,), only=NEAR_UPPER)

    @pl.when(prompt)
    def _():
        pass_on()


    for t in range(3):
        level_three_tile(l2.at[t], t)
    p3[0] = product(jnp.concatenate([as3[0], as3[1]], axis=1), band[...])
    p3[1] = product(as3[2], edge[...])

    def parts3(t, r, size, half):
        return p3[t, r:r + size, 128 * half:128 * half + 128]

    combine(parts3, l3, 1, ROWS3, None)

    for side, blocks2, blocks3 in ((0, (120, 128), (48, 56)), (1, (112,), (40,))):
        for t in range(2):
            for j, row in enumerate(blocks2):
                yf[side, t, 4 * j:4 * j + 4, :] = l2[t, row + 1:row + 5, :]
        for j, row in enumerate(blocks3):
            yf[side, 2, 2 * j:2 * j + 2, :] = l3[0, row + 1:row + 3, :]
        for dz in (1, -1):
            corner = CORNER[dz, 1 - 2 * side]
            row1 = (344 if side == 0 else 328) + (1 if dz == 1 else 0)
            first2, first3, size = (5, 3, 2) if dz == 1 else (0, 0, 1)
            for t in range(4):
                q[corner, t:t + 1, :] = l1[t, row1:row1 + 1, :]
            for t in range(2):
                for j, row in enumerate(blocks2):
                    to = 8 + 4 * t + 2 * j
                    q[corner, to:to + size, :] = l2[t, row + first2:row + first2 + size, :]
            for j, row in enumerate(blocks3):
                q[corner, 4 + 2 * j:4 + 2 * j + size, :] = l3[0, row + first3:row + first3 + size, :]


    for_neighbours(start, (2,), only=NEAR_LOWER)
    @pl.when(jnp.logical_not(prompt))
    def _():
        pass_on()

    for_neighbours(start, (0, 1, 2), only=NEAR_UPPER)
    wait_for(ready.at[1], far_upper)
    for_neighbours(start, (2,), only=[NEXT])
    settle(recv_sem.at[1], NEAR_LOWER, (3,), True)
    for_neighbours(start, (4,), only=[NEXT])
    settle(recv_sem.at[2], NEAR_UPPER, (3,), True)
    for_neighbours(start, (5,), only=[NEXT])

    heights, depths = (32, 16, 8), (8, 4, 2)
    levels = (l1, l2, l3)

    def add(level, t, rows, value):
        ref = levels[level]
        ref[t, rows, :] = ref[t, rows, :] + value

    def add_y(dy, level, t, get):
        height, depth = heights[level], depths[level]
        for j in range(2 if dy == 1 and level else 1):
            add(level, t, pl.ds(j if dy == 1 else height - 1, depth, stride=height), get(j))

    def add_z(dz, level, t, get):
        height, depth = heights[level], depths[level]
        planes = 2 if dz == 1 and level else 1
        to = 0 if dz == 1 else (depth - 1) * height
        for r in range(0, planes * height, 8):
            add(level, t, slice(to + r, to + r + 8), get(r))

    def add_corner(dz, dy, level, t, get):
        height, depth = heights[level], depths[level]
        planes = 2 if dz == 1 and level else 1
        for j in range(2 if dy == 1 and level else 1):
            value = get(j)
            for p in range(planes):
                row = (p if dz == 1 else depth - 1) * height + (j if dy == 1 else height - 1)
                add(level, t, slice(row, row + 1), value[p:p + 1])

    settle(recv_sem.at[3], FACES[2:], (0, 2), True)
    for dy in (1, -1):
        side = 0 if dy == 1 else 1
        for t in range(4):
            add_y(dy, 0, t, lambda j: ry1[side, t])
        for t in range(2):
            add_y(dy, 1, t, lambda j: ryf[side, t, 4 * j:4 * j + 4, :])
        add_y(dy, 2, 0, lambda j: ryf[side, 2, 2 * j:2 * j + 2, :])
    settle(recv_sem.at[4], FACES[:2], (0, 1, 2), True)
    for t in range(4):
        add_z(1, 0, t, lambda r: rz1[0, t, r:r + 8, :])
        add_z(-1, 0, t, lambda r: rz1[1, t, r:r + 8, :])
    for t in range(2):
        add_z(1, 1, t, lambda r: rz2u[t, r:r + 8, :])
        add_z(-1, 1, t, lambda r: rz2d[t, r:r + 8, :])
    add_z(1, 2, 0, lambda r: rz3u[0, r:r + 8, :])
    add_z(-1, 2, 0, lambda r: rz3d[0, r:r + 8, :])
    settle(send_sem.at[0], TARGETS, None, False)
    settle(send_sem.at[1], NEAR_LOWER + NEAR_UPPER, (0, 1, 2), False)
    settle(recv_sem.at[0], [NEXT] + FAR_LOWER, (2, 4), True)
    third = lax.rem(lane, 3)
    low_lanes, high_lane = lane < 2, lane == 127

    def both(low_side, high_side):
        return jnp.where((third == 2) | high_lane, high_side, low_side)

    def spread(value, g):
        moved = value if g == 0 else pltpu.roll(value, LANES - 3 * g, 1)
        return jnp.where(low_lanes, moved, 0.0), jnp.where(high_lane, moved, 0.0)

    def add_columns(level, pairs, keep=(True, True)):
        last = (3, 1, 0)[level]
        for rows, (low_value, high_value) in pairs:
            if last == 0 and keep == (True, True):
                add(level, 0, rows, low_value + high_value)
                continue
            if keep[0]:
                add(level, 0, rows, low_value)
            if keep[1]:
                add(level, last, rows, high_value)

    value = both(rx[0], rx[1])
    for g, (ref, _, row) in enumerate(main_groups):
        level = 0 if g < 32 else (1 if g < 40 else 2)
        add_columns(level, [(slice(row, row + 8), spread(value, g))])
    firsts = {0: 0, 1: 12, 2: 21}

    def add_sides(sides, values, keep):
        for dz, dy in sides:
            value = values(SIDE[dz, dy])
            for level in range(3):
                height, depth = heights[level], depths[level]
                if dy == 0:
                    first = firsts[level] + (height // 8 if dz == 1 else 0)
                    planes = 2 if dz == 1 and level else 1
                    to = 0 if dz == 1 else (depth - 1) * height
                    for r in range(planes * height // 8):
                        add_columns(level, [(slice(to + 8 * r, to + 8 * r + 8), spread(value, first + r))], keep)
                    continue
                for j in range(2 if dy == 1 and level else 1):
                    y = j if dy == 1 else height - 1
                    if level == 0:
                        group = (10 if dy == 1 else 8) + (1 if dz else 0)
                    else:
                        group = {1: (18, 19), 2: (24, 25)}[level][1 if dy == 1 else 0] + j
                    parts = spread(value, group)
                    if dz == 0:
                        if level:
                            parts = tuple(x[1:1 + depth] for x in parts)
                        add_columns(level, [(pl.ds(y, depth, stride=height), parts)], keep)
                        continue
                    for p in range(2 if dz == 1 and level else 1):
                        if level == 0:
                            s = 1 if dz == 1 else 0
                        else:
                            s = depth + 1 + p if dz == 1 else 0
                        z = p if dz == 1 else depth - 1
                        row = slice(z * height + y, z * height + y + 1)
                        add_columns(level, [(row, tuple(x[s:s + 1] for x in parts))], keep)

    add_sides(SIDES[:4], lambda i: both(rru[i], rrd[i]), (True, True))
    add_sides(SIDES[4:], lambda i: rrd[i], (False, True))
    settle(recv_sem.at[6], list(d + (0,) for d in CORNER), (2,), True)
    for dz, dy in CORNER:
        c = CORNER[dz, dy]
        for t in range(4):
            add_corner(dz, dy, 0, t, lambda j: rq[c, t:t + 1, :])
        for t in range(2):
            add_corner(dz, dy, 1, t, lambda j: rq[c, 8 + 4 * t + 2 * j:10 + 4 * t + 2 * j, :])
        add_corner(dz, dy, 2, 0, lambda j: rq[c, 4 + 2 * j:6 + 2 * j, :])
    settle(recv_sem.at[5], [NEXT], (5,), True)
    add_sides(SIDES[4:], lambda i: rru[i], (True, False))

    for z in range(8):
        for t in range(4):
            out1[z, :, LANES * t:LANES * t + LANES] = l1[t, 32 * z:32 * z + 32, :]
    for z in range(4):
        for t in range(2):
            out2[z, :, LANES * t:LANES * t + LANES] = l2[t, 16 * z:16 * z + 16, :]
    for z in range(2):
        out3[z, :, :] = l3[0, 8 * z:8 * z + 8, :]


def store(in1, in2, in3, out1, out2, out3, sem):
    copies = [
        pltpu.make_async_copy(source, target, sem.at[i])
        for i, (source, target) in enumerate(((in1, out1), (in2, out2), (in3, out3)))
    ]
    for copy in copies:
        copy.start()
    for copy in copies:
        copy.wait()


def on_device(counts, volume):
    shapes = tuple(jax.ShapeDtypeStruct(s, F32) for s in ((8, 32, 512), (4, 16, 256), (2, 8, 128)))
    levels = levels_of(counts, shapes, volume)
    return pl.pallas_call(
        store,
        out_shape=shapes,
        in_specs=[pl.BlockSpec(memory_space=pltpu.VMEM)] * 3,
        out_specs=[pl.BlockSpec(memory_space=pltpu.HBM)] * 3,
        scratch_shapes=[pltpu.SemaphoreType.DMA((3,))],
        compiler_params=pltpu.CompilerParams(vmem_limit_bytes=52 * 1024 * 1024),
        name="store",
    )(*levels)


def levels_of(counts, shapes, volume):
    vmem = lambda *shape: pltpu.VMEM(shape, F32)
    return pl.pallas_call(
        functools.partial(pyramid, counts),
        out_shape=shapes,
        in_specs=[pl.BlockSpec(memory_space=pltpu.HBM)],
        out_specs=[pl.BlockSpec(memory_space=pltpu.VMEM)] * 3,
        scratch_shapes=[
            vmem(16, 64, 1024),
            vmem(8, 10 * PITCH1 + 8, LANES), vmem(8, ROWS1, LANES),
            pltpu.VMEM((2, 3, 2 * ROWS1, 256), BF16), vmem(4, ROWS1, 256), vmem(5, ROWS1, LANES),
            vmem(7, 2, 24, LANES), vmem(7, 8 * PITCH2, LANES), vmem(7, ROWS2, LANES), vmem(3, ROWS2, 256),
            vmem(3, ROWS2, LANES),
            vmem(5, 3, 24, LANES), vmem(5, 8 * PITCH3, LANES), vmem(5, ROWS3, LANES), vmem(2, ROWS3, 256),
            vmem(2, ROWS3, LANES),
            pltpu.VMEM((256, 256), BF16), pltpu.VMEM((128, 256), BF16),
            pltpu.VMEM((256, LANES), BF16), pltpu.VMEM((256, LANES), BF16), pltpu.VMEM((2, 256, LANES), BF16),
            vmem(ROWS1, LANES), vmem(ROWS2, LANES), vmem(ROWS3, LANES),
            vmem(2, 8, LANES), vmem(2, 3, 8, LANES), vmem(4, 16, LANES),
            vmem(2, 4, 32, LANES), vmem(2, 32, LANES), vmem(2, 16, LANES), vmem(1, 16, LANES), vmem(1, 8, LANES),
            vmem(2, 4, 8, LANES), vmem(2, 3, 8, LANES), vmem(4, 16, LANES),
            vmem(2, 8, LANES), vmem(8, 8, LANES), vmem(8, 8, LANES), vmem(8, 8, LANES),
            pltpu.SemaphoreType.DMA((6,)),
            pltpu.SemaphoreType.DMA((2,)),
            pltpu.SemaphoreType.DMA((7,)),
            pltpu.SemaphoreType.REGULAR((2,)),
        ],
        compiler_params=pltpu.CompilerParams(
            collective_id=0, has_side_effects=True, vmem_limit_bytes=52 * 1024 * 1024
        ),
        name="pyramid",
    )(volume)


def solution(mesh):
    spec = P("gz", "gy", "gx")
    return jax.shard_map(
        functools.partial(on_device, dict(mesh.shape)),
        mesh=mesh,
        in_specs=(spec,),
        out_specs=(spec, spec, spec),
        check_vma=False,
    )
```

```python
import functools
import math

import jax
import jax.numpy as jnp
from jax import lax
from jax.experimental import pallas as pl
from jax.experimental.pallas import tpu as pltpu
from jax.sharding import PartitionSpec as P

MESH = pl.DeviceIdType.MESH
F32 = jnp.float32
BF16 = jnp.bfloat16
LANES = 128
AXES = ("gz", "gy", "gx")
taps = (1.0, 4.0, 6.0, 4.0, 1.0)

ROWS1, ROWS2, ROWS3 = 352, 144, 64
PITCH1, PITCH2, PITCH3 = 72, 48, 32
DIRECTIONS = [
    (dz, dy, dx)
    for dx in (-1, 1, 0)
    for dz in (1, -1, 0)
    for dy in (-1, 1, 0)
    if (dz, dy, dx) != (0, 0, 0)
]
SIDES = [(1, -1), (-1, -1), (0, -1), (-1, 0), (1, 1), (-1, 1), (0, 1), (1, 0)]
SIDE = {d: i for i, d in enumerate(SIDES)}
UPPER = [d for d in DIRECTIONS if (d[2], d[1], d[0]) > (0, 0, 0)]
LOWER = [d for d in DIRECTIONS if (d[2], d[1], d[0]) < (0, 0, 0)]
TARGETS = [d for d in DIRECTIONS if d[2] < 1 or d == (0, 0, 1)]
NEAR_LOWER, NEAR_UPPER = ([d for d in half if not d[2]] for half in (LOWER, UPPER))
FAR_LOWER, NEXT, BEFORE = [d for d in LOWER if d[2]], (0, 0, 1), (0, 0, -1)
FACES = [(1, 0, 0), (-1, 0, 0), (0, 1, 0), (0, -1, 0)]
GROUP = {0: (0, 0), 3: (0, 1), 1: (1, 0), 2: (1, 1)}
CORNER = {(1, 1): 0, (1, -1): 1, (-1, 1): 2, (-1, -1): 3}


def weighted(pieces):
    groups = {}
    for k, piece in pieces.items():
        groups.setdefault(taps[k], []).append(piece)
    total = None
    for tap, members in groups.items():
        part = members[0] if len(members) == 1 else members[0] + members[1]
        part = part if tap == 1.0 else tap * part
        total = part if total is None else total + part
    return total


def reduce_planes(load, low, high, out):
    return weighted(
        {k: load(2 * out + k - 2) for k in range(5) if low <= 2 * out + k - 2 <= high}
    )


def split(block):
    first = block.astype(BF16)
    rest = block - first.astype(F32)
    second = rest.astype(BF16)
    third = (rest - second.astype(F32)).astype(BF16)
    return third, second, first


def product(block, weights):
    total = None
    for piece in split(block):
        part = jnp.dot(piece, weights, preferred_element_type=F32)
        total = part if total is None else total + part
    return total


def build_weights(band, edge):
    k = lax.broadcasted_iota(jnp.int32, (256, 256), 0)
    n = lax.broadcasted_iota(jnp.int32, (256, 256), 1)
    out = jnp.where(n < 128, n, jnp.where(n == 128, 128, jnp.where(n == 255, -1, 1000)))
    tap = k - 2 * out + 2
    value = jnp.where(tap == 2, 6.0, jnp.where((tap == 1) | (tap == 3), 4.0, jnp.where((tap == 0) | (tap == 4), 1.0, 0.0)))
    band[...] = (value * (1.0 / 4096.0)).astype(BF16)
    k = lax.broadcasted_iota(jnp.int32, (128, 256), 0)
    n = lax.broadcasted_iota(jnp.int32, (128, 256), 1)
    place = jnp.where(k < 2, k, jnp.where(k == 127, -1, 1000))
    out = jnp.where(n < 2, n, jnp.where(n == 127, -1, jnp.where(n == 255, -1, jnp.where(n == 128, 0, -1000))))
    high_in, low_in = k < 2, k == 127
    high_out = (n < 2) | (n == 255)
    low_out = (n == 127) | (n == 128)
    tap = place - 2 * out + 2
    legal = (high_in & high_out) | (low_in & low_out)
    value = jnp.where(tap == 2, 6.0, jnp.where((tap == 1) | (tap == 3), 4.0, jnp.where((tap == 0) | (tap == 4), 1.0, 0.0)))
    edge[...] = jnp.where(legal, value * (1.0 / 4096.0), 0.0).astype(BF16)


def build_end_weights(ends1, ends2, ends3):
    tap1 = [6, 4, 1]
    tap2 = [44, 40, 31, 20, 10, 4, 1]
    tap3 = [344, 336, 315, 284, 246, 204, 161, 120, 84, 56, 35, 20, 10, 4, 1]
    k = lax.broadcasted_iota(jnp.int32, (32, LANES), 0) - 16
    lane = lax.broadcasted_iota(jnp.int32, (32, LANES), 1)
    zero = jnp.zeros((112, LANES), BF16)

    def fill(ref, value):
        ref[0:112, :] = zero
        ref[112:144, :] = value.astype(BF16)
        ref[144:256, :] = zero

    for level, taps_of in enumerate((tap1, tap2, tap3)):
        step = 2 << level
        high = jnp.where((k < 0) & (lane < 2), step * lane - k, 99)
        distance = jnp.where((k >= 0) & (lane == 127), k + step, high)
        scale = 1.0 / 4096.0 ** (level + 1)
        value = jnp.zeros((32, LANES), F32)
        for offset, tap in enumerate(taps_of):
            value = jnp.where(distance == offset, (316 if tap == 315 else tap) * scale, value)
        if level == 0:
            fill(ends1, value)
        elif level == 1:
            fill(ends2, value)
        else:
            fill(ends3.at[0], value)
            fill(ends3.at[1], jnp.where(distance == 2, -scale, 0.0))


def pyramid(counts, vol, out1, out2, out3, v, zs1, as1, cut1, p1, l1, ye1, zs2, as2, p2, l2, ye2, zs3, as3, p3, l3,
            band, edge, ends1, ends2, ends3, x1, x2, x3, xp, yf, q, rz1, rz2u, rz2d, rz3u, rz3d, ry1, ryf, rq, rx, ru, rru, rrd,
            load_sem, send_sem, recv_sem, ready):
    me = {axis: lax.axis_index(axis) for axis in ("gz", "gy", "gx")}
    has = {(axis, 1): me[axis] < counts[axis] - 1 for axis in me}
    has.update({(axis, -1): me[axis] > 0 for axis in me})

    def exists(d):
        ok = None
        for axis, step in zip(("gz", "gy", "gx"), d):
            if step:
                ok = has[axis, step] if ok is None else ok & has[axis, step]
        return ok

    def device(d):
        return {axis: me[axis] + step for axis, step in zip(("gz", "gy", "gx"), d) if step}

    def blank(d):
        dz, dy, dx = d
        zeros = jnp.zeros((8, LANES), F32)
        if d == NEXT:
            rx[0] = zeros
            for i in range(8):
                rru[i] = zeros
            return
        if dx:
            target = rrd.at[SIDE[dz, dy]] if dz or dy else rx.at[1]
            target[...] = zeros
            return
        ru[SIDE[dz, dy]] = zeros
        side = 0 if dy == 1 else 1
        if dz and dy:
            targets = [rq.at[CORNER[dz, dy]]]
        elif dy:
            targets = [ry1.at[side, t] for t in range(4)] + [ryf.at[side, t] for t in range(3)]
        elif dz == 1:
            targets = [rz1.at[0, t] for t in range(4)] + [rz2u.at[t] for t in range(2)] + [rz3u.at[0]]
        else:
            targets = [rz1.at[1, t] for t in range(4)] + [rz2d.at[t] for t in range(2)] + [rz3d.at[0]]
        for target in targets:
            for r in range(0, target.shape[0], 8):
                target[r:r + 8, :] = zeros

    pieces = ((0, 1), (7, 1), (1, 1), (6, 1), (2, 2), (4, 2))
    loads = [
        pltpu.make_async_copy(
            vol.at[:, :, pl.ds(LANES * c, LANES * n)], v.at[:, :, pl.ds(LANES * c, LANES * n)], load_sem.at[i]
        )
        for i, (c, n) in enumerate(pieces)
    ]
    for load in loads:
        load.start()

    barrier = pltpu.get_barrier_semaphore()
    interior = functools.reduce(lambda x, y: x & y, has.values())

    def signal(semaphore, d):
        pl.semaphore_signal(semaphore, inc=1, device_id=device(d), device_id_type=MESH)

    @pl.when(interior)
    def _():
        for d in UPPER:
            signal(barrier, d)

    @pl.when(jnp.logical_not(interior))
    def _():
        for d in UPPER:
            @pl.when(exists(d))
            def _():
                signal(barrier, d)

        for d in TARGETS:
            @pl.when(jnp.logical_not(exists(tuple(-k for k in d))))
            def _():
                blank(d)

    build_weights(band, edge)
    build_end_weights(ends1, ends2, ends3)
    zero8 = jnp.zeros((8, LANES), F32)
    for c in range(8):
        for p in range(11):
            zs1[c, p * PITCH1:p * PITCH1 + 8, :] = zero8
        as1[c, 328:336, :] = zero8
        as1[c, 344:352, :] = zero8
    for c in range(4):
        q[c, 0:8, :] = zero8
        q[c, 8:16, :] = zero8
    for side in range(2):
        for t in range(3):
            yf[side, t] = zero8
    for t in range(7):
        for e in range(2):
            for r in range(0, 24, 8):
                ye1[t, e, r:r + 8, :] = zero8
        for p in range(8):
            zs2[t, p * PITCH2:p * PITCH2 + 8, :] = zero8
            zs2[t, p * PITCH2 + 40:p * PITCH2 + 48, :] = zero8
        for r in range(8, 40, 8):
            zs2[t, 7 * PITCH2 + r:7 * PITCH2 + r + 8, :] = zero8
        as2[t, 136:144, :] = zero8
    for t in range(5):
        for e in range(3):
            for r in range(0, 24, 8):
                ye2[t, e, r:r + 8, :] = zero8
        for p in range(8):
            zs3[t, p * PITCH3:p * PITCH3 + 8, :] = zero8
            zs3[t, p * PITCH3 + 24:p * PITCH3 + 32, :] = zero8
        for p in range(5, 8):
            for r in (8, 16):
                zs3[t, p * PITCH3 + r:p * PITCH3 + r + 8, :] = zero8

    flag = {key: jnp.where(value, 1.0, 0.0).astype(F32) for key, value in has.items()}
    zlo, zhi = flag["gz", -1], flag["gz", 1]
    ylo, yhi = flag["gy", -1], flag["gy", 1]
    lane = lax.broadcasted_iota(jnp.int32, (8, LANES), 1)
    sub = lax.broadcasted_iota(jnp.int32, (8, LANES), 0)
    xflag = jnp.where(lane < 64, flag["gx", 1], flag["gx", -1])

    def transfers(d):
        dz, dy, dx = d
        if dx == 1:
            return {
                2: (xp.at[0], rx.at[0]),
                4: (ru.at[pl.ds(0, 4)], rru.at[pl.ds(0, 4)]),
                5: (ru.at[pl.ds(4, 4)], rru.at[pl.ds(4, 4)]),
            }
        if dx == -1:
            return {2: (xp.at[1], rrd.at[SIDE[dz, dy]]) if dz or dy else (xp.at[0], rx.at[1])}
        along = (xp.at[1], ru.at[SIDE[dz, dy]])
        if dy == 0:
            if dz == 1:
                return {
                    0: (l1.at[pl.ds(0, 4), pl.ds(288, 32), :], rz1.at[0]),
                    1: (l2.at[pl.ds(0, 2), pl.ds(80, 32), :], rz2u),
                    2: (l3.at[pl.ds(0, 1), pl.ds(24, 16), :], rz3u),
                    3: along,
                }
            return {
                0: (l1.at[pl.ds(0, 4), pl.ds(256, 32), :], rz1.at[1]),
                1: (l2.at[pl.ds(0, 2), pl.ds(64, 16), :], rz2d),
                2: (l3.at[pl.ds(0, 1), pl.ds(16, 8), :], rz3d),
                3: along,
            }
        if dz == 0:
            side = 0 if dy == 1 else 1
            return {
                0: (l1.at[pl.ds(0, 4), pl.ds(336 if dy == 1 else 320, 8), :], ry1.at[side]),
                2: (yf.at[side], ryf.at[side]),
                3: along,
            }
        corner = CORNER[dz, dy]
        return {2: (q.at[corner], rq.at[corner]), 3: along}

    def awaited_with(d, stage):
        if d[2]:
            return 5 if stage == 5 else 0
        if stage == 3:
            return 1 if d in NEAR_LOWER else 2
        return (6 if d[0] else 3) if d[1] else 4

    def copies(d, stages=(0, 1, 2, 3, 4, 5)):
        return [
            pltpu.make_async_remote_copy(
                src_ref=pair[0],
                dst_ref=pair[1],
                send_sem=send_sem.at[0 if d[2] or i == 3 else 1],
                recv_sem=recv_sem.at[awaited_with(d, i)],
                device_id=device(d),
                device_id_type=MESH,
            )
            for i, pair in transfers(d).items()
            if i in stages
        ]

    def for_neighbours(act, stages=(0, 1, 2, 3, 4, 5), back=False, only=None):
        chosen = [d for d in (only or TARGETS) if any(i in stages for i in transfers(d))]

        @pl.when(interior)
        def _():
            for d in chosen:
                for copy in copies(d, stages):
                    act(copy)

        @pl.when(jnp.logical_not(interior))
        def _():
            for d in chosen:
                @pl.when(exists(tuple(-k for k in d) if back else d))
                def _():
                    for copy in copies(d, stages):
                        act(copy)

    start = lambda c: c.start()

    def settle(semaphore, only, stages, back):
        parts = []
        for d in only:
            units = sum(
                math.prod(pair[0].shape) // 1024
                for i, pair in transfers(d).items()
                if (i in stages if stages else d[2] or i == 3)
            )
            parts.append((tuple(-k for k in d) if back else d, units))
        axes = [a for j, a in enumerate(AXES) if any(d[j] for d, _ in parts)]

        def wait(state):
            units = sum(u for d, u in parts if all(state[a, k] for a, k in zip(AXES, d) if k))
            if units:
                rows = pl.ds(0, 8 * units)
                pltpu.make_async_copy(zs1.at[0, rows, :], zs1.at[1, rows, :], semaphore).wait()

        def choose(left, state):
            if not left:
                wait(state)
                return
            axis = left[0]
            for low, high in ((True, True), (True, False), (False, True)):
                fits = has[axis, -1] if low else jnp.logical_not(has[axis, -1])
                fits &= has[axis, 1] if high else jnp.logical_not(has[axis, 1])

                @pl.when(fits)
                def _():
                    choose(left[1:], {**state, (axis, -1): low, (axis, 1): high})

        @pl.when(interior)
        def _():
            wait({(a, k): True for a in AXES for k in (-1, 1)})

        @pl.when(jnp.logical_not(interior))
        def _():
            choose(axes, {})

    zflag2 = jnp.where(sub == 0, zlo, jnp.where(sub < 5, 1.0, zhi))
    plane_row1 = lambda s: 256 if s == -1 else (288 if s == 8 else 32 * s)
    plane_row2 = lambda s: 64 if s == -1 else (80 + 16 * (s - 4) if s >= 4 else 16 * s)
    plane_row3 = lambda s: 16 if s == -1 else (24 + 8 * (s - 2) if s >= 2 else 8 * s)
    zscale2 = lambda i: zlo if i == -1 else (zhi if i >= 4 else None)

    def cut(c, row, block):
        group, place = GROUP[c // 2]
        at = place * ROWS1 + row
        for piece, value in enumerate(split(block)):
            cut1[group, piece, at:at + block.shape[0], LANES * (c % 2):LANES * (c % 2) + LANES] = value

    def level_one_tiles(c, n):
        for r in range(0, 64, 8):
            planes = [v[s, r:r + 8, LANES * c:LANES * (c + n)] for s in range(16)]
            for i in range(-1, 9):
                plane = reduce_planes(lambda s: planes[s], 0, 15, i)
                row = (i + 1) * PITCH1 + 8 + r
                for h in range(n):
                    zs1[c + h, row:row + 8, :] = plane[:, LANES * h:LANES * h + LANES]
        for c in range(c, c + n):
            for i in range(-1, 9):
                base = (i + 1) * PITCH1 + 8
                plane = weighted({k: zs1[c, pl.ds(base + k - 2, 32, stride=2), :] for k in range(5)})
                if i == -1:
                    plane = plane * zlo
                elif i == 8:
                    plane = plane * zhi
                row = plane_row1(i)
                if c in (0, 7):
                    as1[c, row:row + 32, :] = plane
                cut(c, row, plane)

            def column(y, p, size):
                return zs1[c, pl.ds(p * PITCH1 + 8 + y, size, stride=PITCH1), :]

            as1[c, 320:328, :] = column(0, 1, 8) * ylo
            as1[c, 336:344, :] = weighted({0: column(62, 1, 8), 1: column(63, 1, 8)}) * yhi
            for s, p, zflag in ((0, 0, zlo), (1, 9, zhi)):
                first = p * PITCH1 + 8
                as1[c, 328 + s:329 + s, :] = zs1[c, first:first + 1, :] * (ylo * zflag)
                as1[c, 344 + s:345 + s, :] = weighted(
                    {0: zs1[c, first + 62:first + 63, :], 1: zs1[c, first + 63:first + 64, :]}
                ) * (yhi * zflag)
            cut(c, 320, as1[c, 320:352, :])

    def level_one_product(blocks):
        group = GROUP[blocks[0]][0]
        total = None
        for piece in range(3):
            part = jnp.dot(cut1[group, piece], band[...], preferred_element_type=F32)
            total = part if total is None else total + part
        for b in blocks:
            at = GROUP[b][1] * ROWS1
            p1[b] = total[at:at + ROWS1]

    def level_two_tile(source, t):
        for e, first in ((0, 320), (1, 336)):
            ye1[t, e, 8:16, :] = source[first:first + 8, :]
            ye1[t, e, 7:8, :] = source[first + 8:first + 9, :]
            ye1[t, e, 16:17, :] = source[first + 9:first + 10, :]
        for i in range(-1, 6):
            plane = reduce_planes(lambda s: source[plane_row1(s):plane_row1(s) + 32, :], -1, 8, i)
            if zscale2(i) is not None:
                plane = plane * zscale2(i)
            row = (i + 1) * PITCH2 + 8
            zs2[t, row:row + 32, :] = plane
        for e, y in ((0, -1), (1, 32)):
            block = weighted({k: ye1[t, e, pl.ds(4 + k, 8, stride=2), :] for k in range(5)})
            zs2[t, pl.ds(8 + y, 8, stride=PITCH2), :] = block * zflag2
        for i in range(-1, 6):
            base = (i + 1) * PITCH2 + 8
            row = plane_row2(i)
            as2[t, row:row + 16, :] = weighted(
                {k: zs2[t, pl.ds(base + k - 2, 16, stride=2), :] for k in range(5)}
            )

        def column2(y):
            return zs2[t, pl.ds(8 + y, 8, stride=PITCH2), :]

        as2[t, 112:120, :] = weighted({3: column2(-1), 4: column2(0)}) * ylo
        as2[t, 120:128, :] = weighted({0: column2(30), 1: column2(31), 2: column2(32)}) * yhi
        as2[t, 128:136, :] = column2(32) * yhi

    def level_three_tile(source, t):
        for e, first in ((0, 112), (1, 120), (2, 128)):
            ye2[t, e, 7:15, :] = source[first:first + 8, :]
        for i in range(-1, 4):
            row = (i + 1) * PITCH3 + 8
            zs3[t, row:row + 16, :] = reduce_planes(
                lambda s: source[plane_row2(s):plane_row2(s) + 16, :], -1, 5, i
            )
        for e, y in ((0, -1), (1, 16), (2, 17)):
            block = weighted({k: ye2[t, e, pl.ds(4 + k, 8, stride=2), :] for k in range(5)})
            zs3[t, pl.ds(8 + y, 8, stride=PITCH3), :] = block
        for i in range(-1, 4):
            base = (i + 1) * PITCH3 + 8
            row = plane_row3(i)
            as3[t, row:row + 8, :] = weighted(
                {k: zs3[t, pl.ds(base + k - 2, 8, stride=2), :] for k in range(5)}
            )

        def column3(y):
            return zs3[t, pl.ds(8 + y, 8, stride=PITCH3), :]

        as3[t, 40:48, :] = weighted({3: column3(-1), 4: column3(0)})
        as3[t, 48:56, :] = weighted({k: column3(14 + k) for k in range(4)})
        as3[t, 56:64, :] = weighted({0: column3(16), 1: column3(17)})

    def combine(parts, result, tiles, rows, mask):
        size = 16
        low = lax.broadcasted_iota(jnp.int32, (size, LANES), 1) < 64
        wide = None if mask is None else jnp.broadcast_to(mask[0:1], (size, LANES))
        total = tiles + 1
        for r in range(0, rows, size):
            over = [parts(t, r, size, 1) for t in range(total)]
            for t in range(total):
                before, after = over[(t - 1) % total], over[(t + 1) % total]
                if before is None:
                    spill = jnp.where(low, 0.0, after)
                elif after is None:
                    spill = jnp.where(low, before, 0.0)
                else:
                    spill = jnp.where(low, before, after)
                main = parts(t, r, size, 0)
                value = spill if main is None else main + spill
                if t == tiles and wide is not None:
                    value = value * wide
                result[t, r:r + size, :] = value

    main_groups = [(l1, 4, 8 * g) for g in range(32)] + [(l2, 2, 8 * g) for g in range(8)] + [(l3, 1, 8 * g) for g in range(2)]
    main_rows = [(x1, 8 * g) for g in range(32)] + [(x2, 8 * g) for g in range(8)] + [(x3, 8 * g) for g in range(2)]
    side_rows = (
        [(x1, 256 + 8 * g) for g in range(12)] + [(x2, 64 + 8 * g) for g in range(9)] + [(x3, 16 + 8 * g) for g in range(6)]
    )

    def pack(groups):
        total = None
        for g, (ref, row) in enumerate(groups):
            piece = ref[row:row + 8, :]
            piece = piece if g == 0 else pltpu.roll(piece, 3 * g, 1)
            total = piece if total is None else total + piece
        return total

    def ends(source, high, low):
        return jnp.concatenate([source[high], source[low]], axis=1)

    for i in range(2):
        loads[i].wait()
        level_one_tiles(*pieces[i])
    for i in range(2, 4):
        loads[i].wait()
    level_one_tiles(*pieces[2])
    level_one_tiles(*pieces[3])
    level_one_product((0, 3))
    level_two_tile(as1.at[0], 5)
    level_two_tile(as1.at[7], 6)
    level_three_tile(as2.at[5], 3)
    level_three_tile(as2.at[6], 4)
    x1[...] = product(ends(as1, 7, 0), ends1[...])
    x2[...] = product(ends(as2, 6, 5), ends2[...])
    block = ends(as3, 4, 3)
    x3[...] = product(block, ends3[0]) + product(block, ends3[1])
    xp[0] = pack(main_rows)
    xp[1] = pack(side_rows)
    one = {key: value.astype(jnp.int32) for key, value in has.items()}
    across_z = 1 + one["gz", 1] + one["gz", -1]
    across = across_z * (1 + one["gy", 1] + one["gy", -1])
    near_lower, near_upper = (one["gy", k] * across_z + one["gz", k] for k in (-1, 1))
    far_lower, far_upper = one["gx", -1] * across, one["gx", 1]

    def wait_for(semaphore, number):
        @pl.when(number > 0)
        def _():
            pl.semaphore_wait(semaphore, number)

    def answer(d):
        signal(ready.at[1 if d[2] else 0], d)


    def enter():
        wait_for(barrier, near_lower + far_lower)

        @pl.when(interior)
        def _():
            for d in [BEFORE] + NEAR_LOWER:
                answer(d)

        @pl.when(jnp.logical_not(interior))
        def _():
            for d in [BEFORE] + NEAR_LOWER:
                @pl.when(exists(d))
                def _():
                    answer(d)

        for_neighbours(start, (2,), only=FAR_LOWER)
        for_neighbours(start, (3,), only=NEAR_LOWER)

    last_column = jnp.logical_not(has["gx", 1])

    @pl.when(jnp.logical_not(last_column))
    def _():
        enter()

    for i in range(4, 6):
        loads[i].wait()
    level_one_tiles(*pieces[4])
    @pl.when(last_column)
    def _():
        enter()

    level_one_tiles(*pieces[5])
    level_one_product((1, 2))

    def parts1(t, r, size, half):
        return None if t == 4 else p1[t, r:r + size, 128 * half:128 * half + 128]

    combine(parts1, l1, 4, ROWS1, xflag)
    for_neighbours(start, (0,), only=LOWER)
    even = lax.rem(me["gz"], 2) == 0
    prompt = me["gx"] == counts["gx"] - 2

    def pass_on():
        wait_for(ready.at[0], near_upper)
        for_neighbours(start, (3,), only=NEAR_UPPER)

    @pl.when(prompt & even)
    def _():
        pass_on()

    for t in range(5):
        level_two_tile(l1.at[t], t)
    for b in range(2):
        block = jnp.concatenate([as2[2 * b], as2[2 * b + 1]], axis=1)
        p2[b] = product(block, band[...])
    p2[2] = product(as2[4], edge[...])

    def parts2(t, r, size, half):
        return p2[t, r:r + size, 128 * half:128 * half + 128]

    combine(parts2, l2, 2, ROWS2, xflag)
    for_neighbours(start, (1,), only=LOWER)

    @pl.when(prompt & jnp.logical_not(even))
    def _():
        pass_on()

    for t in range(3):
        level_three_tile(l2.at[t], t)
    p3[0] = product(jnp.concatenate([as3[0], as3[1]], axis=1), band[...])
    p3[1] = product(as3[2], edge[...])

    def parts3(t, r, size, half):
        return p3[t, r:r + size, 128 * half:128 * half + 128]

    combine(parts3, l3, 1, ROWS3, None)

    for side, blocks2, blocks3 in ((0, (120, 128), (48, 56)), (1, (112,), (40,))):
        for t in range(2):
            for j, row in enumerate(blocks2):
                yf[side, t, 4 * j:4 * j + 4, :] = l2[t, row + 1:row + 5, :]
        for j, row in enumerate(blocks3):
            yf[side, 2, 2 * j:2 * j + 2, :] = l3[0, row + 1:row + 3, :]
        for dz in (1, -1):
            corner = CORNER[dz, 1 - 2 * side]
            row1 = (344 if side == 0 else 328) + (1 if dz == 1 else 0)
            first2, first3, size = (5, 3, 2) if dz == 1 else (0, 0, 1)
            for t in range(4):
                q[corner, t:t + 1, :] = l1[t, row1:row1 + 1, :]
            for t in range(2):
                for j, row in enumerate(blocks2):
                    to = 8 + 4 * t + 2 * j
                    q[corner, to:to + size, :] = l2[t, row + first2:row + first2 + size, :]
            for j, row in enumerate(blocks3):
                q[corner, 4 + 2 * j:4 + 2 * j + size, :] = l3[0, row + first3:row + first3 + size, :]


    for_neighbours(start, (2,), only=NEAR_LOWER)
    @pl.when(jnp.logical_not(prompt))
    def _():
        pass_on()

    for_neighbours(start, (0, 1, 2), only=NEAR_UPPER)
    wait_for(ready.at[1], far_upper)
    for_neighbours(start, (2,), only=[NEXT])
    settle(recv_sem.at[1], NEAR_LOWER, (3,), True)
    for_neighbours(start, (4,), only=[NEXT])
    settle(recv_sem.at[2], NEAR_UPPER, (3,), True)
    for_neighbours(start, (5,), only=[NEXT])

    heights, depths = (32, 16, 8), (8, 4, 2)
    levels = (l1, l2, l3)

    def add(level, t, rows, value):
        ref = levels[level]
        ref[t, rows, :] = ref[t, rows, :] + value

    def add_y(dy, level, t, get):
        height, depth = heights[level], depths[level]
        for j in range(2 if dy == 1 and level else 1):
            add(level, t, pl.ds(j if dy == 1 else height - 1, depth, stride=height), get(j))

    def add_z(dz, level, t, get):
        height, depth = heights[level], depths[level]
        planes = 2 if dz == 1 and level else 1
        to = 0 if dz == 1 else (depth - 1) * height
        for r in range(0, planes * height, 8):
            add(level, t, slice(to + r, to + r + 8), get(r))

    def add_corner(dz, dy, level, t, get):
        height, depth = heights[level], depths[level]
        planes = 2 if dz == 1 and level else 1
        for j in range(2 if dy == 1 and level else 1):
            value = get(j)
            for p in range(planes):
                row = (p if dz == 1 else depth - 1) * height + (j if dy == 1 else height - 1)
                add(level, t, slice(row, row + 1), value[p:p + 1])

    settle(recv_sem.at[3], FACES[2:], (0, 2), True)
    for dy in (1, -1):
        side = 0 if dy == 1 else 1
        for t in range(4):
            add_y(dy, 0, t, lambda j: ry1[side, t])
        for t in range(2):
            add_y(dy, 1, t, lambda j: ryf[side, t, 4 * j:4 * j + 4, :])
        add_y(dy, 2, 0, lambda j: ryf[side, 2, 2 * j:2 * j + 2, :])
    settle(recv_sem.at[4], FACES[:2], (0, 1, 2), True)
    for t in range(4):
        add_z(1, 0, t, lambda r: rz1[0, t, r:r + 8, :])
        add_z(-1, 0, t, lambda r: rz1[1, t, r:r + 8, :])
    for t in range(2):
        add_z(1, 1, t, lambda r: rz2u[t, r:r + 8, :])
        add_z(-1, 1, t, lambda r: rz2d[t, r:r + 8, :])
    add_z(1, 2, 0, lambda r: rz3u[0, r:r + 8, :])
    add_z(-1, 2, 0, lambda r: rz3d[0, r:r + 8, :])
    settle(send_sem.at[0], TARGETS, None, False)
    settle(send_sem.at[1], NEAR_LOWER + NEAR_UPPER, (0, 1, 2), False)
    settle(recv_sem.at[0], [NEXT] + FAR_LOWER, (2, 4), True)
    third = lax.rem(lane, 3)
    low_lanes, high_lane = lane < 2, lane == 127

    def both(low_side, high_side):
        return jnp.where((third == 2) | high_lane, high_side, low_side)

    def spread(value, g):
        moved = value if g == 0 else pltpu.roll(value, LANES - 3 * g, 1)
        return jnp.where(low_lanes, moved, 0.0), jnp.where(high_lane, moved, 0.0)

    def add_columns(level, pairs, keep=(True, True)):
        last = (3, 1, 0)[level]
        for rows, (low_value, high_value) in pairs:
            if last == 0 and keep == (True, True):
                add(level, 0, rows, low_value + high_value)
                continue
            if keep[0]:
                add(level, 0, rows, low_value)
            if keep[1]:
                add(level, last, rows, high_value)

    value = both(rx[0], rx[1])
    for g, (ref, _, row) in enumerate(main_groups):
        level = 0 if g < 32 else (1 if g < 40 else 2)
        add_columns(level, [(slice(row, row + 8), spread(value, g))])
    firsts = {0: 0, 1: 12, 2: 21}

    def add_sides(sides, values, keep):
        for dz, dy in sides:
            value = values(SIDE[dz, dy])
            for level in range(3):
                height, depth = heights[level], depths[level]
                if dy == 0:
                    first = firsts[level] + (height // 8 if dz == 1 else 0)
                    planes = 2 if dz == 1 and level else 1
                    to = 0 if dz == 1 else (depth - 1) * height
                    for r in range(planes * height // 8):
                        add_columns(level, [(slice(to + 8 * r, to + 8 * r + 8), spread(value, first + r))], keep)
                    continue
                for j in range(2 if dy == 1 and level else 1):
                    y = j if dy == 1 else height - 1
                    if level == 0:
                        group = (10 if dy == 1 else 8) + (1 if dz else 0)
                    else:
                        group = {1: (18, 19), 2: (24, 25)}[level][1 if dy == 1 else 0] + j
                    parts = spread(value, group)
                    if dz == 0:
                        if level:
                            parts = tuple(x[1:1 + depth] for x in parts)
                        add_columns(level, [(pl.ds(y, depth, stride=height), parts)], keep)
                        continue
                    for p in range(2 if dz == 1 and level else 1):
                        if level == 0:
                            s = 1 if dz == 1 else 0
                        else:
                            s = depth + 1 + p if dz == 1 else 0
                        z = p if dz == 1 else depth - 1
                        row = slice(z * height + y, z * height + y + 1)
                        add_columns(level, [(row, tuple(x[s:s + 1] for x in parts))], keep)

    add_sides(SIDES[:4], lambda i: both(rru[i], rrd[i]), (True, True))
    add_sides(SIDES[4:], lambda i: rrd[i], (False, True))
    settle(recv_sem.at[6], list(d + (0,) for d in CORNER), (2,), True)
    for dz, dy in CORNER:
        c = CORNER[dz, dy]
        for t in range(4):
            add_corner(dz, dy, 0, t, lambda j: rq[c, t:t + 1, :])
        for t in range(2):
            add_corner(dz, dy, 1, t, lambda j: rq[c, 8 + 4 * t + 2 * j:10 + 4 * t + 2 * j, :])
        add_corner(dz, dy, 2, 0, lambda j: rq[c, 4 + 2 * j:6 + 2 * j, :])
    settle(recv_sem.at[5], [NEXT], (5,), True)
    add_sides(SIDES[4:], lambda i: rru[i], (True, False))

    for z in range(8):
        for t in range(4):
            out1[z, :, LANES * t:LANES * t + LANES] = l1[t, 32 * z:32 * z + 32, :]
    for z in range(4):
        for t in range(2):
            out2[z, :, LANES * t:LANES * t + LANES] = l2[t, 16 * z:16 * z + 16, :]
    for z in range(2):
        out3[z, :, :] = l3[0, 8 * z:8 * z + 8, :]


def store(in1, in2, in3, out1, out2, out3, sem):
    copies = [
        pltpu.make_async_copy(source, target, sem.at[i])
        for i, (source, target) in enumerate(((in1, out1), (in2, out2), (in3, out3)))
    ]
    for copy in copies:
        copy.start()
    for copy in copies:
        copy.wait()


def on_device(counts, volume):
    shapes = tuple(jax.ShapeDtypeStruct(s, F32) for s in ((8, 32, 512), (4, 16, 256), (2, 8, 128)))
    levels = levels_of(counts, shapes, volume)
    return pl.pallas_call(
        store,
        out_shape=shapes,
        in_specs=[pl.BlockSpec(memory_space=pltpu.VMEM)] * 3,
        out_specs=[pl.BlockSpec(memory_space=pltpu.HBM)] * 3,
        scratch_shapes=[pltpu.SemaphoreType.DMA((3,))],
        compiler_params=pltpu.CompilerParams(vmem_limit_bytes=52 * 1024 * 1024),
        name="store",
    )(*levels)


def levels_of(counts, shapes, volume):
    vmem = lambda *shape: pltpu.VMEM(shape, F32)
    return pl.pallas_call(
        functools.partial(pyramid, counts),
        out_shape=shapes,
        in_specs=[pl.BlockSpec(memory_space=pltpu.HBM)],
        out_specs=[pl.BlockSpec(memory_space=pltpu.VMEM)] * 3,
        scratch_shapes=[
            vmem(16, 64, 1024),
            vmem(8, 10 * PITCH1 + 8, LANES), vmem(8, ROWS1, LANES),
            pltpu.VMEM((2, 3, 2 * ROWS1, 256), BF16), vmem(4, ROWS1, 256), vmem(5, ROWS1, LANES),
            vmem(7, 2, 24, LANES), vmem(7, 8 * PITCH2, LANES), vmem(7, ROWS2, LANES), vmem(3, ROWS2, 256),
            vmem(3, ROWS2, LANES),
            vmem(5, 3, 24, LANES), vmem(5, 8 * PITCH3, LANES), vmem(5, ROWS3, LANES), vmem(2, ROWS3, 256),
            vmem(2, ROWS3, LANES),
            pltpu.VMEM((256, 256), BF16), pltpu.VMEM((128, 256), BF16),
            pltpu.VMEM((256, LANES), BF16), pltpu.VMEM((256, LANES), BF16), pltpu.VMEM((2, 256, LANES), BF16),
            vmem(ROWS1, LANES), vmem(ROWS2, LANES), vmem(ROWS3, LANES),
            vmem(2, 8, LANES), vmem(2, 3, 8, LANES), vmem(4, 16, LANES),
            vmem(2, 4, 32, LANES), vmem(2, 32, LANES), vmem(2, 16, LANES), vmem(1, 16, LANES), vmem(1, 8, LANES),
            vmem(2, 4, 8, LANES), vmem(2, 3, 8, LANES), vmem(4, 16, LANES),
            vmem(2, 8, LANES), vmem(8, 8, LANES), vmem(8, 8, LANES), vmem(8, 8, LANES),
            pltpu.SemaphoreType.DMA((6,)),
            pltpu.SemaphoreType.DMA((2,)),
            pltpu.SemaphoreType.DMA((7,)),
            pltpu.SemaphoreType.REGULAR((2,)),
        ],
        compiler_params=pltpu.CompilerParams(
            collective_id=0, has_side_effects=True, vmem_limit_bytes=52 * 1024 * 1024
        ),
        name="pyramid",
    )(volume)


def solution(mesh):
    spec = P("gz", "gy", "gx")
    return jax.shard_map(
        functools.partial(on_device, dict(mesh.shape)),
        mesh=mesh,
        in_specs=(spec,),
        out_specs=(spec, spec, spec),
        check_vma=False,
    )
```
